32 devices in a mesh: dp: 2 (over x), tp: 4 (over z), pp: 4 (over y, core).
Axes of the slice: x: 2, y: 2, z: 4, core: 2. Of those that a mesh axis runs over, the one named last changes fastest.
Arguments:
- x_in: bfloat16 [4, 1, 1024, 768], P('dp'), parts along dimension 0
- g_out: float32 [4, 1, 1024, 768], P('dp'), parts along dimension 0
- ln1_gain: float32 [4, 768], P('pp')
- ln1_bias: float32 [4, 768], P('pp')
- w_qkv: bfloat16 [4, 768, 12, 3, 64], P('pp', None, 'tp')
- b_qkv: bfloat16 [4, 12, 3, 64], P('pp', 'tp')
- w_out: bfloat16 [4, 12, 64, 768], P('pp', 'tp')
- b_out: bfloat16 [4, 768], P('pp')
- ln2_gain: float32 [4, 768], P('pp')
- ln2_bias: float32 [4, 768], P('pp')
- w_up: bfloat16 [4, 768, 3072], P('pp', None, 'tp')
- b_up: bfloat16 [4, 3072], P('pp', 'tp')
- w_down: bfloat16 [4, 3072, 768], P('pp', 'tp')
- b_down: bfloat16 [4, 768], P('pp')
Outputs:
- output 1: bfloat16 [4, 1, 1024, 768], P('dp'), parts along dimension 0
- output 2: float32 [8, 768], P(('dp', 'pp')), parts along dimension 0
- output 3: float32 [8, 768], P(('dp', 'pp')), parts along dimension 0
- output 4: float32 [8, 768, 12, 3, 64], P(('dp', 'pp'), None, 'tp'), parts along dimension 0
- output 5: float32 [8, 12, 3, 64], P(('dp', 'pp'), 'tp'), parts along dimension 0
- output 6: float32 [8, 12, 64, 768], P(('dp', 'pp'), 'tp'), parts along dimension 0
- output 7: float32 [8, 768], P(('dp', 'pp')), parts along dimension 0
- output 8: float32 [8, 768], P(('dp', 'pp')), parts along dimension 0
- output 9: float32 [8, 768], P(('dp', 'pp')), parts along dimension 0
- output 10: float32 [8, 768, 3072], P(('dp', 'pp'), None, 'tp'), parts along dimension 0
- output 11: float32 [8, 3072], P(('dp', 'pp'), 'tp'), parts along dimension 0
- output 12: float32 [8, 3072, 768], P(('dp', 'pp'), 'tp'), parts along dimension 0
- output 13: float32 [8, 768], P(('dp', 'pp')), parts along dimension 0
There are 2 independent parts. The reference program is written for one: setup_inputs(seed, part) draws one part's arguments, and reference() takes and returns one part's arrays. A program takes and returns all parts, laid end to end along the dimension named above; an argument that names none is the same for every part.
All inputs are finite; a program needn't handle non-finite values.
Results may differ from the reference program's by a relative error of at most 0.0183967.
Values are sent between devices in bfloat16 or wider.
A program may use at most 1 GiB of HBM per device.

```python
import jax
import jax.numpy as jnp
from jax import lax

NUM_MICRO = 2
MICRO_ROWS = 1
SEQ_LEN = 1024
MODEL_DIM = 768
NUM_HEADS = 12
HEAD_DIM = 64
FFN_DIM = 3072
NUM_STAGES = 4
ROT_DIM = HEAD_DIM // 4


def norm_core(hidden, gain, shift):
    center = hidden - jnp.mean(hidden, axis=-1, keepdims=True)
    var_term = jnp.mean(center * center, axis=-1, keepdims=True)
    return center * lax.rsqrt(var_term + 1e-5) * gain + shift


def rotary_tables():
    half_rot = ROT_DIM // 2
    inv_freq = 10000.0 ** (-(jnp.arange(half_rot, dtype=jnp.float32) * 2.0) / ROT_DIM)
    angles = jnp.arange(SEQ_LEN, dtype=jnp.float32)[:, None] * inv_freq[None, :]
    angles = jnp.concatenate([angles, angles], axis=-1)
    return jnp.cos(angles)[None, :, None, :], jnp.sin(angles)[None, :, None, :]


def apply_rotary(values, cos_tab, sin_tab):
    half_rot = ROT_DIM // 2
    rot_part = values[..., :ROT_DIM]
    turned = jnp.concatenate([-rot_part[..., half_rot:], rot_part[..., :half_rot]], axis=-1)
    return jnp.concatenate([rot_part * cos_tab + turned * sin_tab, values[..., ROT_DIM:]], axis=-1)


def attention(qkv_proj, cos_tab, sin_tab):
    query = apply_rotary(qkv_proj[:, :, :, 0].astype(jnp.float32), cos_tab, sin_tab).astype(jnp.bfloat16)
    key_rot = apply_rotary(qkv_proj[:, :, :, 1].astype(jnp.float32), cos_tab, sin_tab).astype(jnp.bfloat16)
    value_part = qkv_proj[:, :, :, 2]
    scores = jnp.einsum('bqhe,bkhe->bhqk', query.astype(jnp.float32), key_rot.astype(jnp.float32)) * (HEAD_DIM ** -0.5)
    positions = jnp.arange(SEQ_LEN)
    causal = positions[:, None] >= positions[None, :]
    scores = jnp.where(causal, scores, -1e30)
    probs = jax.nn.softmax(scores, axis=-1).astype(jnp.bfloat16)
    context = jnp.einsum('bhqk,bkhe->bqhe', probs.astype(jnp.float32), value_part.astype(jnp.float32))
    return context.astype(jnp.bfloat16)


def layer_forward(hidden, layer_wts, cos_tab, sin_tab):
    ln1_gain, ln1_bias, w_qkv, b_qkv, w_out, b_out, ln2_gain, ln2_bias, w_up, b_up, w_down, b_down = layer_wts
    tokens = MICRO_ROWS * SEQ_LEN
    hidden_f = hidden.reshape(tokens, MODEL_DIM).astype(jnp.float32)
    normed_a = norm_core(hidden_f, ln1_gain, ln1_bias).astype(jnp.bfloat16)
    normed_m = norm_core(hidden_f, ln2_gain, ln2_bias).astype(jnp.bfloat16)
    qkv_proj = jnp.dot(normed_a, w_qkv.reshape(MODEL_DIM, 3 * MODEL_DIM), preferred_element_type=jnp.float32)
    qkv_proj = (qkv_proj + b_qkv.reshape(3 * MODEL_DIM).astype(jnp.float32)).astype(jnp.bfloat16)
    qkv_proj = qkv_proj.reshape(MICRO_ROWS, SEQ_LEN, NUM_HEADS, 3, HEAD_DIM)
    context = attention(qkv_proj, cos_tab, sin_tab).reshape(tokens, MODEL_DIM)
    attn_sum = jnp.dot(context, w_out.reshape(MODEL_DIM, MODEL_DIM), preferred_element_type=jnp.float32)
    pre_act = jnp.dot(normed_m, w_up, preferred_element_type=jnp.float32) + b_up.astype(jnp.float32)
    hidden_mlp = jax.nn.gelu(pre_act, approximate=False).astype(jnp.bfloat16)
    mlp_sum = jnp.dot(hidden_mlp, w_down, preferred_element_type=jnp.float32)
    total = hidden_f + attn_sum + b_out.astype(jnp.float32) + mlp_sum + b_down.astype(jnp.float32)
    return total.astype(jnp.bfloat16).reshape(MICRO_ROWS, SEQ_LEN, MODEL_DIM)


def setup_inputs(seed: int = 0, part: int = 0) -> dict:
    weight_keys = jax.random.split(jax.random.key(seed), 12)
    data_keys = jax.random.split(jax.random.fold_in(jax.random.key(seed + 1), part), 2)
    act_shape = (NUM_MICRO, MICRO_ROWS, SEQ_LEN, MODEL_DIM)
    tokens = NUM_MICRO * MICRO_ROWS * SEQ_LEN
    vec_shape = (NUM_STAGES, MODEL_DIM)
    x_in = jax.random.normal(data_keys[0], act_shape, jnp.float32).astype(jnp.bfloat16)
    g_out = jax.random.normal(data_keys[1], act_shape, jnp.float32) * (tokens ** -0.5)
    return {
        'x_in': x_in,
        'g_out': g_out,
        'ln1_gain': 1.0 + 0.3 * jax.random.normal(weight_keys[0], vec_shape, jnp.float32),
        'ln1_bias': 0.3 * jax.random.normal(weight_keys[1], vec_shape, jnp.float32),
        'w_qkv': (jax.random.normal(weight_keys[2], (NUM_STAGES, MODEL_DIM, NUM_HEADS, 3, HEAD_DIM), jnp.float32) * MODEL_DIM ** -0.5).astype(jnp.bfloat16),
        'b_qkv': (0.5 * jax.random.normal(weight_keys[3], (NUM_STAGES, NUM_HEADS, 3, HEAD_DIM), jnp.float32)).astype(jnp.bfloat16),
        'w_out': (jax.random.normal(weight_keys[4], (NUM_STAGES, NUM_HEADS, HEAD_DIM, MODEL_DIM), jnp.float32) * MODEL_DIM ** -0.5).astype(jnp.bfloat16),
        'b_out': (0.5 * jax.random.normal(weight_keys[5], vec_shape, jnp.float32)).astype(jnp.bfloat16),
        'ln2_gain': 1.0 + 0.3 * jax.random.normal(weight_keys[6], vec_shape, jnp.float32),
        'ln2_bias': 0.3 * jax.random.normal(weight_keys[7], vec_shape, jnp.float32),
        'w_up': (jax.random.normal(weight_keys[8], (NUM_STAGES, MODEL_DIM, FFN_DIM), jnp.float32) * MODEL_DIM ** -0.5).astype(jnp.bfloat16),
        'b_up': (0.5 * jax.random.normal(weight_keys[9], (NUM_STAGES, FFN_DIM), jnp.float32)).astype(jnp.bfloat16),
        'w_down': (jax.random.normal(weight_keys[10], (NUM_STAGES, FFN_DIM, MODEL_DIM), jnp.float32) * FFN_DIM ** -0.5).astype(jnp.bfloat16),
        'b_down': (0.5 * jax.random.normal(weight_keys[11], vec_shape, jnp.float32)).astype(jnp.bfloat16),
    }


def reference(x_in, g_out, ln1_gain, ln1_bias, w_qkv, b_qkv, w_out, b_out, ln2_gain, ln2_bias, w_up, b_up, w_down, b_down):
    params = (ln1_gain, ln1_bias, w_qkv, b_qkv, w_out, b_out, ln2_gain, ln2_bias, w_up, b_up, w_down, b_down)
    cos_tab, sin_tab = rotary_tables()

    def layer_step(hidden, layer_wts):
        return layer_forward(hidden, layer_wts, cos_tab, sin_tab), None

    def stack_forward(layer_stack, hidden):
        final, unused = lax.scan(jax.checkpoint(layer_step), hidden, layer_stack)
        return final

    def micro_step(grad_acc, micro_pair):
        x_micro, g_micro = micro_pair
        y_micro, pullback = jax.vjp(lambda layer_stack: stack_forward(layer_stack, x_micro), params)
        (grads,) = pullback(g_micro.astype(jnp.bfloat16))
        grad_acc = jax.tree.map(lambda running, update: running + update.astype(jnp.float32), grad_acc, grads)
        return grad_acc, y_micro

    zeros = jax.tree.map(lambda weight: jnp.zeros(weight.shape, jnp.float32), params)
    grad_sum, y_all = lax.scan(micro_step, zeros, (x_in, g_out))
    return (y_all, grad_sum[0], grad_sum[1], grad_sum[2], grad_sum[3], grad_sum[4], grad_sum[5], grad_sum[6], grad_sum[7], grad_sum[8], grad_sum[9], grad_sum[10], grad_sum[11])
```

```python
import functools

import jax
import jax.numpy as jnp
from jax import lax
from jax.experimental import pallas as pl
from jax.experimental.pallas import tpu as pltpu
from jax.sharding import PartitionSpec as P

BF = jnp.bfloat16
F32 = jnp.float32
ROPE_BASE = 10000.0
LN_EPS = 1e-5
HEADS = 3
HEAD = 64
PART = HEADS * HEAD
BLOCK = 256
ROWS = 2 * BLOCK
STAGE_SPECS = (P('pp', None), P('pp', None), P('pp', None, 'tp', None, None), P('pp', 'tp', None, None), P('pp', 'tp', None, None), P('pp', None), P('pp', None), P('pp', None), P('pp', None, 'tp'), P('pp', 'tp'), P('pp', 'tp', None), P('pp', None))
GRAD_SPECS = (P(('dp', 'pp'), None), P(('dp', 'pp'), None), P(('dp', 'pp'), None, 'tp', None, None), P(('dp', 'pp'), 'tp', None, None), P(('dp', 'pp'), 'tp', None, None), P(('dp', 'pp'), None), P(('dp', 'pp'), None), P(('dp', 'pp'), None), P(('dp', 'pp'), None, 'tp'), P(('dp', 'pp'), 'tp'), P(('dp', 'pp'), 'tp', None), P(('dp', 'pp'), None))
MESH_ID = pl.DeviceIdType.MESH


def dot(left, right, left_dim, right_dim):
    return lax.dot_general(left, right, (((left_dim,), (right_dim,)), ((), ())), preferred_element_type=F32)


def normalise(hidden):
    hidden_f = hidden.astype(F32)
    center = hidden_f - jnp.mean(hidden_f, axis=-1, keepdims=True)
    scale = lax.rsqrt(jnp.mean(center * center, axis=-1, keepdims=True) + LN_EPS)
    return center * scale, scale


def turn_matrix(width, transposed):
    row = lax.broadcasted_iota(jnp.int32, (width, width), 0)
    col = lax.broadcasted_iota(jnp.int32, (width, width), 1)
    if transposed:
        row, col = col, row
    dim = col % HEAD
    minus = (dim < 8) & (row == col + 8)
    plus = (dim >= 8) & (dim < 16) & (row == col - 8)
    return (plus.astype(F32) - minus.astype(F32)).astype(BF)


def rotate(values, cos_tab, sin_tab, transposed):
    turned = dot(values, turn_matrix(values.shape[1], transposed), 1, 0)
    return (values.astype(F32) * cos_tab + turned * sin_tab).astype(BF)


def causal_mask(core, block, n_keys):
    row = lax.broadcasted_iota(jnp.int32, (BLOCK, n_keys), 0)
    col = lax.broadcasted_iota(jnp.int32, (BLOCK, n_keys), 1)
    part = col // BLOCK
    starts = (core, 1 - core, 3 - core, 2 + core)
    start = jnp.where(part == 0, starts[0], jnp.where(part == 1, starts[1], jnp.where(part == 2, starts[2], starts[3])))
    mine = core if block == 0 else 3 - core
    return mine * BLOCK + row >= start * BLOCK + (col - part * BLOCK)


def interleave(own, other):
    return jnp.concatenate([own[:BLOCK], other[:BLOCK], own[BLOCK:], other[BLOCK:]], axis=0)


def pick(arr, head):
    return arr[:, head * HEAD:(head + 1) * HEAD]


def attend(query, keys, values, core):
    ctx_rows, lse_rows = [], []
    for block in range(2):
        n_keys = (2, 4)[block] * BLOCK
        mask = causal_mask(core, block, n_keys)
        ctxs, lses = [], []
        for head in range(HEADS):
            q_part = pick(query, head)[block * BLOCK:(block + 1) * BLOCK]
            scores = dot(q_part, pick(keys, head)[:n_keys], 1, 1) * (HEAD ** -0.5)
            scores = jnp.where(mask, scores, -1e30)
            top = jnp.max(scores, axis=-1, keepdims=True)
            expo = jnp.exp(scores - top)
            total = jnp.sum(expo, axis=-1, keepdims=True)
            probs = (expo / total).astype(BF)
            ctxs.append(dot(probs, pick(values, head)[:n_keys], 1, 0).astype(BF))
            lses.append(top + jnp.log(total))
        ctx_rows.append(jnp.concatenate(ctxs, axis=1))
        lse_rows.append(jnp.concatenate(lses, axis=1))
    return jnp.concatenate(ctx_rows, axis=0), jnp.concatenate(lse_rows, axis=0)


def attend_back(query, keys, values, lse, grad_ctx, core):
    dq_rows, dk_sum, dv_sum = [], None, None
    for block in range(2):
        n_keys = (2, 4)[block] * BLOCK
        mask = causal_mask(core, block, n_keys)
        rows = slice(block * BLOCK, (block + 1) * BLOCK)
        dqs, dks, dvs = [], [], []
        for head in range(HEADS):
            q_part = pick(query, head)[rows]
            k_part = pick(keys, head)[:n_keys]
            v_part = pick(values, head)[:n_keys]
            d_part = pick(grad_ctx, head)[rows]
            scores = dot(q_part, k_part, 1, 1) * (HEAD ** -0.5)
            probs = jnp.where(mask, jnp.exp(scores - lse[rows, head:head + 1]), 0.0)
            dprobs = dot(d_part, v_part, 1, 1).astype(BF).astype(F32)
            delta = jnp.sum(probs * dprobs, axis=-1, keepdims=True)
            dscores = (probs * (dprobs - delta) * (HEAD ** -0.5)).astype(BF)
            dqs.append(dot(dscores, k_part, 1, 0))
            dks.append(dot(dscores, q_part, 0, 0))
            dvs.append(dot(probs.astype(BF), d_part, 0, 0))
        dq_rows.append(jnp.concatenate(dqs, axis=1))
        dk_now, dv_now = jnp.concatenate(dks, axis=1), jnp.concatenate(dvs, axis=1)
        if block == 0:
            dk_sum, dv_sum = dk_now, dv_now
        else:
            dk_sum = jnp.concatenate([dk_now[:ROWS] + dk_sum, dk_now[ROWS:]], axis=0)
            dv_sum = jnp.concatenate([dv_now[:ROWS] + dv_sum, dv_now[ROWS:]], axis=0)
    return jnp.concatenate(dq_rows, axis=0), dk_sum, dv_sum


def sum_kernel(n_tp, part_ref, base_ref, shift_ref, out_ref, landed, send_a, recv_a, send_b, recv_b):
    rank = lax.axis_index('tp')
    share = out_ref.shape[0] // n_tp
    barrier = pltpu.get_barrier_semaphore()
    peers = [lax.rem(rank + step, n_tp) for step in range(1, n_tp)]
    for peer in peers:
        pl.semaphore_signal(barrier, inc=1, device_id={'tp': peer}, device_id_type=MESH_ID)
    pl.semaphore_wait(barrier, n_tp - 1)

    def rows_of(index):
        return pl.ds(pl.multiple_of(index * share, share), share)

    scatter = []
    for step, peer in enumerate(peers):
        copy = pltpu.make_async_remote_copy(
            src_ref=part_ref.at[rows_of(peer)], dst_ref=landed.at[step],
            send_sem=send_a.at[step], recv_sem=recv_a.at[step],
            device_id={'tp': peer}, device_id_type=MESH_ID)
        copy.start()
        scatter.append(copy)
    mine = rows_of(rank)
    total = base_ref[mine, :].astype(F32) + shift_ref[...] + part_ref[mine, :].astype(F32)
    for step, copy in enumerate(scatter):
        copy.wait_recv()
        total += landed[step].astype(F32)
    out_ref[mine, :] = total.astype(BF)
    gather = []
    for step, peer in enumerate(peers):
        copy = pltpu.make_async_remote_copy(
            src_ref=out_ref.at[mine], dst_ref=out_ref.at[mine],
            send_sem=send_b.at[step], recv_sem=recv_b.at[step],
            device_id={'tp': peer}, device_id_type=MESH_ID)
        copy.start()
        gather.append(copy)
    for copy in scatter:
        copy.wait_send()
    for copy in gather:
        copy.wait()


def sum_over_tp(part, base, shift, n_tp):
    rows, width = part.shape
    return pl.pallas_call(
        functools.partial(sum_kernel, n_tp),
        out_shape=jax.ShapeDtypeStruct((rows, width), BF),
        in_specs=[pl.BlockSpec(memory_space=pltpu.VMEM)] * 3,
        out_specs=pl.BlockSpec(memory_space=pltpu.VMEM),
        scratch_shapes=[pltpu.VMEM((n_tp - 1, rows // n_tp, width), BF)] + [pltpu.SemaphoreType.DMA((n_tp - 1,))] * 4,
        compiler_params=pltpu.CompilerParams(collective_id=0, has_side_effects=True),
        cost_estimate=pl.CostEstimate(flops=30_000_000_000, bytes_accessed=4_000_000, transcendentals=0),
    )(part, base, shift)


def solution(mesh):
    n_stages = mesh.shape['pp']
    n_tp = mesh.shape['tp']
    swap_core = [(stage, stage ^ 1) for stage in range(n_stages)]

    def device_fn(x_in, g_out, ln1_gain, ln1_bias, w_qkv, b_qkv, w_out, b_out, ln2_gain, ln2_bias, w_up, b_up, w_down, b_down):
        stage = lax.axis_index('pp')
        core = stage % 2
        seq_len, width = x_in.shape[2:]
        ffn = w_up.shape[2]

        def own_tokens(array):
            blocks = lax.dynamic_index_in_dim(array, stage // 2, 0, keepdims=False).reshape(4, BLOCK, width)
            first = lax.dynamic_index_in_dim(blocks, core, 0, keepdims=False)
            second = lax.dynamic_index_in_dim(blocks, 3 - core, 0, keepdims=False)
            return jnp.concatenate([first, second], axis=0).astype(BF)

        hidden = own_tokens(x_in)
        grad = own_tokens(g_out)

        half_rot = HEAD // 8
        inv_freq = ROPE_BASE ** (-(jnp.arange(half_rot, dtype=F32) * 2.0) / (2 * half_rot))
        spot = jnp.concatenate([core * BLOCK + jnp.arange(BLOCK), (3 - core) * BLOCK + jnp.arange(BLOCK)])
        angles = spot.astype(F32)[:, None] * inv_freq[None, :]
        still = jnp.zeros((ROWS, HEAD - 2 * half_rot), F32)
        cos_tab = jnp.tile(jnp.concatenate([jnp.cos(angles), jnp.cos(angles), still + 1.0], axis=1), (1, 2 * HEADS))
        sin_tab = jnp.tile(jnp.concatenate([jnp.sin(angles), jnp.sin(angles), still], axis=1), (1, 2 * HEADS))

        wq_rows = jnp.transpose(w_qkv[0], (2, 1, 3, 0)).reshape(3 * PART, width)
        bundle = jnp.concatenate([wq_rows, w_out[0].reshape(PART, width), w_up[0], w_down[0]], axis=0)
        bias_qkv = jnp.transpose(b_qkv[0], (1, 0, 2)).reshape(3 * PART).astype(F32)
        pad = jnp.zeros((width - 3 * PART,), F32)
        vectors = jnp.stack([ln1_gain[0], ln1_bias[0], ln2_gain[0], ln2_bias[0], b_out[0].astype(F32) + b_down[0].astype(F32), b_up[0].astype(F32), jnp.concatenate([bias_qkv, pad]), jnp.zeros((width,), F32)])

        first_wave = lax.ppermute(bundle, 'pp', [(0, 2), (2, 0)])
        held, first_wave = lax.optimization_barrier((bundle, first_wave))
        second_wave = lax.ppermute(held, 'pp', [(1, 3), (3, 1)])
        partner = lax.ppermute(bundle, 'pp', swap_core)
        first_pass = lax.ppermute(first_wave, 'pp', [(2, 3), (0, 1)])
        second_pass = lax.ppermute(second_wave, 'pp', [(3, 2), (1, 0)])
        all_vectors = lax.all_gather(vectors, 'pp')
        sources = (
            (bundle, partner, first_wave, first_pass),
            (partner, bundle, second_pass, second_wave),
            (first_wave, first_pass, bundle, partner),
            (second_pass, second_wave, partner, bundle),
        )

        def choose(options):
            return jnp.where(stage == 0, options[0], jnp.where(stage == 1, options[1], jnp.where(stage == 2, options[2], options[3])))

        cut = (3 * PART, 4 * PART, 4 * PART + width)
        saved = []
        for layer in range(n_stages):
            weights = choose(sources[layer])
            wq, wo, wu, wd = weights[:cut[0]], weights[cut[0]:cut[1]], weights[cut[1]:cut[2]], weights[cut[2]:]
            vec = all_vectors[layer]
            xhat, scale = normalise(hidden)
            normed_a = (xhat * vec[0] + vec[1]).astype(BF)
            normed_m = (xhat * vec[2] + vec[3]).astype(BF)
            qkv = (dot(normed_a, wq, 1, 1) + vec[6, :3 * PART]).astype(BF)
            turned = rotate(qkv[:, :2 * PART], cos_tab, sin_tab, False)
            query = turned[:, :PART]
            key_value = jnp.concatenate([turned[:, PART:], qkv[:, 2 * PART:]], axis=1)
            other = lax.ppermute(key_value, 'pp', swap_core)
            kv_all = interleave(key_value, other)
            context, lse = attend(query, kv_all[:, :PART], kv_all[:, PART:], core)
            pre_act = dot(normed_m, wu, 1, 0) + vec[5]
            active = jax.nn.gelu(pre_act, approximate=False).astype(BF)
            part = (dot(context, wo, 1, 0) + dot(active, wd, 1, 0)).astype(BF)
            saved.append((hidden, query, kv_all, context, lse, pre_act, weights))
            hidden = sum_over_tp(part, hidden, vec[4:5], n_tp)

        gathered = lax.all_gather(hidden, 'pp').reshape(2, 2, 2, BLOCK, width)
        y_out = jnp.stack([gathered[:, 0, 0], gathered[:, 1, 0], gathered[:, 1, 1], gathered[:, 0, 1]], axis=1).reshape(x_in.shape)

        big_grad = jnp.zeros(bundle.shape, F32)
        small = []
        zero_row = jnp.zeros((1, width), F32)
        for layer in reversed(range(n_stages)):
            hidden, query, kv_all, context, lse, pre_act, weights = saved[layer]
            wq, wo, wu, wd = weights[:cut[0]], weights[cut[0]:cut[1]], weights[cut[1]:cut[2]], weights[cut[2]:]
            vec = all_vectors[layer]
            xhat, scale = normalise(hidden)
            normed_a = (xhat * vec[0] + vec[1]).astype(BF)
            normed_m = (xhat * vec[2] + vec[3]).astype(BF)
            gauss = 0.5 * (1.0 + lax.erf(pre_act * (2.0 ** -0.5)))
            active = (pre_act * gauss).astype(BF)
            slope = gauss + pre_act * jnp.exp(-0.5 * pre_act * pre_act) * 0.3989422804014327
            grad_pre = dot(grad, wd, 1, 1) * slope
            grad_pre_b = grad_pre.astype(BF)
            grad_m = dot(grad_pre_b, wu, 1, 1)
            grad_ctx = dot(grad, wo, 1, 1).astype(BF)
            dq, dk_all, dv_all = attend_back(query, kv_all[:, :PART], kv_all[:, PART:], lse, grad_ctx, core)
            dkv = jnp.concatenate([dk_all, dv_all], axis=1).reshape(4, BLOCK, 2 * PART)
            back = lax.ppermute(jnp.concatenate([dkv[1], dkv[3]], axis=0), 'pp', swap_core)
            dkv = (jnp.concatenate([dkv[0], dkv[2]], axis=0) + back).astype(BF)
            dqk = rotate(jnp.concatenate([dq.astype(BF), dkv[:, :PART]], axis=1), cos_tab, sin_tab, True)
            grad_qkv = jnp.concatenate([dqk, dkv[:, PART:]], axis=1)
            grad_a = dot(grad_qkv, wq, 1, 0)
            small.append(jnp.stack([
                jnp.sum(grad_a * xhat, axis=0), jnp.sum(grad_a, axis=0), jnp.sum(grad_m * xhat, axis=0), jnp.sum(grad_m, axis=0),
                jnp.sum(grad.astype(F32), axis=0), jnp.sum(grad_pre, axis=0),
                jnp.concatenate([jnp.sum(grad_qkv.astype(F32), axis=0), pad]), pad_row(width)]))
            grad_big = jnp.concatenate([dot(grad_qkv, normed_a, 0, 0), dot(context, grad, 0, 0), dot(normed_m, grad_pre_b, 0, 0), dot(active, grad, 0, 0)], axis=0)
            if layer:
                grad_x = grad_a * vec[0] + grad_m * vec[2]
                branch = scale * (grad_x - jnp.mean(grad_x, axis=-1, keepdims=True) - xhat * jnp.mean(grad_x * xhat, axis=-1, keepdims=True))
                grad = sum_over_tp(branch.astype(BF), grad, zero_row, n_tp)
            near = lax.ppermute(grad_big.astype(BF), 'pp', [(layer ^ 1, layer), (layer ^ 3, layer ^ 2)])
            grad_big = grad_big + near.astype(F32)
            far = lax.ppermute(grad_big.astype(BF), 'pp', [(layer ^ 2, layer)])
            big_grad = jnp.where(stage == layer, grad_big + far.astype(F32), big_grad)

        small = lax.psum(jnp.stack(small[::-1]), 'pp')
        small = lax.dynamic_index_in_dim(small, stage, 0, keepdims=False)
        norms = lax.psum(small[:4], 'tp')
        grad_qkv = jnp.transpose(big_grad[:cut[0]].reshape(3, HEADS, HEAD, width), (3, 1, 0, 2))
        grads = (
            norms[0], norms[1], grad_qkv, jnp.transpose(small[6, :3 * PART].reshape(3, HEADS, HEAD), (1, 0, 2)),
            big_grad[cut[0]:cut[1]].reshape(HEADS, HEAD, width), small[4], norms[2], norms[3],
            big_grad[cut[1]:cut[2]], small[5], big_grad[cut[2]:], small[4])
        return tuple([y_out] + [item[None] for item in grads])

    return jax.shard_map(device_fn, mesh=mesh, in_specs=(P('dp'), P('dp')) + STAGE_SPECS, out_specs=(P('dp'),) + GRAD_SPECS, check_vma=False)


def pad_row(width):
    return jnp.zeros((width,), F32)
```

```python
import functools

import jax
import jax.numpy as jnp
from jax import lax
from jax.experimental import pallas as pl
from jax.experimental.pallas import tpu as pltpu
from jax.sharding import PartitionSpec as P

BF = jnp.bfloat16
F32 = jnp.float32
ROPE_BASE = 10000.0
LN_EPS = 1e-5
HEADS = 3
HEAD = 64
PART = HEADS * HEAD
BLOCK = 256
ROWS = 2 * BLOCK
STAGE_SPECS = (P('pp', None), P('pp', None), P('pp', None, 'tp', None, None), P('pp', 'tp', None, None), P('pp', 'tp', None, None), P('pp', None), P('pp', None), P('pp', None), P('pp', None, 'tp'), P('pp', 'tp'), P('pp', 'tp', None), P('pp', None))
GRAD_SPECS = (P(('dp', 'pp'), None), P(('dp', 'pp'), None), P(('dp', 'pp'), None, 'tp', None, None), P(('dp', 'pp'), 'tp', None, None), P(('dp', 'pp'), 'tp', None, None), P(('dp', 'pp'), None), P(('dp', 'pp'), None), P(('dp', 'pp'), None), P(('dp', 'pp'), None, 'tp'), P(('dp', 'pp'), 'tp'), P(('dp', 'pp'), 'tp', None), P(('dp', 'pp'), None))
MESH_ID = pl.DeviceIdType.MESH


def tie(*values):
    return lax.optimization_barrier(values)


def dot(left, right, left_dim, right_dim):
    return lax.dot_general(left, right, (((left_dim,), (right_dim,)), ((), ())), preferred_element_type=F32)


def normalise(hidden):
    hidden_f = hidden.astype(F32)
    center = hidden_f - jnp.mean(hidden_f, axis=-1, keepdims=True)
    scale = lax.rsqrt(jnp.mean(center * center, axis=-1, keepdims=True) + LN_EPS)
    return center * scale, scale


def turn_matrix(width, transposed):
    row = lax.broadcasted_iota(jnp.int32, (width, width), 0)
    col = lax.broadcasted_iota(jnp.int32, (width, width), 1)
    if transposed:
        row, col = col, row
    dim = col % HEAD
    minus = (dim < 8) & (row == col + 8)
    plus = (dim >= 8) & (dim < 16) & (row == col - 8)
    return (plus.astype(F32) - minus.astype(F32)).astype(BF)


def rotate(values, cos_tab, sin_tab, transposed):
    turned = dot(values, turn_matrix(values.shape[1], transposed), 1, 0)
    return (values.astype(F32) * cos_tab + turned * sin_tab).astype(BF)


def causal_mask(core, block, n_keys):
    row = lax.broadcasted_iota(jnp.int32, (BLOCK, n_keys), 0)
    col = lax.broadcasted_iota(jnp.int32, (BLOCK, n_keys), 1)
    part = col // BLOCK
    starts = (core, 1 - core, 3 - core, 2 + core)
    start = jnp.where(part == 0, starts[0], jnp.where(part == 1, starts[1], jnp.where(part == 2, starts[2], starts[3])))
    mine = core if block == 0 else 3 - core
    return mine * BLOCK + row >= start * BLOCK + (col - part * BLOCK)


def interleave(own, other):
    return jnp.concatenate([own[:BLOCK], other[:BLOCK], own[BLOCK:], other[BLOCK:]], axis=0)


def pick(arr, head):
    return arr[:, head * HEAD:(head + 1) * HEAD]


def attend(query, keys, values, core):
    ctx_rows, lse_rows = [], []
    for block in range(2):
        n_keys = (2, 4)[block] * BLOCK
        mask = causal_mask(core, block, n_keys)
        ctxs, lses = [], []
        for head in range(HEADS):
            q_part = pick(query, head)[block * BLOCK:(block + 1) * BLOCK]
            scores = dot(q_part, pick(keys, head)[:n_keys], 1, 1) * (HEAD ** -0.5)
            scores = jnp.where(mask, scores, -1e30)
            top = jnp.max(scores, axis=-1, keepdims=True)
            expo = jnp.exp(scores - top)
            total = jnp.sum(expo, axis=-1, keepdims=True)
            probs = (expo / total).astype(BF)
            ctxs.append(dot(probs, pick(values, head)[:n_keys], 1, 0).astype(BF))
            lses.append(top + jnp.log(total))
        ctx_rows.append(jnp.concatenate(ctxs, axis=1))
        lse_rows.append(jnp.concatenate(lses, axis=1))
    return jnp.concatenate(ctx_rows, axis=0), jnp.concatenate(lse_rows, axis=0)


def attend_back(query, keys, values, lse, grad_ctx, core, midway=None):
    dq_rows, dk_sum, dv_sum = [], None, None
    for block in range(2):
        n_keys = (2, 4)[block] * BLOCK
        mask = causal_mask(core, block, n_keys)
        rows = slice(block * BLOCK, (block + 1) * BLOCK)
        dqs, dks, dvs = [], [], []
        for head in range(HEADS):
            q_part = pick(query, head)[rows]
            k_part = pick(keys, head)[:n_keys]
            v_part = pick(values, head)[:n_keys]
            d_part = pick(grad_ctx, head)[rows]
            scores = dot(q_part, k_part, 1, 1) * (HEAD ** -0.5)
            probs = jnp.where(mask, jnp.exp(scores - lse[rows, head:head + 1]), 0.0)
            dprobs = dot(d_part, v_part, 1, 1).astype(BF).astype(F32)
            delta = jnp.sum(probs * dprobs, axis=-1, keepdims=True)
            dscores = (probs * (dprobs - delta) * (HEAD ** -0.5)).astype(BF)
            dqs.append(dot(dscores, k_part, 1, 0))
            dks.append(dot(dscores, q_part, 0, 0))
            dvs.append(dot(probs.astype(BF), d_part, 0, 0))
        dq_rows.append(jnp.concatenate(dqs, axis=1))
        dk_now, dv_now = jnp.concatenate(dks, axis=1), jnp.concatenate(dvs, axis=1)
        if block == 0:
            dk_sum, dv_sum = dk_now, dv_now
            if midway is not None:
                query, dk_sum = midway(query, dk_sum)
        else:
            dk_sum = jnp.concatenate([dk_now[:ROWS] + dk_sum, dk_now[ROWS:]], axis=0)
            dv_sum = jnp.concatenate([dv_now[:ROWS] + dv_sum, dv_now[ROWS:]], axis=0)
    return jnp.concatenate(dq_rows, axis=0), dk_sum, dv_sum


def line_sum_kernel(n_tp, n_chunks, pieces, n_lhs, n_rhs, *refs):
    part_ref, base_ref, shift_ref = refs[:3]
    lhs = refs[3:3 + n_lhs]
    rhs = refs[3 + n_lhs:3 + n_lhs + n_rhs]
    rest = refs[3 + n_lhs + n_rhs:]
    if pieces:
        out_ref, prod_ref, prod_b_ref = rest[:3]
        rest = rest[3:]
    else:
        out_ref = rest[0]
        rest = rest[1:]
    inbox, half, across, send_p, recv_p, send_s, recv_s, send_f, recv_f = rest
    rank = lax.axis_index('tp')
    is_inner = lax.rem((rank + 1) // 2, 2)
    near = rank + 1 - 2 * lax.rem(rank, 2)
    mirror = n_tp - 1 - rank
    size = out_ref.shape[0] // n_chunks
    barrier = pltpu.get_barrier_semaphore()
    pl.semaphore_signal(barrier, inc=1, device_id={'tp': near}, device_id_type=MESH_ID)

    @pl.when(is_inner == 1)
    def greet():
        pl.semaphore_signal(barrier, inc=1, device_id={'tp': mirror}, device_id_type=MESH_ID)

    pl.semaphore_wait(barrier, 1 + is_inner)

    def span(chunk):
        return pl.ds(chunk * size, size)

    def part_copy(chunk):
        return pltpu.make_async_remote_copy(
            src_ref=part_ref.at[span(chunk)], dst_ref=inbox.at[span(chunk)], send_sem=send_p.at[chunk],
            recv_sem=recv_p.at[chunk], device_id={'tp': near}, device_id_type=MESH_ID)

    def half_copy(chunk):
        return pltpu.make_async_remote_copy(
            src_ref=half.at[span(chunk)], dst_ref=across.at[span(chunk)], send_sem=send_s.at[chunk],
            recv_sem=recv_s.at[chunk], device_id={'tp': mirror}, device_id_type=MESH_ID)

    def final_copy(chunk):
        return pltpu.make_async_remote_copy(
            src_ref=out_ref.at[span(chunk)], dst_ref=out_ref.at[span(chunk)], send_sem=send_f.at[chunk],
            recv_sem=recv_f.at[chunk], device_id={'tp': near}, device_id_type=MESH_ID)

    @pl.when(is_inner == 0)
    def outer_start():
        for chunk in range(n_chunks):
            part_copy(chunk).start()

    def finish(chunk):
        rows = span(chunk)
        half_copy(chunk).wait_recv()
        both = half[rows, :].astype(F32) + across[rows, :].astype(F32)
        out_ref[rows, :] = (base_ref[rows, :].astype(F32) + shift_ref[...] + both).astype(BF)
        final_copy(chunk).start()

    for chunk in range(n_chunks):
        @pl.when(is_inner == 1)
        def merge():
            rows = span(chunk)
            part_copy(chunk).wait_recv()
            half[rows, :] = (part_ref[rows, :].astype(F32) + inbox[rows, :].astype(F32)).astype(BF)
            half_copy(chunk).start()

        for left, first, count, right, row in pieces[chunk::n_chunks]:
            value = dot(lhs[left][:, first:first + count], rhs[right][...], 0, 0)
            prod_ref[row:row + count, :] = value
            prod_b_ref[row:row + count, :] = value.astype(BF)

        if chunk:
            @pl.when(is_inner == 1)
            def close():
                finish(chunk - 1)

    @pl.when(is_inner == 1)
    def inner_end():
        finish(n_chunks - 1)
        for chunk in range(n_chunks):
            half_copy(chunk).wait_send()
            final_copy(chunk).wait_send()

    @pl.when(is_inner == 0)
    def outer_end():
        for chunk in range(n_chunks):
            final_copy(chunk).wait_recv()
            part_copy(chunk).wait_send()


def sum_over_tp(part, base, shift, n_tp, lhs=(), rhs=(), pairs=()):
    n_chunks = 8
    rows, width = part.shape
    pieces, row = [], 0
    for left, right in pairs:
        cols = lhs[left].shape[1]
        first = 0
        while first < cols:
            count = cols - first if cols - first < 384 else 256
            pieces.append((left, first, count, right, row))
            first, row = first + count, row + count
    out_shape = [jax.ShapeDtypeStruct((rows, width), BF)]
    if pieces:
        out_shape += [jax.ShapeDtypeStruct((row, width), F32), jax.ShapeDtypeStruct((row, width), BF)]
    block = pl.BlockSpec(memory_space=pltpu.VMEM)
    return pl.pallas_call(
        functools.partial(line_sum_kernel, n_tp, n_chunks, tuple(pieces), len(lhs), len(rhs)),
        out_shape=tuple(out_shape),
        in_specs=[block] * (3 + len(lhs) + len(rhs)),
        out_specs=tuple([block] * len(out_shape)),
        scratch_shapes=[pltpu.VMEM((rows, width), BF)] * 3 + [pltpu.SemaphoreType.DMA((n_chunks,))] * 6,
        compiler_params=pltpu.CompilerParams(collective_id=1 if pieces else 0, has_side_effects=True),
        cost_estimate=pl.CostEstimate(flops=25_000_000_000, bytes_accessed=4_000_000, transcendentals=0),
    )(part, base, shift, *lhs, *rhs)


def small_kernel(n_pp, n_tp, n_norm, rows_ref, out_ref, box, stage_sum, norm_box, send_a, recv_a, send_b, recv_b):
    stage, rank = lax.axis_index('pp'), lax.axis_index('tp')
    barrier = pltpu.get_barrier_semaphore()
    for step in range(1, n_pp):
        pl.semaphore_signal(barrier, inc=1, device_id={'pp': lax.rem(stage + step, n_pp)}, device_id_type=MESH_ID)
    for step in range(1, n_tp):
        pl.semaphore_signal(barrier, inc=1, device_id={'tp': lax.rem(rank + step, n_tp)}, device_id_type=MESH_ID)
    pl.semaphore_wait(barrier, n_pp + n_tp - 2)
    sends = []
    for step in range(1, n_pp):
        peer = lax.rem(stage + step, n_pp)
        copy = pltpu.make_async_remote_copy(
            src_ref=rows_ref.at[peer], dst_ref=box.at[step - 1], send_sem=send_a.at[step - 1],
            recv_sem=recv_a.at[step - 1], device_id={'pp': peer}, device_id_type=MESH_ID)
        copy.start()
        sends.append(copy)
    total = rows_ref[stage]
    for step, copy in enumerate(sends):
        copy.wait_recv()
        total += box[step]
    stage_sum[...] = total
    norm_box[rank] = total[:n_norm]
    shares = []
    for step in range(1, n_tp):
        copy = pltpu.make_async_remote_copy(
            src_ref=stage_sum.at[pl.ds(0, n_norm)], dst_ref=norm_box.at[rank], send_sem=send_b.at[step - 1],
            recv_sem=recv_b.at[step - 1], device_id={'tp': lax.rem(rank + step, n_tp)}, device_id_type=MESH_ID)
        copy.start()
        shares.append(copy)
    for copy in shares:
        copy.wait()
    norms = norm_box[0]
    for index in range(1, n_tp):
        norms += norm_box[index]
    out_ref[:n_norm, :] = norms
    out_ref[n_norm:, :] = total[n_norm:]
    for copy in sends:
        copy.wait_send()


def sum_small(rows, n_tp):
    n_pp, count, width = rows.shape
    n_norm = count // 2
    return pl.pallas_call(
        functools.partial(small_kernel, n_pp, n_tp, n_norm),
        out_shape=jax.ShapeDtypeStruct((count, width), F32),
        in_specs=[pl.BlockSpec(memory_space=pltpu.VMEM)],
        out_specs=pl.BlockSpec(memory_space=pltpu.VMEM),
        scratch_shapes=[pltpu.VMEM((n_pp - 1, count, width), F32), pltpu.VMEM((count, width), F32), pltpu.VMEM((n_tp, n_norm, width), F32),
                        pltpu.SemaphoreType.DMA((n_pp - 1,)), pltpu.SemaphoreType.DMA((n_pp - 1,)), pltpu.SemaphoreType.DMA((n_tp - 1,)), pltpu.SemaphoreType.DMA((n_tp - 1,))],
        compiler_params=pltpu.CompilerParams(collective_id=2, has_side_effects=True),
        cost_estimate=pl.CostEstimate(flops=8_000_000_000, bytes_accessed=200_000, transcendentals=0),
    )(rows)


def solution(mesh):
    n_stages = mesh.shape['pp']
    n_tp = mesh.shape['tp']
    swap_core = [(stage, stage ^ 1) for stage in range(n_stages)]

    def device_fn(x_in, g_out, ln1_gain, ln1_bias, w_qkv, b_qkv, w_out, b_out, ln2_gain, ln2_bias, w_up, b_up, w_down, b_down):
        stage = lax.axis_index('pp')
        core = stage % 2
        seq_len, width = x_in.shape[2:]
        ffn = w_up.shape[2]

        def own_tokens(array):
            blocks = lax.dynamic_index_in_dim(array, stage // 2, 0, keepdims=False).reshape(4, BLOCK, width)
            first = lax.dynamic_index_in_dim(blocks, core, 0, keepdims=False)
            second = lax.dynamic_index_in_dim(blocks, 3 - core, 0, keepdims=False)
            return jnp.concatenate([first, second], axis=0).astype(BF)

        hidden = own_tokens(x_in)
        grad = own_tokens(g_out)

        half_rot = HEAD // 8
        inv_freq = ROPE_BASE ** (-(jnp.arange(half_rot, dtype=F32) * 2.0) / (2 * half_rot))
        spot = jnp.concatenate([core * BLOCK + jnp.arange(BLOCK), (3 - core) * BLOCK + jnp.arange(BLOCK)])
        angles = spot.astype(F32)[:, None] * inv_freq[None, :]
        still = jnp.zeros((ROWS, HEAD - 2 * half_rot), F32)
        cos_tab = jnp.tile(jnp.concatenate([jnp.cos(angles), jnp.cos(angles), still + 1.0], axis=1), (1, 2 * HEADS))
        sin_tab = jnp.tile(jnp.concatenate([jnp.sin(angles), jnp.sin(angles), still], axis=1), (1, 2 * HEADS))

        wq_rows = jnp.transpose(w_qkv[0], (2, 1, 3, 0)).reshape(3 * PART, width)
        bundle = jnp.concatenate([wq_rows, w_out[0].reshape(PART, width), w_up[0], w_down[0]], axis=0)
        bias_qkv = jnp.transpose(b_qkv[0], (1, 0, 2)).reshape(3 * PART).astype(F32)
        pad = jnp.zeros((width - 3 * PART,), F32)
        vectors = jnp.stack([ln1_gain[0], ln1_bias[0], ln2_gain[0], ln2_bias[0], b_out[0].astype(F32) + b_down[0].astype(F32), b_up[0].astype(F32), jnp.concatenate([bias_qkv, pad]), jnp.zeros((width,), F32)])

        n_att = 4 * PART
        pair_a, pair_b = [(0, 2), (2, 0)], [(1, 3), (3, 1)]
        own = (bundle[:n_att], bundle[n_att:])
        wave_a = lax.ppermute(own[0], 'pp', pair_a)
        later, wave_a = tie(own[1], wave_a)
        wave_m = lax.ppermute(later, 'pp', pair_a)
        later, wave_m = tie(bundle, wave_m)
        second_wave = lax.ppermute(later, 'pp', pair_b)
        partner = lax.ppermute(bundle, 'pp', swap_core)
        partner = (partner[:n_att], partner[n_att:])
        first_wave = (wave_a, wave_m)
        first_pass = tuple(lax.ppermute(item, 'pp', [(2, 3), (0, 1)]) for item in first_wave)
        all_vectors = lax.all_gather(vectors, 'pp')
        sources = {0: (own, partner, first_wave, first_pass), 2: (first_wave, first_pass, own, partner)}

        def choose(options):
            return jnp.where(stage == 0, options[0], jnp.where(stage == 1, options[1], jnp.where(stage == 2, options[2], options[3])))

        saved = []
        for layer in range(n_stages):
            w_att = choose([item[0] for item in sources[layer]])
            w_mlp = choose([item[1] for item in sources[layer]])
            weights = (w_att[:3 * PART], w_att[3 * PART:], w_mlp[:width], w_mlp[width:])
            wq, wo, wu, wd = weights
            vec = all_vectors[layer]
            xhat, scale = normalise(hidden)
            normed_a = (xhat * vec[0] + vec[1]).astype(BF)
            normed_m = (xhat * vec[2] + vec[3]).astype(BF)
            qkv = (dot(normed_a, wq, 1, 1) + vec[6, :3 * PART]).astype(BF)
            turned = rotate(qkv[:, :2 * PART], cos_tab, sin_tab, False)
            query = turned[:, :PART]
            key_value = jnp.concatenate([turned[:, PART:], qkv[:, 2 * PART:]], axis=1)
            other = lax.ppermute(key_value, 'pp', swap_core)
            kv_all = interleave(key_value, other)
            context, lse = attend(query, kv_all[:, :PART], kv_all[:, PART:], core)
            pre_act = dot(normed_m, wu, 1, 0) + vec[5]
            active = jax.nn.gelu(pre_act, approximate=False).astype(BF)
            part = (dot(context, wo, 1, 0) + dot(active, wd, 1, 0)).astype(BF)
            saved.append((hidden, query, kv_all, context, lse, pre_act, weights))
            if layer == n_stages - 1:
                summed = lax.psum(part, 'tp')
                final = (hidden.astype(F32) + vec[4:5] + summed.astype(F32)).astype(BF)
                break
            (hidden,) = sum_over_tp(part, hidden, vec[4:5], n_tp)
            if layer == 0:
                hidden, second_wave = tie(hidden, second_wave)
                second_pass = lax.ppermute(second_wave, 'pp', [(3, 2), (1, 0)])
                second_wave = (second_wave[:n_att], second_wave[n_att:])
                second_pass = (second_pass[:n_att], second_pass[n_att:])
                sources[1] = (partner, own, second_pass, second_wave)
                sources[3] = (second_pass, second_wave, partner, own)

        gathered = lax.all_gather(final, 'pp').reshape(2, 2, 2, BLOCK, width)
        y_out = jnp.stack([gathered[:, 0, 0], gathered[:, 1, 0], gathered[:, 1, 1], gathered[:, 0, 1]], axis=1).reshape(x_in.shape)

        def send_near(prod_b, layer):
            return lax.ppermute(prod_b, 'pp', [(layer ^ 1, layer), (layer ^ 3, layer ^ 2)])

        def send_far(prod, layer):
            return lax.ppermute(prod, 'pp', [(layer ^ 2, layer)])

        def add_near(prod, near):
            return (prod + near.astype(F32)).astype(BF)

        small = {}
        prod, prod_b, near, far = {}, {}, {}, {}
        zero_row = jnp.zeros((1, width), F32)
        for layer in reversed(range(n_stages)):
            hidden, query, kv_all, context, lse, pre_act, (wq, wo, wu, wd) = saved[layer]
            vec = all_vectors[layer]
            xhat, scale = normalise(hidden)
            normed_a = (xhat * vec[0] + vec[1]).astype(BF)
            normed_m = (xhat * vec[2] + vec[3]).astype(BF)
            gauss = 0.5 * (1.0 + lax.erf(pre_act * (2.0 ** -0.5)))
            active = (pre_act * gauss).astype(BF)
            slope = gauss + pre_act * jnp.exp(-0.5 * pre_act * pre_act) * 0.3989422804014327
            grad_pre = dot(grad, wd, 1, 1) * slope
            grad_pre_b = grad_pre.astype(BF)
            grad_m = dot(grad_pre_b, wu, 1, 1)
            grad_ctx = dot(grad, wo, 1, 1).astype(BF)
            if layer < 2:
                prod[layer, 'm'] = jnp.concatenate([dot(normed_m, grad_pre_b, 0, 0), dot(active, grad, 0, 0)], axis=0)
                prod_b[layer, 'm'] = prod[layer, 'm'].astype(BF)
            midway = None
            if layer == 1:
                grad_ctx, far[3], near[2], prod_b[1, 'm'] = tie(grad_ctx, far[3], near[2], prod_b[1, 'm'])
                half_sum = add_near(prod[2], near[2])
                near[1, 'm'] = send_near(prod_b[1, 'm'], 1)
            if layer == 0:
                grad_ctx, far[2], near[1, 'a'], far[1, 'm'], prod_b[0, 'm'] = tie(grad_ctx, far[2], near[1, 'a'], far[1, 'm'], prod_b[0, 'm'])
                far[1, 'a'] = send_far(add_near(prod[1, 'a'], near[1, 'a']), 1)
                near[0, 'm'] = send_near(prod_b[0, 'm'], 0)

                def midway(query, dk_sum):
                    query, dk_sum, near[0, 'm'] = tie(query, dk_sum, near[0, 'm'])
                    far[0, 'm'] = send_far(add_near(prod[0, 'm'], near[0, 'm']), 0)
                    return query, dk_sum
            dq, dk_all, dv_all = attend_back(query, kv_all[:, :PART], kv_all[:, PART:], lse, grad_ctx, core, midway)
            dkv = jnp.concatenate([dk_all, dv_all], axis=1).reshape(4, BLOCK, 2 * PART)
            back = lax.ppermute(jnp.concatenate([dkv[1], dkv[3]], axis=0), 'pp', swap_core)
            dkv = (jnp.concatenate([dkv[0], dkv[2]], axis=0) + back).astype(BF)
            dqk = rotate(jnp.concatenate([dq.astype(BF), dkv[:, :PART]], axis=1), cos_tab, sin_tab, True)
            grad_qkv = jnp.concatenate([dqk, dkv[:, PART:]], axis=1)
            grad_a = dot(grad_qkv, wq, 1, 0)
            small[layer] = jnp.stack([
                jnp.sum(grad_a * xhat, axis=0), jnp.sum(grad_a, axis=0), jnp.sum(grad_m * xhat, axis=0), jnp.sum(grad_m, axis=0),
                jnp.sum(grad.astype(F32), axis=0), jnp.sum(grad_pre, axis=0),
                jnp.concatenate([jnp.sum(grad_qkv.astype(F32), axis=0), pad]), pad_row(width)])
            if layer == 0:
                prod[0, 'a'] = jnp.concatenate([dot(grad_qkv, normed_a, 0, 0), dot(context, grad, 0, 0)], axis=0)
                near[0, 'a'] = send_near(prod[0, 'a'].astype(BF), 0)
                far[0, 'a'] = send_far(add_near(prod[0, 'a'], near[0, 'a']), 0)
                break
            grad_x = grad_a * vec[0] + grad_m * vec[2]
            branch = scale * (grad_x - jnp.mean(grad_x, axis=-1, keepdims=True) - xhat * jnp.mean(grad_x * xhat, axis=-1, keepdims=True))
            branch = branch.astype(BF)
            if layer == 2:
                half_sum = add_near(prod[3], near[3])
                branch, half_sum = tie(branch, half_sum)
                far[3] = send_far(half_sum, 3)
            if layer == 1:
                half_sum, quarter_sum = tie(half_sum, add_near(prod[1, 'm'], near[1, 'm']))
                branch, half_sum, quarter_sum = tie(branch, half_sum, quarter_sum)
                far[2] = send_far(half_sum, 2)
                far[1, 'm'] = send_far(quarter_sum, 1)
            if layer > 1:
                grad, prod[layer], prod_b[layer] = sum_over_tp(
                    branch, grad, zero_row, n_tp, (grad_qkv, context, normed_m, active), (normed_a, grad, grad_pre_b),
                    ((0, 0), (1, 1), (2, 2), (3, 1)))
                near[layer] = send_near(prod_b[layer], layer)
            else:
                grad, prod[1, 'a'], prod_b[1, 'a'] = sum_over_tp(
                    branch, grad, zero_row, n_tp, (grad_qkv, context), (normed_a, grad), ((0, 0), (1, 1)))
                near[1, 'a'] = send_near(prod_b[1, 'a'], 1)

        def total_of(key):
            return prod[key] + near[key].astype(F32) + far[key].astype(F32)

        def collect(kind, rows):
            upper = jnp.where(stage == 3, total_of(3)[rows], total_of(2)[rows])
            upper = jnp.where(stage == 1, total_of((1, kind)), upper)
            (upper,) = lax.optimization_barrier((upper,))
            return jnp.where(stage == 0, total_of((0, kind)), upper)

        small = sum_small(jnp.stack([small[layer] for layer in range(n_stages)]), n_tp)
        norms = small
        grad_att, grad_mlp = collect('a', slice(0, n_att)), collect('m', slice(n_att, None))
        grad_qkv = jnp.transpose(grad_att[:3 * PART].reshape(3, HEADS, HEAD, width), (3, 1, 0, 2))
        grads = (
            norms[0], norms[1], grad_qkv, jnp.transpose(small[6, :3 * PART].reshape(3, HEADS, HEAD), (1, 0, 2)),
            grad_att[3 * PART:].reshape(HEADS, HEAD, width), small[4], norms[2], norms[3],
            grad_mlp[:width], small[5], grad_mlp[width:], small[4])
        return tuple([y_out] + [item[None] for item in grads])

    return jax.shard_map(device_fn, mesh=mesh, in_specs=(P('dp'), P('dp')) + STAGE_SPECS, out_specs=(P('dp'),) + GRAD_SPECS, check_vma=False)


def pad_row(width):
    return jnp.zeros((width,), F32)
```

```python
import functools

import jax
import jax.numpy as jnp
from jax import lax
from jax.experimental import pallas as pl
from jax.experimental.pallas import tpu as pltpu
from jax.sharding import PartitionSpec as P

BF = jnp.bfloat16
F32 = jnp.float32
ROPE_BASE = 10000.0
LN_EPS = 1e-5
HEADS = 3
HEAD = 64
PART = HEADS * HEAD
BLOCK = 256
ROWS = 2 * BLOCK
STAGE_SPECS = (P('pp', None), P('pp', None), P('pp', None, 'tp', None, None), P('pp', 'tp', None, None), P('pp', 'tp', None, None), P('pp', None), P('pp', None), P('pp', None), P('pp', None, 'tp'), P('pp', 'tp'), P('pp', 'tp', None), P('pp', None))
GRAD_SPECS = (P(('dp', 'pp'), None), P(('dp', 'pp'), None), P(('dp', 'pp'), None, 'tp', None, None), P(('dp', 'pp'), 'tp', None, None), P(('dp', 'pp'), 'tp', None, None), P(('dp', 'pp'), None), P(('dp', 'pp'), None), P(('dp', 'pp'), None), P(('dp', 'pp'), None, 'tp'), P(('dp', 'pp'), 'tp'), P(('dp', 'pp'), 'tp', None), P(('dp', 'pp'), None))
CHUNKS = 8
LIMIT = 60 * 2 ** 20
MESH_ID = pl.DeviceIdType.MESH


def tie(*values):
    return lax.optimization_barrier(values)


def dot(left, right, left_dim, right_dim):
    return lax.dot_general(left, right, (((left_dim,), (right_dim,)), ((), ())), preferred_element_type=F32)


def normalise(hidden):
    hidden_f = hidden.astype(F32)
    center = hidden_f - jnp.mean(hidden_f, axis=-1, keepdims=True)
    scale = lax.rsqrt(jnp.mean(center * center, axis=-1, keepdims=True) + LN_EPS)
    return center * scale, scale


def turn_matrix(width, transposed):
    row = lax.broadcasted_iota(jnp.int32, (width, width), 0)
    col = lax.broadcasted_iota(jnp.int32, (width, width), 1)
    if transposed:
        row, col = col, row
    dim = col % HEAD
    minus = (dim < 8) & (row == col + 8)
    plus = (dim >= 8) & (dim < 16) & (row == col - 8)
    return (plus.astype(F32) - minus.astype(F32)).astype(BF)


def rotate_head(values, cos_tab, sin_tab, transposed):
    turned = dot(values, turn_matrix(HEAD, transposed), 1, 0)
    return (values.astype(F32) * cos_tab + turned * sin_tab).astype(BF)


def block_rows(block):
    return slice(block * BLOCK, (block + 1) * BLOCK)


def pick_weights(stage, options, first, count, scratch, sem):
    for index, option in enumerate(options):
        @pl.when(stage == index)
        def fetch():
            pltpu.make_async_copy(option.at[pl.ds(first, count)], scratch, sem).start()

    return pltpu.make_async_copy(options[0].at[pl.ds(first, count)], scratch, sem).wait


def meet(n_tp, with_sum, with_core):
    rank, stage = lax.axis_index('tp'), lax.axis_index('pp')
    barrier = pltpu.get_barrier_semaphore()
    count = 0
    if with_core:
        pl.semaphore_signal(barrier, inc=1, device_id={'pp': stage + 1 - 2 * lax.rem(stage, 2)}, device_id_type=MESH_ID)
        count = 1
    if with_sum:
        is_inner = lax.rem((rank + 1) // 2, 2)
        near = rank + 1 - 2 * lax.rem(rank, 2)
        pl.semaphore_signal(barrier, inc=1, device_id={'tp': near}, device_id_type=MESH_ID)

        @pl.when(is_inner == 1)
        def greet():
            pl.semaphore_signal(barrier, inc=1, device_id={'tp': n_tp - 1 - rank}, device_id_type=MESH_ID)

        count = count + 1 + is_inner
    pl.semaphore_wait(barrier, count)


class LineSum:
    def __init__(self, n_tp, part, base, out, inbox, half, across, sems):
        self.part, self.base, self.out, self.inbox, self.half, self.across, self.sems = part, base, out, inbox, half, across, sems
        rank = lax.axis_index('tp')
        self.is_inner = lax.rem((rank + 1) // 2, 2)
        self.near = rank + 1 - 2 * lax.rem(rank, 2)
        self.mirror = n_tp - 1 - rank
        self.n_chunks = CHUNKS
        self.size = out.shape[0] // CHUNKS

    def span(self, chunk):
        return pl.ds(chunk * self.size, self.size)

    def copy(self, kind, chunk):
        source, target, device = ((self.part, self.inbox, self.near), (self.half, self.across, self.mirror), (self.out, self.out, self.near))[kind]
        return pltpu.make_async_remote_copy(
            src_ref=source.at[self.span(chunk)], dst_ref=target.at[self.span(chunk)], send_sem=self.sems[2 * kind].at[chunk],
            recv_sem=self.sems[2 * kind + 1].at[chunk], device_id={'tp': device}, device_id_type=MESH_ID)

    def offer(self, chunks):
        @pl.when(self.is_inner == 0)
        def start():
            for chunk in chunks:
                self.copy(0, chunk).start()

    def finish(self, chunk):
        rows = self.span(chunk)
        self.copy(1, chunk).wait_recv()
        both = self.half[rows, :].astype(F32) + self.across[rows, :].astype(F32)
        self.out[rows, :] = (self.base(rows) + both).astype(BF)
        self.copy(2, chunk).start()

    def step(self, chunk):
        @pl.when(self.is_inner == 1)
        def merge():
            rows = self.span(chunk)
            self.copy(0, chunk).wait_recv()
            self.half[rows, :] = (self.part[rows, :].astype(F32) + self.inbox[rows, :].astype(F32)).astype(BF)
            self.copy(1, chunk).start()

    def close(self, chunk):
        @pl.when(self.is_inner == 1)
        def end():
            self.finish(chunk)

    def drain(self):
        @pl.when(self.is_inner == 1)
        def inner_end():
            for chunk in range(self.n_chunks):
                self.copy(1, chunk).wait_send()
                self.copy(2, chunk).wait_send()

        @pl.when(self.is_inner == 0)
        def outer_end():
            for chunk in range(self.n_chunks):
                self.copy(2, chunk).wait_recv()
                self.copy(0, chunk).wait_send()


def line_scratch(rows, width):
    return [pltpu.VMEM((rows, width), BF)] * 3 + [pltpu.SemaphoreType.DMA((CHUNKS,))] * 6


def forward_kernel(n_tp, with_sum, h_ref, opt0, opt1, opt2, opt3, vec_ref, bq_ref, cos_ref, sin_ref,
                   out_ref, q_ref, kv_ref, ctx_ref, lse_ref, pre_ref, weights, w_sem, active, kv_send, kv_recv, *line_refs):
    stage = lax.axis_index('pp')
    core = lax.rem(stage, 2)
    width = h_ref.shape[1]
    wait_weights = pick_weights(stage, (opt0, opt1, opt2, opt3), 0, weights.shape[0], weights, w_sem)
    meet(n_tp, with_sum, True)
    wait_weights()

    def project(normed, index):
        return (dot(normed, weights[index * HEAD:(index + 1) * HEAD, :], 1, 1) + bq_ref[index:index + 1, :]).astype(BF)

    swaps = []
    for block in range(2):
        rows = block_rows(block)
        xhat, _ = normalise(h_ref[rows, :])
        normed_a = (xhat * vec_ref[0:1, :] + vec_ref[1:2, :]).astype(BF)
        active[rows, :] = (xhat * vec_ref[2:3, :] + vec_ref[3:4, :]).astype(BF)
        cos_tab, sin_tab = cos_ref[rows, :], sin_ref[rows, :]
        place = slice(2 * block * BLOCK, (2 * block + 1) * BLOCK)
        for head in range(HEADS):
            q_ref[head, rows, :] = rotate_head(project(normed_a, head), cos_tab, sin_tab, False)
            kv_ref[head, place, :] = rotate_head(project(normed_a, HEADS + head), cos_tab, sin_tab, False)
            kv_ref[HEADS + head, place, :] = project(normed_a, 2 * HEADS + head)
        copy = pltpu.make_async_remote_copy(
            src_ref=kv_ref.at[:, pl.ds(2 * block * BLOCK, BLOCK), :], dst_ref=kv_ref.at[:, pl.ds((2 * block + 1) * BLOCK, BLOCK), :],
            send_sem=kv_send.at[block], recv_sem=kv_recv.at[block],
            device_id={'pp': stage + 1 - 2 * core}, device_id_type=MESH_ID)
        copy.start()
        swaps.append(copy)
    for block in range(2):
        rows = block_rows(block)
        pre_act = dot(active[rows, :], weights[4 * PART:4 * PART + width, :], 1, 0) + vec_ref[5:6, :]
        pre_ref[rows, :] = pre_act
        active[rows, :] = (0.5 * pre_act * (1.0 + lax.erf(pre_act * (2.0 ** -0.5)))).astype(BF)
    for copy in swaps:
        copy.wait_recv()
    if with_sum:
        part_ref = line_refs[0]
        line = LineSum(n_tp, part_ref, lambda rows: h_ref[rows, :].astype(F32) + vec_ref[4:5, :], out_ref, *line_refs[1:4], line_refs[4:])
    else:
        part_ref = out_ref
    for block in range(2):
        rows = block_rows(block)
        n_keys = (2, 4)[block] * BLOCK
        mask = causal_mask(core, block, n_keys)
        part = dot(active[rows, :], weights[4 * PART + width:, :], 1, 0)
        for head in range(HEADS):
            scores = dot(q_ref[head, rows, :], kv_ref[head, :n_keys, :], 1, 1) * (HEAD ** -0.5)
            scores = jnp.where(mask, scores, -1e30)
            top = jnp.max(scores, axis=-1, keepdims=True)
            expo = jnp.exp(scores - top)
            total = jnp.sum(expo, axis=-1, keepdims=True)
            probs = (expo / total).astype(BF)
            context = dot(probs, kv_ref[HEADS + head, :n_keys, :], 1, 0).astype(BF)
            ctx_ref[head, rows, :] = context
            lse_ref[head, rows, :] = top + jnp.log(total)
            part += dot(context, weights[3 * PART + head * HEAD:3 * PART + (head + 1) * HEAD, :], 1, 0)
        part_ref[rows, :] = part.astype(BF)
        if with_sum:
            line.offer(range(block * CHUNKS // 2, (block + 1) * CHUNKS // 2))
    if with_sum:
        for chunk in range(CHUNKS):
            line.step(chunk)
            if chunk:
                line.close(chunk - 1)
        line.close(CHUNKS - 1)
        line.drain()
    for copy in swaps:
        copy.wait_send()


def forward_layer(hidden, options, vec, bias_q, cos_tab, sin_tab, n_tp, with_sum):
    rows, width = hidden.shape
    block, anywhere = pl.BlockSpec(memory_space=pltpu.VMEM), pl.BlockSpec(memory_space=pl.ANY)
    scratch = [pltpu.VMEM(options[0].shape, BF), pltpu.SemaphoreType.DMA, pltpu.VMEM((rows, width), BF), pltpu.SemaphoreType.DMA((2,)), pltpu.SemaphoreType.DMA((2,))]
    if with_sum:
        scratch += [pltpu.VMEM((rows, width), BF)] + line_scratch(rows, width)
    return pl.pallas_call(
        functools.partial(forward_kernel, n_tp, with_sum),
        out_shape=(jax.ShapeDtypeStruct((rows, width), BF), jax.ShapeDtypeStruct((HEADS, rows, HEAD), BF), jax.ShapeDtypeStruct((2 * HEADS, 2 * rows, HEAD), BF),
                   jax.ShapeDtypeStruct((HEADS, rows, HEAD), BF), jax.ShapeDtypeStruct((HEADS, rows, 1), F32), jax.ShapeDtypeStruct((rows, width), F32)),
        in_specs=[block] + [anywhere] * 4 + [block] * 4,
        out_specs=tuple([block] * 6),
        scratch_shapes=scratch,
        compiler_params=pltpu.CompilerParams(collective_id=0 if with_sum else 1, has_side_effects=True, vmem_limit_bytes=LIMIT),
        cost_estimate=pl.CostEstimate(flops=40_000_000_000, bytes_accessed=8_000_000, transcendentals=0),
    )(hidden, *options, vec, bias_q, cos_tab, sin_tab)


def mlp_back_kernel(g_ref, h_ref, pre_ref, opt0, opt1, opt2, opt3, vec_ref, gx_ref, prod_ref, prod_b_ref, small_ref,
                    weights, w_sem, normed, gpre, active):
    stage = lax.axis_index('pp')
    width = h_ref.shape[1]
    wait_weights = pick_weights(stage, (opt0, opt1, opt2, opt3), 4 * PART, weights.shape[0], weights, w_sem)
    wait_weights()
    sums = [0.0] * 4
    for block in range(2):
        rows = block_rows(block)
        grad = g_ref[rows, :]
        pre_act = pre_ref[rows, :]
        gauss = 0.5 * (1.0 + lax.erf(pre_act * (2.0 ** -0.5)))
        active[rows, :] = (pre_act * gauss).astype(BF)
        slope = gauss + pre_act * jnp.exp(-0.5 * pre_act * pre_act) * 0.3989422804014327
        grad_pre = dot(grad, weights[width:, :], 1, 1) * slope
        gpre[rows, :] = grad_pre.astype(BF)
        sums[3] += jnp.sum(grad_pre, axis=0, keepdims=True)
        sums[2] += jnp.sum(grad.astype(F32), axis=0, keepdims=True)
        xhat, _ = normalise(h_ref[rows, :])
        normed[rows, :] = (xhat * vec_ref[2:3, :] + vec_ref[3:4, :]).astype(BF)
        grad_m = dot(gpre[rows, :], weights[:width, :], 1, 1)
        sums[0] += jnp.sum(grad_m * xhat, axis=0, keepdims=True)
        sums[1] += jnp.sum(grad_m, axis=0, keepdims=True)
        gx_ref[rows, :] = grad_m * vec_ref[2:3, :]
    for index, value in enumerate(sums):
        small_ref[index:index + 1, :] = value
    for first in range(0, width, 256):
        for left, right, row in ((normed, gpre, 0), (active, g_ref, width)):
            value = dot(left[:, first:first + 256], right[...], 0, 0)
            prod_ref[row + first:row + first + 256, :] = value
            prod_b_ref[row + first:row + first + 256, :] = value.astype(BF)


def mlp_back(grad, hidden, pre_act, options, vec):
    rows, width = hidden.shape
    block, anywhere = pl.BlockSpec(memory_space=pltpu.VMEM), pl.BlockSpec(memory_space=pl.ANY)
    return pl.pallas_call(
        mlp_back_kernel,
        out_shape=(jax.ShapeDtypeStruct((rows, width), F32), jax.ShapeDtypeStruct((2 * width, width), F32), jax.ShapeDtypeStruct((2 * width, width), BF), jax.ShapeDtypeStruct((4, width), F32)),
        in_specs=[block] * 3 + [anywhere] * 4 + [block],
        out_specs=tuple([block] * 4),
        scratch_shapes=[pltpu.VMEM((2 * width, width), BF), pltpu.SemaphoreType.DMA] + [pltpu.VMEM((rows, width), BF)] * 3,
        compiler_params=pltpu.CompilerParams(vmem_limit_bytes=LIMIT),
        cost_estimate=pl.CostEstimate(flops=10_000_000_000, bytes_accessed=12_000_000, transcendentals=0),
    )(grad, hidden, pre_act, *options, vec)


def att_back_kernel(n_tp, with_sum, g_ref, h_ref, gx_ref, q_ref, kv_ref, ctx_ref, lse_ref, opt0, opt1, opt2, opt3, vec_ref, cos_ref, sin_ref, *refs):
    if with_sum:
        out_ref, prod_ref, prod_b_ref, small_ref, bq_ref = refs[:5]
        refs = refs[5:]
    else:
        prod_ref, prod_b_ref, small_ref, bq_ref = refs[:4]
        refs = refs[4:]
    weights, w_sem, dkv, landed, dqkv, normed, kv_send, kv_recv = refs[:8]
    line_refs = refs[8:]
    stage = lax.axis_index('pp')
    core = lax.rem(stage, 2)
    wait_weights = pick_weights(stage, (opt0, opt1, opt2, opt3), 0, weights.shape[0], weights, w_sem)
    meet(n_tp, with_sum, True)
    wait_weights()
    for block in (1, 0):
        rows = block_rows(block)
        n_keys = (2, 4)[block] * BLOCK
        mask = causal_mask(core, block, n_keys)
        for head in range(HEADS):
            d_ctx = dot(g_ref[rows, :], weights[3 * PART + head * HEAD:3 * PART + (head + 1) * HEAD, :], 1, 1).astype(BF)
            q_part = q_ref[head, rows, :]
            k_part = kv_ref[head, :n_keys, :]
            scores = dot(q_part, k_part, 1, 1) * (HEAD ** -0.5)
            probs = jnp.where(mask, jnp.exp(scores - lse_ref[head, rows, :]), 0.0)
            dprobs = dot(d_ctx, kv_ref[HEADS + head, :n_keys, :], 1, 1).astype(BF).astype(F32)
            delta = jnp.sum(probs * dprobs, axis=-1, keepdims=True)
            dscores = (probs * (dprobs - delta) * (HEAD ** -0.5)).astype(BF)
            dqkv[head, rows, :] = dot(dscores, k_part, 1, 0).astype(BF)
            d_k = dot(dscores, q_part, 0, 0)
            d_v = dot(probs.astype(BF), d_ctx, 0, 0)
            if block == 1:
                dkv[head] = d_k
                dkv[HEADS + head] = d_v
            else:
                dkv[head, :n_keys, :] += d_k
                dkv[HEADS + head, :n_keys, :] += d_v
    swaps = []
    for block in range(2):
        copy = pltpu.make_async_remote_copy(
            src_ref=dkv.at[:, pl.ds((2 * block + 1) * BLOCK, BLOCK), :], dst_ref=landed.at[:, pl.ds(block * BLOCK, BLOCK), :],
            send_sem=kv_send.at[block], recv_sem=kv_recv.at[block],
            device_id={'pp': stage + 1 - 2 * core}, device_id_type=MESH_ID)
        copy.start()
        swaps.append(copy)
    if with_sum:
        part_ref = line_refs[0]
        line = LineSum(n_tp, part_ref, lambda rows: g_ref[rows, :].astype(F32), out_ref, *line_refs[1:4], line_refs[4:])
    sums = [0.0] * 2
    bias = [0.0] * (3 * HEADS)
    for copy in swaps:
        copy.wait_recv()
    for block in range(2):
        rows = block_rows(block)
        own = slice(2 * block * BLOCK, (2 * block + 1) * BLOCK)
        cos_tab, sin_tab = cos_ref[rows, :], sin_ref[rows, :]
        grad_a = 0.0
        for head in range(HEADS):
            d_q = rotate_head(dqkv[head, rows, :], cos_tab, sin_tab, True)
            d_k = rotate_head((dkv[head, own, :] + landed[head, rows, :]).astype(BF), cos_tab, sin_tab, True)
            d_v = (dkv[HEADS + head, own, :] + landed[HEADS + head, rows, :]).astype(BF)
            for kind, value in enumerate((d_q, d_k, d_v)):
                index = kind * HEADS + head
                dqkv[index, rows, :] = value
                bias[index] += jnp.sum(value.astype(F32), axis=0, keepdims=True)
                grad_a += dot(value, weights[index * HEAD:(index + 1) * HEAD, :], 1, 0)
        xhat, scale = normalise(h_ref[rows, :])
        normed[rows, :] = (xhat * vec_ref[0:1, :] + vec_ref[1:2, :]).astype(BF)
        sums[0] += jnp.sum(grad_a * xhat, axis=0, keepdims=True)
        sums[1] += jnp.sum(grad_a, axis=0, keepdims=True)
        if with_sum:
            grad_x = grad_a * vec_ref[0:1, :] + gx_ref[rows, :]
            branch = scale * (grad_x - jnp.mean(grad_x, axis=-1, keepdims=True) - xhat * jnp.mean(grad_x * xhat, axis=-1, keepdims=True))
            part_ref[rows, :] = branch.astype(BF)
            line.offer(range(block * CHUNKS // 2, (block + 1) * CHUNKS // 2))
    for index, value in enumerate(sums):
        small_ref[index:index + 1, :] = value
    for index, value in enumerate(bias):
        bq_ref[index:index + 1, :] = value

    def product(index):
        value = dot(dqkv[index], normed[...], 0, 0) if index < 3 * HEADS else dot(ctx_ref[index - 3 * HEADS], g_ref[...], 0, 0)
        prod_ref[index * HEAD:(index + 1) * HEAD, :] = value
        prod_b_ref[index * HEAD:(index + 1) * HEAD, :] = value.astype(BF)

    n_prod = 4 * HEADS
    for chunk in range(CHUNKS):
        if with_sum:
            line.step(chunk)
        for index in range(chunk * n_prod // CHUNKS, (chunk + 1) * n_prod // CHUNKS):
            product(index)
        if with_sum and chunk:
            line.close(chunk - 1)
    if with_sum:
        line.close(CHUNKS - 1)
        line.drain()
    for copy in swaps:
        copy.wait_send()


def att_back(grad, hidden, gx, query, kv_all, context, lse, options, vec, cos_tab, sin_tab, n_tp, with_sum):
    rows, width = hidden.shape
    block, anywhere = pl.BlockSpec(memory_space=pltpu.VMEM), pl.BlockSpec(memory_space=pl.ANY)
    n_att = 4 * PART
    out_shape = [jax.ShapeDtypeStruct((n_att, width), F32), jax.ShapeDtypeStruct((n_att, width), BF), jax.ShapeDtypeStruct((2, width), F32), jax.ShapeDtypeStruct((3 * HEADS, HEAD), F32)]
    scratch = [pltpu.VMEM((n_att, width), BF), pltpu.SemaphoreType.DMA, pltpu.VMEM((2 * HEADS, 2 * rows, HEAD), F32), pltpu.VMEM((2 * HEADS, rows, HEAD), F32),
               pltpu.VMEM((3 * HEADS, rows, HEAD), BF), pltpu.VMEM((rows, width), BF), pltpu.SemaphoreType.DMA((2,)), pltpu.SemaphoreType.DMA((2,))]
    if with_sum:
        out_shape = [jax.ShapeDtypeStruct((rows, width), BF)] + out_shape
        scratch += [pltpu.VMEM((rows, width), BF)] + line_scratch(rows, width)
    return pl.pallas_call(
        functools.partial(att_back_kernel, n_tp, with_sum),
        out_shape=tuple(out_shape),
        in_specs=[block] * 7 + [anywhere] * 4 + [block] * 3,
        out_specs=tuple([block] * len(out_shape)),
        scratch_shapes=scratch,
        compiler_params=pltpu.CompilerParams(collective_id=3 if with_sum else 4, has_side_effects=True, vmem_limit_bytes=LIMIT),
        cost_estimate=pl.CostEstimate(flops=45_000_000_000, bytes_accessed=12_000_000, transcendentals=0),
    )(grad, hidden, gx, query, kv_all, context, lse, *options, vec, cos_tab, sin_tab)


def causal_mask(core, block, n_keys):
    row = lax.broadcasted_iota(jnp.int32, (BLOCK, n_keys), 0)
    col = lax.broadcasted_iota(jnp.int32, (BLOCK, n_keys), 1)
    part = col // BLOCK
    starts = (core, 1 - core, 3 - core, 2 + core)
    start = jnp.where(part == 0, starts[0], jnp.where(part == 1, starts[1], jnp.where(part == 2, starts[2], starts[3])))
    mine = core if block == 0 else 3 - core
    return mine * BLOCK + row >= start * BLOCK + (col - part * BLOCK)


def small_kernel(n_pp, n_tp, n_norm, rows_ref, out_ref, box, stage_sum, norm_box, send_a, recv_a, send_b, recv_b):
    stage, rank = lax.axis_index('pp'), lax.axis_index('tp')
    barrier = pltpu.get_barrier_semaphore()
    for step in range(1, n_pp):
        pl.semaphore_signal(barrier, inc=1, device_id={'pp': lax.rem(stage + step, n_pp)}, device_id_type=MESH_ID)
    for step in range(1, n_tp):
        pl.semaphore_signal(barrier, inc=1, device_id={'tp': lax.rem(rank + step, n_tp)}, device_id_type=MESH_ID)
    pl.semaphore_wait(barrier, n_pp + n_tp - 2)
    sends = []
    for step in range(1, n_pp):
        peer = lax.rem(stage + step, n_pp)
        copy = pltpu.make_async_remote_copy(
            src_ref=rows_ref.at[peer], dst_ref=box.at[step - 1], send_sem=send_a.at[step - 1],
            recv_sem=recv_a.at[step - 1], device_id={'pp': peer}, device_id_type=MESH_ID)
        copy.start()
        sends.append(copy)
    total = rows_ref[stage]
    for step, copy in enumerate(sends):
        copy.wait_recv()
        total += box[step]
    stage_sum[...] = total
    norm_box[rank] = total[:n_norm]
    shares = []
    for step in range(1, n_tp):
        copy = pltpu.make_async_remote_copy(
            src_ref=stage_sum.at[pl.ds(0, n_norm)], dst_ref=norm_box.at[rank], send_sem=send_b.at[step - 1],
            recv_sem=recv_b.at[step - 1], device_id={'tp': lax.rem(rank + step, n_tp)}, device_id_type=MESH_ID)
        copy.start()
        shares.append(copy)
    for copy in shares:
        copy.wait()
    norms = norm_box[0]
    for index in range(1, n_tp):
        norms += norm_box[index]
    out_ref[:n_norm, :] = norms
    out_ref[n_norm:, :] = total[n_norm:]
    for copy in sends:
        copy.wait_send()


def sum_small(rows, n_tp):
    n_pp, count, width = rows.shape
    n_norm = count // 2
    return pl.pallas_call(
        functools.partial(small_kernel, n_pp, n_tp, n_norm),
        out_shape=jax.ShapeDtypeStruct((count, width), F32),
        in_specs=[pl.BlockSpec(memory_space=pltpu.VMEM)],
        out_specs=pl.BlockSpec(memory_space=pltpu.VMEM),
        scratch_shapes=[pltpu.VMEM((n_pp - 1, count, width), F32), pltpu.VMEM((count, width), F32), pltpu.VMEM((n_tp, n_norm, width), F32),
                        pltpu.SemaphoreType.DMA((n_pp - 1,)), pltpu.SemaphoreType.DMA((n_pp - 1,)), pltpu.SemaphoreType.DMA((n_tp - 1,)), pltpu.SemaphoreType.DMA((n_tp - 1,))],
        compiler_params=pltpu.CompilerParams(collective_id=2, has_side_effects=True),
        cost_estimate=pl.CostEstimate(flops=8_000_000_000, bytes_accessed=200_000, transcendentals=0),
    )(rows)


def solution(mesh):
    n_stages = mesh.shape['pp']
    n_tp = mesh.shape['tp']
    swap_core = [(stage, stage ^ 1) for stage in range(n_stages)]

    def device_fn(x_in, g_out, ln1_gain, ln1_bias, w_qkv, b_qkv, w_out, b_out, ln2_gain, ln2_bias, w_up, b_up, w_down, b_down):
        stage = lax.axis_index('pp')
        core = stage % 2
        _, width = x_in.shape[2:]

        def own_tokens(array):
            blocks = lax.dynamic_index_in_dim(array, stage // 2, 0, keepdims=False).reshape(4, BLOCK, width)
            first = lax.dynamic_index_in_dim(blocks, core, 0, keepdims=False)
            second = lax.dynamic_index_in_dim(blocks, 3 - core, 0, keepdims=False)
            return jnp.concatenate([first, second], axis=0).astype(BF)

        hidden = own_tokens(x_in)
        grad = own_tokens(g_out)

        half_rot = HEAD // 8
        inv_freq = ROPE_BASE ** (-(jnp.arange(half_rot, dtype=F32) * 2.0) / (2 * half_rot))
        spot = jnp.concatenate([core * BLOCK + jnp.arange(BLOCK), (3 - core) * BLOCK + jnp.arange(BLOCK)])
        angles = spot.astype(F32)[:, None] * inv_freq[None, :]
        still = jnp.zeros((ROWS, HEAD - 2 * half_rot), F32)
        cos_tab = jnp.tile(jnp.concatenate([jnp.cos(angles), jnp.cos(angles), still + 1.0], axis=1), (1, 1))
        sin_tab = jnp.tile(jnp.concatenate([jnp.sin(angles), jnp.sin(angles), still], axis=1), (1, 1))

        wq_rows = jnp.transpose(w_qkv[0], (2, 1, 3, 0)).reshape(3 * PART, width)
        bundle = jnp.concatenate([wq_rows, w_out[0].reshape(PART, width), w_up[0], w_down[0]], axis=0)
        bias_qkv = jnp.transpose(b_qkv[0], (1, 0, 2)).reshape(3 * PART).astype(F32)
        pad = jnp.zeros((width - 3 * PART,), F32)
        vectors = jnp.stack([ln1_gain[0], ln1_bias[0], ln2_gain[0], ln2_bias[0], b_out[0].astype(F32) + b_down[0].astype(F32), b_up[0].astype(F32), jnp.concatenate([bias_qkv, pad]), jnp.zeros((width,), F32)])

        pair_a, pair_b = [(0, 2), (2, 0)], [(1, 3), (3, 1)]
        first_wave = lax.ppermute(bundle, 'pp', pair_a)
        later, first_wave = tie(bundle, first_wave)
        second_wave = lax.ppermute(later, 'pp', pair_b)
        partner = lax.ppermute(bundle, 'pp', swap_core)
        first_pass = lax.ppermute(first_wave, 'pp', [(2, 3), (0, 1)])
        all_vectors = lax.all_gather(vectors, 'pp')
        sources = {0: (bundle, partner, first_wave, first_pass), 2: (first_wave, first_pass, bundle, partner)}
        saved = []
        for layer in range(n_stages):
            vec = all_vectors[layer]
            bias_q = vec[6, :3 * PART].reshape(3 * HEADS, HEAD)
            last = layer == n_stages - 1
            result, query, kv_all, context, lse, pre_act = forward_layer(hidden, sources[layer], vec, bias_q, cos_tab, sin_tab, n_tp, not last)
            saved.append((hidden, query, kv_all, context, lse, pre_act))
            if last:
                summed = lax.psum(result, 'tp')
                break
            hidden = result
            if layer == 0:
                hidden, second_wave = tie(hidden, second_wave)
                second_pass = lax.ppermute(second_wave, 'pp', [(3, 2), (1, 0)])
                sources[1] = (partner, bundle, second_pass, second_wave)
                sources[3] = (second_pass, second_wave, partner, bundle)

        def send_near(prod_b, layer):
            return lax.ppermute(prod_b, 'pp', [(layer ^ 1, layer), (layer ^ 3, layer ^ 2)])

        def send_far(prod, layer):
            return lax.ppermute(prod, 'pp', [(layer ^ 2, layer)])

        def add_near(prod, near):
            return (prod + near.astype(F32)).astype(BF)

        small = {}
        prod, prod_b, near, far = {}, {}, {}, {}
        for layer in reversed(range(n_stages)):
            hidden, query, kv_all, context, lse, pre_act = saved[layer]
            vec = all_vectors[layer]
            key_m, key_a = (layer, 'm'), (layer, 'a')
            gx, prod[key_m], prod_b[key_m], small_m = mlp_back(grad, hidden, pre_act, sources[layer], vec)
            near[key_m] = send_near(prod_b[key_m], layer)
            above = (layer + 1, 'a')
            if above in near:
                gx, near[above] = tie(gx, near[above])
                far[above] = send_far(add_near(prod[above], near[above]), layer + 1)
            if layer < 2:
                gx, near[key_m] = tie(gx, near[key_m])
                far[key_m] = send_far(add_near(prod[key_m], near[key_m]), layer)
            out = att_back(grad, hidden, gx, query, kv_all, context, lse, sources[layer], vec, cos_tab, sin_tab, n_tp, layer > 0)
            prod[key_a], prod_b[key_a], small_a, bias_a = out[-4:]
            small[layer] = jnp.concatenate([small_a, small_m, jnp.concatenate([bias_a.reshape(1, 3 * PART), pad[None]], axis=1), jnp.zeros((1, width), F32)], axis=0)
            near[key_a] = send_near(prod_b[key_a], layer)
            if layer:
                grad = out[0]
            if layer == 3:
                grad, summed = tie(grad, summed)
            if layer > 1:
                grad, near[key_m] = tie(grad, near[key_m])
                far[key_m] = send_far(add_near(prod[key_m], near[key_m]), layer)
        far[0, 'a'] = send_far(add_near(prod[0, 'a'], near[0, 'a']), 0)

        final = (saved[-1][0].astype(F32) + all_vectors[-1][4:5] + summed.astype(F32)).astype(BF)
        gathered = lax.all_gather(final, 'pp').reshape(2, 2, 2, BLOCK, width)
        y_out = jnp.stack([gathered[:, 0, 0], gathered[:, 1, 0], gathered[:, 1, 1], gathered[:, 0, 1]], axis=1).reshape(x_in.shape)

        def total_of(key):
            return prod[key] + near[key].astype(F32) + far[key].astype(F32)

        def collect(kind):
            upper = jnp.where(stage == 3, total_of((3, kind)), total_of((2, kind)))
            (upper,) = lax.optimization_barrier((upper,))
            upper = jnp.where(stage == 1, total_of((1, kind)), upper)
            (upper,) = lax.optimization_barrier((upper,))
            return jnp.where(stage == 0, total_of((0, kind)), upper)

        small = sum_small(jnp.stack([small[layer] for layer in range(n_stages)]), n_tp)
        norms = small
        grad_att, grad_mlp = collect('a'), collect('m')
        grad_qkv = jnp.transpose(grad_att[:3 * PART].reshape(3, HEADS, HEAD, width), (3, 1, 0, 2))
        grads = (
            norms[0], norms[1], grad_qkv, jnp.transpose(small[6, :3 * PART].reshape(3, HEADS, HEAD), (1, 0, 2)),
            grad_att[3 * PART:].reshape(HEADS, HEAD, width), small[4], norms[2], norms[3],
            grad_mlp[:width], small[5], grad_mlp[width:], small[4])
        return tuple([y_out] + [item[None] for item in grads])

    return jax.shard_map(device_fn, mesh=mesh, in_specs=(P('dp'), P('dp')) + STAGE_SPECS, out_specs=(P('dp'),) + GRAD_SPECS, check_vma=False)
```

```python
import functools

import jax
import jax.numpy as jnp
from jax import lax
from jax.experimental import pallas as pl
from jax.experimental.pallas import tpu as pltpu
from jax.sharding import PartitionSpec as P

BF = jnp.bfloat16
F32 = jnp.float32
ROPE_BASE = 10000.0
LN_EPS = 1e-5
HEADS = 3
HEAD = 64
PART = HEADS * HEAD
BLOCK = 256
ROWS = 2 * BLOCK
STAGE_SPECS = (P('pp', None), P('pp', None), P('pp', None, 'tp', None, None), P('pp', 'tp', None, None), P('pp', 'tp', None, None), P('pp', None), P('pp', None), P('pp', None), P('pp', None, 'tp'), P('pp', 'tp'), P('pp', 'tp', None), P('pp', None))
GRAD_SPECS = (P(('dp', 'pp'), None), P(('dp', 'pp'), None), P(('dp', 'pp'), None, 'tp', None, None), P(('dp', 'pp'), 'tp', None, None), P(('dp', 'pp'), 'tp', None, None), P(('dp', 'pp'), None), P(('dp', 'pp'), None), P(('dp', 'pp'), None), P(('dp', 'pp'), None, 'tp'), P(('dp', 'pp'), 'tp'), P(('dp', 'pp'), 'tp', None), P(('dp', 'pp'), None))
CHUNKS = 8
LIMIT = 60 * 2 ** 20
MESH_ID = pl.DeviceIdType.MESH


def tie(*values):
    return lax.optimization_barrier(values)


def dot(left, right, left_dim, right_dim):
    return lax.dot_general(left, right, (((left_dim,), (right_dim,)), ((), ())), preferred_element_type=F32)


def normalise(hidden):
    hidden_f = hidden.astype(F32)
    center = hidden_f - jnp.mean(hidden_f, axis=-1, keepdims=True)
    scale = lax.rsqrt(jnp.mean(center * center, axis=-1, keepdims=True) + LN_EPS)
    return center * scale, scale


def turn_matrix(width, transposed):
    row = lax.broadcasted_iota(jnp.int32, (width, width), 0)
    col = lax.broadcasted_iota(jnp.int32, (width, width), 1)
    if transposed:
        row, col = col, row
    dim = col % HEAD
    minus = (dim < 8) & (row == col + 8)
    plus = (dim >= 8) & (dim < 16) & (row == col - 8)
    return (plus.astype(F32) - minus.astype(F32)).astype(BF)


def rotate_head(values, cos_tab, sin_tab, transposed):
    turned = dot(values, turn_matrix(HEAD, transposed), 1, 0)
    return (values.astype(F32) * cos_tab + turned * sin_tab).astype(BF)


def block_rows(block):
    return slice(block * BLOCK, (block + 1) * BLOCK)


def pick_weights(stage, options, first, count, scratch, sem):
    for index, option in enumerate(options):
        @pl.when(stage == index)
        def fetch():
            pltpu.make_async_copy(option.at[pl.ds(first, count)], scratch, sem).start()

    return pltpu.make_async_copy(options[0].at[pl.ds(first, count)], scratch, sem).wait


def meet(n_tp, with_sum, with_core, with_stage=False):
    rank, stage = lax.axis_index('tp'), lax.axis_index('pp')
    barrier = pltpu.get_barrier_semaphore()
    count = 0
    if with_core:
        pl.semaphore_signal(barrier, inc=1, device_id={'pp': stage + 1 - 2 * lax.rem(stage, 2)}, device_id_type=MESH_ID)
        count = 1
    if with_stage:
        pl.semaphore_signal(barrier, inc=1, device_id={'pp': lax.rem(stage + 2, 4)}, device_id_type=MESH_ID)
        count += 1
    if with_sum:
        is_inner = lax.rem((rank + 1) // 2, 2)
        near = rank + 1 - 2 * lax.rem(rank, 2)
        pl.semaphore_signal(barrier, inc=1, device_id={'tp': near}, device_id_type=MESH_ID)

        @pl.when(is_inner == 1)
        def greet():
            pl.semaphore_signal(barrier, inc=1, device_id={'tp': n_tp - 1 - rank}, device_id_type=MESH_ID)

        count = count + 1 + is_inner
    pl.semaphore_wait(barrier, count)


class LineSum:
    def __init__(self, n_tp, part, base, out, inbox, half, across, sems):
        self.part, self.base, self.out, self.inbox, self.half, self.across, self.sems = part, base, out, inbox, half, across, sems
        rank = lax.axis_index('tp')
        self.is_inner = lax.rem((rank + 1) // 2, 2)
        self.near = rank + 1 - 2 * lax.rem(rank, 2)
        self.mirror = n_tp - 1 - rank
        self.n_chunks = CHUNKS
        self.size = out.shape[0] // CHUNKS

    def span(self, chunk):
        return pl.ds(chunk * self.size, self.size)

    def copy(self, kind, chunk):
        source, target, device = ((self.part, self.inbox, self.near), (self.half, self.across, self.mirror), (self.out, self.out, self.near))[kind]
        return pltpu.make_async_remote_copy(
            src_ref=source.at[self.span(chunk)], dst_ref=target.at[self.span(chunk)], send_sem=self.sems[2 * kind].at[chunk],
            recv_sem=self.sems[2 * kind + 1].at[chunk], device_id={'tp': device}, device_id_type=MESH_ID)

    def offer(self, chunks):
        @pl.when(self.is_inner == 0)
        def start():
            for chunk in chunks:
                self.copy(0, chunk).start()

    def finish(self, chunk):
        rows = self.span(chunk)
        self.copy(1, chunk).wait_recv()
        both = self.half[rows, :].astype(F32) + self.across[rows, :].astype(F32)
        self.out[rows, :] = (self.base(rows) + both).astype(BF)
        self.copy(2, chunk).start()

    def step(self, chunk):
        @pl.when(self.is_inner == 1)
        def merge():
            rows = self.span(chunk)
            self.copy(0, chunk).wait_recv()
            self.half[rows, :] = (self.part[rows, :].astype(F32) + self.inbox[rows, :].astype(F32)).astype(BF)
            self.copy(1, chunk).start()

    def close(self, chunk):
        @pl.when(self.is_inner == 1)
        def end():
            self.finish(chunk)

    def drain(self):
        @pl.when(self.is_inner == 1)
        def inner_end():
            for chunk in range(self.n_chunks):
                self.copy(1, chunk).wait_send()
                self.copy(2, chunk).wait_send()

        @pl.when(self.is_inner == 0)
        def outer_end():
            for chunk in range(self.n_chunks):
                self.copy(2, chunk).wait_recv()
                self.copy(0, chunk).wait_send()


def line_scratch(rows, width):
    return [pltpu.VMEM((rows, width), BF)] * 3 + [pltpu.SemaphoreType.DMA((CHUNKS,))] * 6


class StageSum:
    def __init__(self, layer, prod, prod_b, result, staged, near, far, half, sems):
        self.prod, self.prod_b, self.result, self.staged, self.near, self.far, self.half, self.sems = prod, prod_b, result, staged, near, far, half, sems
        self.stage = lax.axis_index('pp')
        self.is_owner = self.stage == layer
        self.is_relay = self.stage == (layer ^ 2)
        self.is_giver = lax.rem(self.stage, 2) != layer % 2
        self.is_keeper = lax.rem(self.stage, 2) == layer % 2

    def load(self):
        return pltpu.make_async_copy(self.prod, self.staged, self.sems.at[0])

    def store(self):
        return pltpu.make_async_copy(self.staged, self.result, self.sems.at[1])

    def hand(self):
        return pltpu.make_async_remote_copy(
            src_ref=self.prod_b, dst_ref=self.near, send_sem=self.sems.at[2], recv_sem=self.sems.at[3],
            device_id={'pp': self.stage + 1 - 2 * lax.rem(self.stage, 2)}, device_id_type=MESH_ID)

    def cross(self):
        return pltpu.make_async_remote_copy(
            src_ref=self.half, dst_ref=self.far, send_sem=self.sems.at[4], recv_sem=self.sems.at[5],
            device_id={'pp': lax.rem(self.stage + 2, 4)}, device_id_type=MESH_ID)

    def blocks(self):
        return [pl.ds(first, BLOCK) for first in range(0, self.staged.shape[0], BLOCK)]

    def begin(self):
        @pl.when(self.is_giver)
        def give():
            self.hand().start()

        @pl.when(self.is_keeper)
        def keep():
            self.load().start()

    def relay(self):
        @pl.when(self.is_relay)
        def send_on():
            self.load().wait()
            self.hand().wait_recv()
            for rows in self.blocks():
                self.half[rows, :] = (self.staged[rows, :] + self.near[rows, :].astype(F32)).astype(BF)
            self.cross().start()

    def end(self):
        @pl.when(self.is_owner)
        def close():
            self.load().wait()
            self.hand().wait_recv()
            self.cross().wait_recv()
            for rows in self.blocks():
                self.staged[rows, :] += self.near[rows, :].astype(F32) + self.far[rows, :].astype(F32)
            self.store().start()
            self.store().wait()

        @pl.when(self.is_relay)
        def relayed():
            self.cross().wait_send()

        @pl.when(self.is_giver)
        def given():
            self.hand().wait_send()


def stage_scratch(rows, width):
    return [pltpu.VMEM((rows, width), F32)] + [pltpu.VMEM((rows, width), BF)] * 3 + [pltpu.SemaphoreType.DMA((6,))]


def forward_kernel(n_tp, with_sum, h_ref, opt0, opt1, opt2, opt3, vec_ref, bq_ref, cos_ref, sin_ref,
                   out_ref, q_ref, kv_ref, ctx_ref, lse_ref, pre_ref, weights, w_sem, active, kv_send, kv_recv, *line_refs):
    stage = lax.axis_index('pp')
    core = lax.rem(stage, 2)
    width = h_ref.shape[1]
    wait_weights = pick_weights(stage, (opt0, opt1, opt2, opt3), 0, weights.shape[0], weights, w_sem)
    meet(n_tp, with_sum, True)
    wait_weights()

    def project(normed, index):
        return (dot(normed, weights[index * HEAD:(index + 1) * HEAD, :], 1, 1) + bq_ref[index:index + 1, :]).astype(BF)

    swaps = []
    for block in range(2):
        rows = block_rows(block)
        xhat, _ = normalise(h_ref[rows, :])
        normed_a = (xhat * vec_ref[0:1, :] + vec_ref[1:2, :]).astype(BF)
        active[rows, :] = (xhat * vec_ref[2:3, :] + vec_ref[3:4, :]).astype(BF)
        cos_tab, sin_tab = cos_ref[rows, :], sin_ref[rows, :]
        place = slice(2 * block * BLOCK, (2 * block + 1) * BLOCK)
        for head in range(HEADS):
            q_ref[head, rows, :] = rotate_head(project(normed_a, head), cos_tab, sin_tab, False)
            kv_ref[head, place, :] = rotate_head(project(normed_a, HEADS + head), cos_tab, sin_tab, False)
            kv_ref[HEADS + head, place, :] = project(normed_a, 2 * HEADS + head)
        copy = pltpu.make_async_remote_copy(
            src_ref=kv_ref.at[:, pl.ds(2 * block * BLOCK, BLOCK), :], dst_ref=kv_ref.at[:, pl.ds((2 * block + 1) * BLOCK, BLOCK), :],
            send_sem=kv_send.at[block], recv_sem=kv_recv.at[block],
            device_id={'pp': stage + 1 - 2 * core}, device_id_type=MESH_ID)
        copy.start()
        swaps.append(copy)
    for block in range(2):
        rows = block_rows(block)
        pre_act = dot(active[rows, :], weights[4 * PART:4 * PART + width, :], 1, 0) + vec_ref[5:6, :]
        pre_ref[rows, :] = pre_act
        active[rows, :] = (0.5 * pre_act * (1.0 + lax.erf(pre_act * (2.0 ** -0.5)))).astype(BF)
    for copy in swaps:
        copy.wait_recv()
    if with_sum:
        part_ref = line_refs[0]
        line = LineSum(n_tp, part_ref, lambda rows: h_ref[rows, :].astype(F32) + vec_ref[4:5, :], out_ref, *line_refs[1:4], line_refs[4:])
    else:
        part_ref = out_ref
    for block in range(2):
        rows = block_rows(block)
        n_keys = (2, 4)[block] * BLOCK
        mask = causal_mask(core, block, n_keys)
        part = dot(active[rows, :], weights[4 * PART + width:, :], 1, 0)
        for head in range(HEADS):
            scores = dot(q_ref[head, rows, :], kv_ref[head, :n_keys, :], 1, 1) * (HEAD ** -0.5)
            scores = jnp.where(mask, scores, -1e30)
            top = jnp.max(scores, axis=-1, keepdims=True)
            expo = jnp.exp(scores - top)
            total = jnp.sum(expo, axis=-1, keepdims=True)
            probs = (expo / total).astype(BF)
            context = dot(probs, kv_ref[HEADS + head, :n_keys, :], 1, 0).astype(BF)
            ctx_ref[head, rows, :] = context
            lse_ref[head, rows, :] = top + jnp.log(total)
            part += dot(context, weights[3 * PART + head * HEAD:3 * PART + (head + 1) * HEAD, :], 1, 0)
        part_ref[rows, :] = part.astype(BF)
        if with_sum:
            line.offer(range(block * CHUNKS // 2, (block + 1) * CHUNKS // 2))
    if with_sum:
        for chunk in range(CHUNKS):
            line.step(chunk)
            if chunk:
                line.close(chunk - 1)
        line.close(CHUNKS - 1)
        line.drain()
    for copy in swaps:
        copy.wait_send()


def forward_layer(hidden, options, vec, bias_q, cos_tab, sin_tab, n_tp, with_sum):
    rows, width = hidden.shape
    block, anywhere = pl.BlockSpec(memory_space=pltpu.VMEM), pl.BlockSpec(memory_space=pl.ANY)
    scratch = [pltpu.VMEM(options[0].shape, BF), pltpu.SemaphoreType.DMA, pltpu.VMEM((rows, width), BF), pltpu.SemaphoreType.DMA((2,)), pltpu.SemaphoreType.DMA((2,))]
    if with_sum:
        scratch += [pltpu.VMEM((rows, width), BF)] + line_scratch(rows, width)
    return pl.pallas_call(
        functools.partial(forward_kernel, n_tp, with_sum),
        out_shape=(jax.ShapeDtypeStruct((rows, width), BF), jax.ShapeDtypeStruct((HEADS, rows, HEAD), BF), jax.ShapeDtypeStruct((2 * HEADS, 2 * rows, HEAD), BF),
                   jax.ShapeDtypeStruct((HEADS, rows, HEAD), BF), jax.ShapeDtypeStruct((HEADS, rows, 1), F32), jax.ShapeDtypeStruct((rows, width), F32)),
        in_specs=[block] + [anywhere] * 4 + [block] * 4,
        out_specs=tuple([block] * 6),
        scratch_shapes=scratch,
        compiler_params=pltpu.CompilerParams(collective_id=0 if with_sum else 1, has_side_effects=True, vmem_limit_bytes=LIMIT),
        cost_estimate=pl.CostEstimate(flops=40_000_000_000, bytes_accessed=8_000_000, transcendentals=0),
    )(hidden, *options, vec, bias_q, cos_tab, sin_tab)


def mlp_back_kernel(n_tp, g_ref, h_ref, pre_ref, opt0, opt1, opt2, opt3, vec_ref, gx_ref, prod_ref, prod_b_ref, small_ref,
                    weights, w_sem, normed, gpre, active):
    stage = lax.axis_index('pp')
    width = h_ref.shape[1]
    wait_weights = pick_weights(stage, (opt0, opt1, opt2, opt3), 4 * PART, weights.shape[0], weights, w_sem)
    wait_weights()
    sums = [0.0] * 4
    for block in range(2):
        rows = block_rows(block)
        grad = g_ref[rows, :]
        pre_act = pre_ref[rows, :]
        gauss = 0.5 * (1.0 + lax.erf(pre_act * (2.0 ** -0.5)))
        active[rows, :] = (pre_act * gauss).astype(BF)
        slope = gauss + pre_act * jnp.exp(-0.5 * pre_act * pre_act) * 0.3989422804014327
        grad_pre = dot(grad, weights[width:, :], 1, 1) * slope
        gpre[rows, :] = grad_pre.astype(BF)
        sums[3] += jnp.sum(grad_pre, axis=0, keepdims=True)
        sums[2] += jnp.sum(grad.astype(F32), axis=0, keepdims=True)
        xhat, _ = normalise(h_ref[rows, :])
        normed[rows, :] = (xhat * vec_ref[2:3, :] + vec_ref[3:4, :]).astype(BF)
        grad_m = dot(gpre[rows, :], weights[:width, :], 1, 1)
        sums[0] += jnp.sum(grad_m * xhat, axis=0, keepdims=True)
        sums[1] += jnp.sum(grad_m, axis=0, keepdims=True)
        gx_ref[rows, :] = grad_m * vec_ref[2:3, :]
    for index, value in enumerate(sums):
        small_ref[index:index + 1, :] = value
    for first in range(0, width, 256):
        for left, right, row in ((normed, gpre, 0), (active, g_ref, width)):
            value = dot(left[:, first:first + 256], right[...], 0, 0)
            prod_ref[row + first:row + first + 256, :] = value
            prod_b_ref[row + first:row + first + 256, :] = value.astype(BF)


def mlp_back(grad, hidden, pre_act, options, vec, n_tp):
    rows, width = hidden.shape
    block, anywhere = pl.BlockSpec(memory_space=pltpu.VMEM), pl.BlockSpec(memory_space=pl.ANY)
    return pl.pallas_call(
        functools.partial(mlp_back_kernel, n_tp),
        out_shape=(jax.ShapeDtypeStruct((rows, width), F32), jax.ShapeDtypeStruct((2 * width, width), F32), jax.ShapeDtypeStruct((2 * width, width), BF), jax.ShapeDtypeStruct((4, width), F32)),
        in_specs=[block] * 3 + [anywhere] * 4 + [block],
        out_specs=tuple([block] * 4),
        scratch_shapes=[pltpu.VMEM((2 * width, width), BF), pltpu.SemaphoreType.DMA] + [pltpu.VMEM((rows, width), BF)] * 3,
        compiler_params=pltpu.CompilerParams(vmem_limit_bytes=LIMIT),
        cost_estimate=pl.CostEstimate(flops=10_000_000_000, bytes_accessed=12_000_000, transcendentals=0),
    )(grad, hidden, pre_act, *options, vec)


def att_back_kernel(n_tp, layer, with_sum, n_red, g_ref, h_ref, gx_ref, q_ref, kv_ref, ctx_ref, lse_ref, opt0, opt1, opt2, opt3, vec_ref, cos_ref, sin_ref, *refs):
    n_in = (2, 4)[n_red - 1] + (0 if layer == 3 else n_red if layer < 2 else 1)
    given, refs = refs[:n_in], refs[n_in:]
    if with_sum:
        out_ref, refs = refs[0], refs[1:]
    prod_ref, prod_b_ref, small_ref, bq_ref = refs[:4]
    results, refs = refs[4:4 + n_red], refs[4 + n_red:]
    weights, w_sem, dkv, landed, dqkv, normed, kv_send, kv_recv = refs[:8]
    line_refs = refs[8:]
    reductions = []
    for index in range(n_red):
        own = line_refs[-5 * (n_red - index):][:5]
        reductions.append(StageSum(layer + index, given[2 * index], given[2 * index + 1], results[index], *own))
    line_refs = line_refs[:len(line_refs) - 5 * n_red]
    stage = lax.axis_index('pp')
    core = lax.rem(stage, 2)
    wait_weights = pick_weights(stage, (opt0, opt1, opt2, opt3), 0, weights.shape[0], weights, w_sem)
    meet(n_tp, with_sum, True, True)
    for item in reductions:
        item.begin()
    wait_weights()
    for block in (1, 0):
        rows = block_rows(block)
        n_keys = (2, 4)[block] * BLOCK
        mask = causal_mask(core, block, n_keys)
        for head in range(HEADS):
            d_ctx = dot(g_ref[rows, :], weights[3 * PART + head * HEAD:3 * PART + (head + 1) * HEAD, :], 1, 1).astype(BF)
            q_part = q_ref[head, rows, :]
            k_part = kv_ref[head, :n_keys, :]
            scores = dot(q_part, k_part, 1, 1) * (HEAD ** -0.5)
            probs = jnp.where(mask, jnp.exp(scores - lse_ref[head, rows, :]), 0.0)
            dprobs = dot(d_ctx, kv_ref[HEADS + head, :n_keys, :], 1, 1).astype(BF).astype(F32)
            delta = jnp.sum(probs * dprobs, axis=-1, keepdims=True)
            dscores = (probs * (dprobs - delta) * (HEAD ** -0.5)).astype(BF)
            dqkv[head, rows, :] = dot(dscores, k_part, 1, 0).astype(BF)
            d_k = dot(dscores, q_part, 0, 0)
            d_v = dot(probs.astype(BF), d_ctx, 0, 0)
            if block == 1:
                dkv[head] = d_k
                dkv[HEADS + head] = d_v
            else:
                dkv[head, :n_keys, :] += d_k
                dkv[HEADS + head, :n_keys, :] += d_v
        if block == 1:
            for item in reversed(reductions):
                item.relay()
    swaps = []
    for block in range(2):
        copy = pltpu.make_async_remote_copy(
            src_ref=dkv.at[:, pl.ds((2 * block + 1) * BLOCK, BLOCK), :], dst_ref=landed.at[:, pl.ds(block * BLOCK, BLOCK), :],
            send_sem=kv_send.at[block], recv_sem=kv_recv.at[block],
            device_id={'pp': stage + 1 - 2 * core}, device_id_type=MESH_ID)
        copy.start()
        swaps.append(copy)
    if with_sum:
        part_ref = line_refs[0]
        line = LineSum(n_tp, part_ref, lambda rows: g_ref[rows, :].astype(F32), out_ref, *line_refs[1:4], line_refs[4:])
    sums = [0.0] * 2
    bias = [0.0] * (3 * HEADS)
    for copy in swaps:
        copy.wait_recv()
    for block in range(2):
        rows = block_rows(block)
        own = slice(2 * block * BLOCK, (2 * block + 1) * BLOCK)
        cos_tab, sin_tab = cos_ref[rows, :], sin_ref[rows, :]
        grad_a = 0.0
        for head in range(HEADS):
            d_q = rotate_head(dqkv[head, rows, :], cos_tab, sin_tab, True)
            d_k = rotate_head((dkv[head, own, :] + landed[head, rows, :]).astype(BF), cos_tab, sin_tab, True)
            d_v = (dkv[HEADS + head, own, :] + landed[HEADS + head, rows, :]).astype(BF)
            for kind, value in enumerate((d_q, d_k, d_v)):
                index = kind * HEADS + head
                dqkv[index, rows, :] = value
                bias[index] += jnp.sum(value.astype(F32), axis=0, keepdims=True)
                grad_a += dot(value, weights[index * HEAD:(index + 1) * HEAD, :], 1, 0)
        xhat, scale = normalise(h_ref[rows, :])
        normed[rows, :] = (xhat * vec_ref[0:1, :] + vec_ref[1:2, :]).astype(BF)
        sums[0] += jnp.sum(grad_a * xhat, axis=0, keepdims=True)
        sums[1] += jnp.sum(grad_a, axis=0, keepdims=True)
        if with_sum:
            grad_x = grad_a * vec_ref[0:1, :] + gx_ref[rows, :]
            branch = scale * (grad_x - jnp.mean(grad_x, axis=-1, keepdims=True) - xhat * jnp.mean(grad_x * xhat, axis=-1, keepdims=True))
            part_ref[rows, :] = branch.astype(BF)
            line.offer(range(block * CHUNKS // 2, (block + 1) * CHUNKS // 2))
    for index, value in enumerate(sums):
        small_ref[index:index + 1, :] = value
    for index, value in enumerate(bias):
        bq_ref[index:index + 1, :] = value

    def product(index):
        value = dot(dqkv[index], normed[...], 0, 0) if index < 3 * HEADS else dot(ctx_ref[index - 3 * HEADS], g_ref[...], 0, 0)
        prod_ref[index * HEAD:(index + 1) * HEAD, :] = value
        prod_b_ref[index * HEAD:(index + 1) * HEAD, :] = value.astype(BF)

    n_prod = 4 * HEADS
    for chunk in range(CHUNKS):
        if with_sum:
            line.step(chunk)
        for index in range(chunk * n_prod // CHUNKS, (chunk + 1) * n_prod // CHUNKS):
            product(index)
        if with_sum and chunk:
            line.close(chunk - 1)
    if with_sum:
        line.close(CHUNKS - 1)
        line.drain()
    for copy in swaps:
        copy.wait_send()
    for item in reversed(reductions):
        item.end()


def att_back(layer, grad, hidden, gx, query, kv_all, context, lse, options, vec, cos_tab, sin_tab, n_tp, with_sum, parts, buffers):
    rows, width = hidden.shape
    block, anywhere = pl.BlockSpec(memory_space=pltpu.VMEM), pl.BlockSpec(memory_space=pl.ANY)
    n_att = 4 * PART
    out_shape = [jax.ShapeDtypeStruct((n_att, width), F32), jax.ShapeDtypeStruct((n_att, width), BF), jax.ShapeDtypeStruct((2, width), F32), jax.ShapeDtypeStruct((3 * HEADS, HEAD), F32)]
    scratch = [pltpu.VMEM((n_att, width), BF), pltpu.SemaphoreType.DMA, pltpu.VMEM((2 * HEADS, 2 * rows, HEAD), F32), pltpu.VMEM((2 * HEADS, rows, HEAD), F32),
               pltpu.VMEM((3 * HEADS, rows, HEAD), BF), pltpu.VMEM((rows, width), BF), pltpu.SemaphoreType.DMA((2,)), pltpu.SemaphoreType.DMA((2,))]
    if with_sum:
        out_shape = [jax.ShapeDtypeStruct((rows, width), BF)] + out_shape
        scratch += [pltpu.VMEM((rows, width), BF)] + line_scratch(rows, width)
    specs = [block] * len(out_shape)
    extra, aliases = [], {}
    for prod, prod_b in parts:
        extra += [prod, prod_b]
        scratch += stage_scratch(*prod.shape)
    for index, (prod, _) in enumerate(parts):
        if buffers[index] is not None:
            aliases[14 + len(extra)] = len(out_shape) + index
            extra.append(buffers[index])
    out_shape += [jax.ShapeDtypeStruct(prod.shape, F32) for prod, _ in parts]
    specs += [anywhere] * len(parts)
    return pl.pallas_call(
        functools.partial(att_back_kernel, n_tp, layer, with_sum, len(parts)),
        out_shape=tuple(out_shape),
        in_specs=[block] * 7 + [anywhere] * 4 + [block] * 3 + [anywhere] * len(extra),
        out_specs=tuple(specs),
        scratch_shapes=scratch,
        input_output_aliases=aliases,
        compiler_params=pltpu.CompilerParams(collective_id=3 + layer, has_side_effects=True, vmem_limit_bytes=LIMIT),
        cost_estimate=pl.CostEstimate(flops=45_000_000_000, bytes_accessed=12_000_000, transcendentals=0),
    )(grad, hidden, gx, query, kv_all, context, lse, *options, vec, cos_tab, sin_tab, *extra)


def causal_mask(core, block, n_keys):
    row = lax.broadcasted_iota(jnp.int32, (BLOCK, n_keys), 0)
    col = lax.broadcasted_iota(jnp.int32, (BLOCK, n_keys), 1)
    part = col // BLOCK
    starts = (core, 1 - core, 3 - core, 2 + core)
    start = jnp.where(part == 0, starts[0], jnp.where(part == 1, starts[1], jnp.where(part == 2, starts[2], starts[3])))
    mine = core if block == 0 else 3 - core
    return mine * BLOCK + row >= start * BLOCK + (col - part * BLOCK)


def final_kernel(n_pp, n_tp, n_norm, rows_ref, prod_ref, prod_b_ref, buffer_ref, out_ref, result_ref, box, stage_sum, norm_box, send_a, recv_a, send_b, recv_b, *own):
    stage, rank = lax.axis_index('pp'), lax.axis_index('tp')
    barrier = pltpu.get_barrier_semaphore()
    for step in range(1, n_pp):
        pl.semaphore_signal(barrier, inc=1, device_id={'pp': lax.rem(stage + step, n_pp)}, device_id_type=MESH_ID)
    for step in range(1, n_tp):
        pl.semaphore_signal(barrier, inc=1, device_id={'tp': lax.rem(rank + step, n_tp)}, device_id_type=MESH_ID)
    pl.semaphore_wait(barrier, n_pp + n_tp - 2)
    last = StageSum(0, prod_ref, prod_b_ref, result_ref, *own)
    last.begin()
    sends = []
    for step in range(1, n_pp):
        peer = lax.rem(stage + step, n_pp)
        copy = pltpu.make_async_remote_copy(
            src_ref=rows_ref.at[peer], dst_ref=box.at[step - 1], send_sem=send_a.at[step - 1],
            recv_sem=recv_a.at[step - 1], device_id={'pp': peer}, device_id_type=MESH_ID)
        copy.start()
        sends.append(copy)
    last.relay()
    total = rows_ref[stage]
    for step, copy in enumerate(sends):
        copy.wait_recv()
        total += box[step]
    stage_sum[...] = total
    norm_box[rank] = total[:n_norm]
    shares = []
    for step in range(1, n_tp):
        copy = pltpu.make_async_remote_copy(
            src_ref=stage_sum.at[pl.ds(0, n_norm)], dst_ref=norm_box.at[rank], send_sem=send_b.at[step - 1],
            recv_sem=recv_b.at[step - 1], device_id={'tp': lax.rem(rank + step, n_tp)}, device_id_type=MESH_ID)
        copy.start()
        shares.append(copy)
    for copy in shares:
        copy.wait()
    norms = norm_box[0]
    for index in range(1, n_tp):
        norms += norm_box[index]
    out_ref[:n_norm, :] = norms
    out_ref[n_norm:, :] = total[n_norm:]
    for copy in sends:
        copy.wait_send()
    last.end()


def sum_final(rows, prod, prod_b, buffer, n_tp):
    n_pp, count, width = rows.shape
    n_norm = count // 2
    anywhere = pl.BlockSpec(memory_space=pl.ANY)
    return pl.pallas_call(
        functools.partial(final_kernel, n_pp, n_tp, n_norm),
        out_shape=(jax.ShapeDtypeStruct((count, width), F32), jax.ShapeDtypeStruct(prod.shape, F32)),
        in_specs=[pl.BlockSpec(memory_space=pltpu.VMEM)] + [anywhere] * 3,
        out_specs=(pl.BlockSpec(memory_space=pltpu.VMEM), anywhere),
        scratch_shapes=[pltpu.VMEM((n_pp - 1, count, width), F32), pltpu.VMEM((count, width), F32), pltpu.VMEM((n_tp, n_norm, width), F32),
                        pltpu.SemaphoreType.DMA((n_pp - 1,)), pltpu.SemaphoreType.DMA((n_pp - 1,)), pltpu.SemaphoreType.DMA((n_tp - 1,)), pltpu.SemaphoreType.DMA((n_tp - 1,))]
        + stage_scratch(*prod.shape),
        input_output_aliases={3: 1},
        compiler_params=pltpu.CompilerParams(collective_id=2, has_side_effects=True, vmem_limit_bytes=LIMIT),
        cost_estimate=pl.CostEstimate(flops=20_000_000_000, bytes_accessed=8_000_000, transcendentals=0),
    )(rows, prod, prod_b, buffer)


def solution(mesh):
    n_stages = mesh.shape['pp']
    n_tp = mesh.shape['tp']
    swap_core = [(stage, stage ^ 1) for stage in range(n_stages)]

    def device_fn(x_in, g_out, ln1_gain, ln1_bias, w_qkv, b_qkv, w_out, b_out, ln2_gain, ln2_bias, w_up, b_up, w_down, b_down):
        stage = lax.axis_index('pp')
        core = stage % 2
        seq_len, width = x_in.shape[2:]
        ffn = w_up.shape[2]

        def own_tokens(array):
            blocks = lax.dynamic_index_in_dim(array, stage // 2, 0, keepdims=False).reshape(4, BLOCK, width)
            first = lax.dynamic_index_in_dim(blocks, core, 0, keepdims=False)
            second = lax.dynamic_index_in_dim(blocks, 3 - core, 0, keepdims=False)
            return jnp.concatenate([first, second], axis=0).astype(BF)

        hidden = own_tokens(x_in)
        grad = own_tokens(g_out)

        half_rot = HEAD // 8
        inv_freq = ROPE_BASE ** (-(jnp.arange(half_rot, dtype=F32) * 2.0) / (2 * half_rot))
        spot = jnp.concatenate([core * BLOCK + jnp.arange(BLOCK), (3 - core) * BLOCK + jnp.arange(BLOCK)])
        angles = spot.astype(F32)[:, None] * inv_freq[None, :]
        still = jnp.zeros((ROWS, HEAD - 2 * half_rot), F32)
        cos_tab = jnp.tile(jnp.concatenate([jnp.cos(angles), jnp.cos(angles), still + 1.0], axis=1), (1, 1))
        sin_tab = jnp.tile(jnp.concatenate([jnp.sin(angles), jnp.sin(angles), still], axis=1), (1, 1))

        wq_rows = jnp.transpose(w_qkv[0], (2, 1, 3, 0)).reshape(3 * PART, width)
        bundle = jnp.concatenate([wq_rows, w_out[0].reshape(PART, width), w_up[0], w_down[0]], axis=0)
        bias_qkv = jnp.transpose(b_qkv[0], (1, 0, 2)).reshape(3 * PART).astype(F32)
        pad = jnp.zeros((width - 3 * PART,), F32)
        vectors = jnp.stack([ln1_gain[0], ln1_bias[0], ln2_gain[0], ln2_bias[0], b_out[0].astype(F32) + b_down[0].astype(F32), b_up[0].astype(F32), jnp.concatenate([bias_qkv, pad]), jnp.zeros((width,), F32)])

        n_att = 4 * PART
        pair_a, pair_b = [(0, 2), (2, 0)], [(1, 3), (3, 1)]
        first_wave = lax.ppermute(bundle, 'pp', pair_a)
        later, first_wave = tie(bundle, first_wave)
        second_wave = lax.ppermute(later, 'pp', pair_b)
        partner = lax.ppermute(bundle, 'pp', swap_core)
        all_vectors = lax.all_gather(vectors, 'pp')
        first_wave, hidden, grad, cos_tab, sin_tab, all_vectors = tie(first_wave, hidden, grad, cos_tab, sin_tab, all_vectors)
        first_pass = lax.ppermute(first_wave, 'pp', [(2, 3), (0, 1)])
        sources = {0: (bundle, partner, first_wave, first_pass), 2: (first_wave, first_pass, bundle, partner)}
        saved = []
        for layer in range(n_stages):
            vec = all_vectors[layer]
            bias_q = vec[6, :3 * PART].reshape(3 * HEADS, HEAD)
            last = layer == n_stages - 1
            result, query, kv_all, context, lse, pre_act = forward_layer(hidden, sources[layer], vec, bias_q, cos_tab, sin_tab, n_tp, not last)
            saved.append((hidden, query, kv_all, context, lse, pre_act))
            if last:
                summed = lax.psum(result, 'tp')
                break
            hidden = result
            if layer == 0:
                hidden, second_wave = tie(hidden, second_wave)
                second_pass = lax.ppermute(second_wave, 'pp', [(3, 2), (1, 0)])
                sources[1] = (partner, bundle, second_pass, second_wave)
                sources[3] = (second_pass, second_wave, partner, bundle)

        small, prod = {}, {}
        grad_att = grad_mlp = None
        for layer in reversed(range(n_stages)):
            hidden, query, kv_all, context, lse, pre_act = saved[layer]
            vec = all_vectors[layer]
            gx, prod_m, prod_m_b, small_m = mlp_back(grad, hidden, pre_act, sources[layer], vec, n_tp)
            parts, buffers = [(prod_m, prod_m_b)], [grad_mlp]
            if layer < n_stages - 1:
                parts.append(prod[layer + 1])
                buffers.append(grad_att)
            out = att_back(layer, grad, hidden, gx, query, kv_all, context, lse, sources[layer], vec, cos_tab, sin_tab, n_tp, layer > 0, parts, buffers)
            if layer:
                grad, out = out[0], out[1:]
            prod[layer] = (out[0], out[1])
            small_a, bias_a, grad_mlp = out[2:5]
            if layer < n_stages - 1:
                grad_att = out[5]
            small[layer] = jnp.concatenate([small_a, small_m, jnp.concatenate([bias_a.reshape(1, 3 * PART), pad[None]], axis=1), jnp.zeros((1, width), F32)], axis=0)
            if layer == n_stages - 1:
                grad, summed = tie(grad, summed)
        small, grad_att = sum_final(jnp.stack([small[layer] for layer in range(n_stages)]), *prod[0], grad_att, n_tp)
        norms = small

        final = (saved[-1][0].astype(F32) + all_vectors[-1][4:5] + summed.astype(F32)).astype(BF)
        gathered = lax.all_gather(final, 'pp').reshape(2, 2, 2, BLOCK, width)
        y_out = jnp.stack([gathered[:, 0, 0], gathered[:, 1, 0], gathered[:, 1, 1], gathered[:, 0, 1]], axis=1).reshape(x_in.shape)

        grad_qkv = jnp.transpose(grad_att[:3 * PART].reshape(3, HEADS, HEAD, width), (3, 1, 0, 2))
        grads = (
            norms[0], norms[1], grad_qkv, jnp.transpose(small[6, :3 * PART].reshape(3, HEADS, HEAD), (1, 0, 2)),
            grad_att[3 * PART:].reshape(HEADS, HEAD, width), small[4], norms[2], norms[3],
            grad_mlp[:width], small[5], grad_mlp[width:], small[4])
        return tuple([y_out] + [item[None] for item in grads])

    return jax.shard_map(device_fn, mesh=mesh, in_specs=(P('dp'), P('dp')) + STAGE_SPECS, out_specs=(P('dp'),) + GRAD_SPECS, check_vma=False)
```

```python
import functools

import jax
import jax.numpy as jnp
from jax import lax
from jax.experimental import pallas as pl
from jax.experimental.pallas import tpu as pltpu
from jax.sharding import PartitionSpec as P

BF = jnp.bfloat16
F32 = jnp.float32
ROPE_BASE = 10000.0
LN_EPS = 1e-5
HEADS = 3
HEAD = 64
PART = HEADS * HEAD
BLOCK = 256
ROWS = 2 * BLOCK
STAGE_SPECS = (P('pp', None), P('pp', None), P('pp', None, 'tp', None, None), P('pp', 'tp', None, None), P('pp', 'tp', None, None), P('pp', None), P('pp', None), P('pp', None), P('pp', None, 'tp'), P('pp', 'tp'), P('pp', 'tp', None), P('pp', None))
GRAD_SPECS = (P(('dp', 'pp'), None), P(('dp', 'pp'), None), P(('dp', 'pp'), None, 'tp', None, None), P(('dp', 'pp'), 'tp', None, None), P(('dp', 'pp'), 'tp', None, None), P(('dp', 'pp'), None), P(('dp', 'pp'), None), P(('dp', 'pp'), None), P(('dp', 'pp'), None, 'tp'), P(('dp', 'pp'), 'tp'), P(('dp', 'pp'), 'tp', None), P(('dp', 'pp'), None))
CHUNKS = 8
SMALL = 24
LIMIT = 60 * 2 ** 20
MESH_ID = pl.DeviceIdType.MESH


def tie(*values):
    return lax.optimization_barrier(values)


def dot(left, right, left_dim, right_dim):
    return lax.dot_general(left, right, (((left_dim,), (right_dim,)), ((), ())), preferred_element_type=F32)


def normalise(hidden):
    hidden_f = hidden.astype(F32)
    center = hidden_f - jnp.mean(hidden_f, axis=-1, keepdims=True)
    scale = lax.rsqrt(jnp.mean(center * center, axis=-1, keepdims=True) + LN_EPS)
    return center * scale, scale


def turn_matrix(width, transposed):
    row = lax.broadcasted_iota(jnp.int32, (width, width), 0)
    col = lax.broadcasted_iota(jnp.int32, (width, width), 1)
    if transposed:
        row, col = col, row
    dim = col % HEAD
    minus = (dim < 8) & (row == col + 8)
    plus = (dim >= 8) & (dim < 16) & (row == col - 8)
    return (plus.astype(F32) - minus.astype(F32)).astype(BF)


def rotate_head(values, cos_tab, sin_tab, transposed):
    turned = dot(values, turn_matrix(HEAD, transposed), 1, 0)
    return (values.astype(F32) * cos_tab + turned * sin_tab).astype(BF)


def block_rows(block):
    return slice(block * BLOCK, (block + 1) * BLOCK)


def pick_weights(stage, options, first, count, scratch, sem):
    for index, option in enumerate(options):
        @pl.when(stage == index)
        def fetch():
            pltpu.make_async_copy(option.at[pl.ds(first, count)], scratch, sem).start()

    return pltpu.make_async_copy(options[0].at[pl.ds(first, count)], scratch, sem).wait


def meet(n_tp, with_sum, with_core, with_stage=False):
    rank, stage = lax.axis_index('tp'), lax.axis_index('pp')
    barrier = pltpu.get_barrier_semaphore()
    count = 0
    if with_core:
        pl.semaphore_signal(barrier, inc=1, device_id={'pp': stage + 1 - 2 * lax.rem(stage, 2)}, device_id_type=MESH_ID)
        count = 1
    if with_stage:
        pl.semaphore_signal(barrier, inc=1, device_id={'pp': lax.rem(stage + 2, 4)}, device_id_type=MESH_ID)
        count += 1
    if with_sum:
        is_inner = lax.rem((rank + 1) // 2, 2)
        near = rank + 1 - 2 * lax.rem(rank, 2)
        pl.semaphore_signal(barrier, inc=1, device_id={'tp': near}, device_id_type=MESH_ID)

        @pl.when(is_inner == 1)
        def greet():
            pl.semaphore_signal(barrier, inc=1, device_id={'tp': n_tp - 1 - rank}, device_id_type=MESH_ID)

        count = count + 1 + is_inner
    pl.semaphore_wait(barrier, count)


class LineSum:
    def __init__(self, n_tp, part, base, out, inbox, half, across, sems):
        self.part, self.base, self.out, self.inbox, self.half, self.across, self.sems = part, base, out, inbox, half, across, sems
        rank = lax.axis_index('tp')
        self.is_inner = lax.rem((rank + 1) // 2, 2)
        self.near = rank + 1 - 2 * lax.rem(rank, 2)
        self.mirror = n_tp - 1 - rank
        self.n_chunks = CHUNKS
        self.size = out.shape[0] // CHUNKS

    def span(self, chunk):
        return pl.ds(chunk * self.size, self.size)

    def copy(self, kind, chunk):
        source, target, device = ((self.part, self.inbox, self.near), (self.half, self.across, self.mirror), (self.out, self.out, self.near))[kind]
        return pltpu.make_async_remote_copy(
            src_ref=source.at[self.span(chunk)], dst_ref=target.at[self.span(chunk)], send_sem=self.sems[2 * kind].at[chunk],
            recv_sem=self.sems[2 * kind + 1].at[chunk], device_id={'tp': device}, device_id_type=MESH_ID)

    def offer(self, chunks):
        @pl.when(self.is_inner == 0)
        def start():
            for chunk in chunks:
                self.copy(0, chunk).start()

    def finish(self, chunk):
        rows = self.span(chunk)
        self.copy(1, chunk).wait_recv()
        both = self.half[rows, :].astype(F32) + self.across[rows, :].astype(F32)
        self.out[rows, :] = (self.base(rows) + both).astype(BF)
        self.copy(2, chunk).start()

    def step(self, chunk):
        @pl.when(self.is_inner == 1)
        def merge():
            rows = self.span(chunk)
            self.copy(0, chunk).wait_recv()
            self.half[rows, :] = (self.part[rows, :].astype(F32) + self.inbox[rows, :].astype(F32)).astype(BF)
            self.copy(1, chunk).start()

    def close(self, chunk):
        @pl.when(self.is_inner == 1)
        def end():
            self.finish(chunk)

    def drain(self):
        @pl.when(self.is_inner == 1)
        def inner_end():
            for chunk in range(self.n_chunks):
                self.copy(1, chunk).wait_send()
                self.copy(2, chunk).wait_send()

        @pl.when(self.is_inner == 0)
        def outer_end():
            for chunk in range(self.n_chunks):
                self.copy(2, chunk).wait_recv()
                self.copy(0, chunk).wait_send()


def line_scratch(rows, width):
    return [pltpu.VMEM((rows, width), BF)] * 3 + [pltpu.SemaphoreType.DMA((CHUNKS,))] * 6


class StageSum:
    def __init__(self, layer, prod, prod_b, result, staged, near, far, half, sems):
        self.prod, self.prod_b, self.result, self.staged, self.near, self.far, self.half, self.sems = prod, prod_b, result, staged, near, far, half, sems
        self.stage = lax.axis_index('pp')
        self.is_owner = self.stage == layer
        self.is_relay = self.stage == (layer ^ 2)
        self.is_giver = lax.rem(self.stage, 2) != layer % 2
        self.is_keeper = lax.rem(self.stage, 2) == layer % 2

    def load(self):
        return pltpu.make_async_copy(self.prod, self.staged, self.sems.at[0])

    def store(self):
        return pltpu.make_async_copy(self.staged, self.result, self.sems.at[1])

    def hand(self):
        return pltpu.make_async_remote_copy(
            src_ref=self.prod_b, dst_ref=self.near, send_sem=self.sems.at[2], recv_sem=self.sems.at[3],
            device_id={'pp': self.stage + 1 - 2 * lax.rem(self.stage, 2)}, device_id_type=MESH_ID)

    def cross(self):
        return pltpu.make_async_remote_copy(
            src_ref=self.half, dst_ref=self.far, send_sem=self.sems.at[4], recv_sem=self.sems.at[5],
            device_id={'pp': lax.rem(self.stage + 2, 4)}, device_id_type=MESH_ID)

    def blocks(self):
        return [pl.ds(first, BLOCK) for first in range(0, self.staged.shape[0], BLOCK)]

    def begin(self):
        @pl.when(self.is_giver)
        def give():
            self.hand().start()

        if self.prod is not None:
            @pl.when(self.is_keeper)
            def keep():
                self.load().start()

    def ready(self):
        if self.prod is not None:
            self.load().wait()

    def relay(self):
        @pl.when(self.is_relay)
        def send_on():
            self.ready()
            self.hand().wait_recv()
            for rows in self.blocks():
                self.half[rows, :] = (self.staged[rows, :] + self.near[rows, :].astype(F32)).astype(BF)
            self.cross().start()

    def end(self):
        @pl.when(self.is_owner)
        def close():
            self.ready()
            self.hand().wait_recv()
            self.cross().wait_recv()
            for rows in self.blocks():
                self.staged[rows, :] += self.near[rows, :].astype(F32) + self.far[rows, :].astype(F32)
            self.store().start()
            self.store().wait()

        @pl.when(self.is_relay)
        def relayed():
            self.cross().wait_send()

        @pl.when(self.is_giver)
        def given():
            self.hand().wait_send()


def stage_scratch(rows, width):
    return [pltpu.VMEM((rows, width), F32)] + [pltpu.VMEM((rows, width), BF)] * 3 + [pltpu.SemaphoreType.DMA((6,))]


def forward_kernel(n_tp, with_sum, h_ref, opt0, opt1, opt2, opt3, vec_ref, bq_ref, cos_ref, sin_ref,
                   out_ref, q_ref, kv_ref, ctx_ref, lse_ref, pre_ref, weights, w_sem, active, kv_send, kv_recv, *line_refs):
    stage = lax.axis_index('pp')
    core = lax.rem(stage, 2)
    width = h_ref.shape[1]
    wait_weights = pick_weights(stage, (opt0, opt1, opt2, opt3), 0, weights.shape[0], weights, w_sem)
    meet(n_tp, with_sum, True)
    wait_weights()

    def project(normed, index):
        return (dot(normed, weights[index * HEAD:(index + 1) * HEAD, :], 1, 1) + bq_ref[index:index + 1, :]).astype(BF)

    swaps = []
    for block in range(2):
        rows = block_rows(block)
        xhat, _ = normalise(h_ref[rows, :])
        normed_a = (xhat * vec_ref[0:1, :] + vec_ref[1:2, :]).astype(BF)
        active[rows, :] = (xhat * vec_ref[2:3, :] + vec_ref[3:4, :]).astype(BF)
        cos_tab, sin_tab = cos_ref[rows, :], sin_ref[rows, :]
        place = slice(2 * block * BLOCK, (2 * block + 1) * BLOCK)
        for head in range(HEADS):
            q_ref[head, rows, :] = rotate_head(project(normed_a, head), cos_tab, sin_tab, False)
            kv_ref[head, place, :] = rotate_head(project(normed_a, HEADS + head), cos_tab, sin_tab, False)
            kv_ref[HEADS + head, place, :] = project(normed_a, 2 * HEADS + head)
        copy = pltpu.make_async_remote_copy(
            src_ref=kv_ref.at[:, pl.ds(2 * block * BLOCK, BLOCK), :], dst_ref=kv_ref.at[:, pl.ds((2 * block + 1) * BLOCK, BLOCK), :],
            send_sem=kv_send.at[block], recv_sem=kv_recv.at[block],
            device_id={'pp': stage + 1 - 2 * core}, device_id_type=MESH_ID)
        copy.start()
        swaps.append(copy)
    def grow(block):
        rows = block_rows(block)
        pre_act = dot(active[rows, :], weights[4 * PART:4 * PART + width, :], 1, 0) + vec_ref[5:6, :]
        pre_ref[rows, :] = pre_act
        active[rows, :] = (0.5 * pre_act * (1.0 + lax.erf(pre_act * (2.0 ** -0.5)))).astype(BF)

    grow(0)
    for copy in swaps:
        copy.wait_recv()
    if with_sum:
        part_ref = line_refs[0]
        line = LineSum(n_tp, part_ref, lambda rows: h_ref[rows, :].astype(F32) + vec_ref[4:5, :], out_ref, *line_refs[1:4], line_refs[4:])
    else:
        part_ref = out_ref
    for block in range(2):
        rows = block_rows(block)
        n_keys = (2, 4)[block] * BLOCK
        mask = causal_mask(core, block, n_keys)
        if block:
            grow(1)
        part = dot(active[rows, :], weights[4 * PART + width:, :], 1, 0)
        for head in range(HEADS):
            scores = dot(q_ref[head, rows, :], kv_ref[head, :n_keys, :], 1, 1) * (HEAD ** -0.5)
            scores = jnp.where(mask, scores, -1e30)
            top = jnp.max(scores, axis=-1, keepdims=True)
            expo = jnp.exp(scores - top)
            total = jnp.sum(expo, axis=-1, keepdims=True)
            probs = (expo / total).astype(BF)
            context = dot(probs, kv_ref[HEADS + head, :n_keys, :], 1, 0).astype(BF)
            ctx_ref[head, rows, :] = context
            lse_ref[head, rows, :] = top + jnp.log(total)
            part += dot(context, weights[3 * PART + head * HEAD:3 * PART + (head + 1) * HEAD, :], 1, 0)
            if with_sum and block:
                line.step(head)
                if head:
                    line.close(head - 1)
        part_ref[rows, :] = part.astype(BF)
        if with_sum:
            line.offer(range(block * CHUNKS // 2, (block + 1) * CHUNKS // 2))
    if with_sum:
        for chunk in range(HEADS, CHUNKS):
            line.step(chunk)
            line.close(chunk - 1)
        line.close(CHUNKS - 1)
        line.drain()
    for copy in swaps:
        copy.wait_send()


def forward_layer(hidden, options, vec, bias_q, cos_tab, sin_tab, n_tp, with_sum):
    rows, width = hidden.shape
    block, anywhere = pl.BlockSpec(memory_space=pltpu.VMEM), pl.BlockSpec(memory_space=pl.ANY)
    scratch = [pltpu.VMEM(options[0].shape, BF), pltpu.SemaphoreType.DMA, pltpu.VMEM((rows, width), BF), pltpu.SemaphoreType.DMA((2,)), pltpu.SemaphoreType.DMA((2,))]
    if with_sum:
        scratch += [pltpu.VMEM((rows, width), BF)] + line_scratch(rows, width)
    return pl.pallas_call(
        functools.partial(forward_kernel, n_tp, with_sum),
        out_shape=(jax.ShapeDtypeStruct((rows, width), BF), jax.ShapeDtypeStruct((HEADS, rows, HEAD), BF), jax.ShapeDtypeStruct((2 * HEADS, 2 * rows, HEAD), BF),
                   jax.ShapeDtypeStruct((HEADS, rows, HEAD), BF), jax.ShapeDtypeStruct((HEADS, rows, 1), F32), jax.ShapeDtypeStruct((rows, width), F32)),
        in_specs=[block] + [anywhere] * 4 + [block] * 4,
        out_specs=tuple([block] * 6),
        scratch_shapes=scratch,
        compiler_params=pltpu.CompilerParams(collective_id=0 if with_sum else 1, has_side_effects=True, vmem_limit_bytes=LIMIT),
        cost_estimate=pl.CostEstimate(flops=40_000_000_000, bytes_accessed=8_000_000, transcendentals=0),
    )(hidden, *options, vec, bias_q, cos_tab, sin_tab)


def mlp_body(g_ref, h_ref, pre_ref, vec_ref, weights, base, gx_ref, prod_ref, prod_b_ref, small_ref, small_row, normed, gpre, active, hook):
    width = h_ref.shape[1]
    sums = [0.0] * 4
    for block in range(2):
        rows = block_rows(block)
        grad = g_ref[rows, :]
        pre_act = pre_ref[rows, :]
        gauss = 0.5 * (1.0 + lax.erf(pre_act * (2.0 ** -0.5)))
        active[rows, :] = (pre_act * gauss).astype(BF)
        slope = gauss + pre_act * jnp.exp(-0.5 * pre_act * pre_act) * 0.3989422804014327
        grad_pre = dot(grad, weights[base + width:base + 2 * width, :], 1, 1) * slope
        gpre[rows, :] = grad_pre.astype(BF)
        sums[3] += jnp.sum(grad_pre, axis=0, keepdims=True)
        sums[2] += jnp.sum(grad.astype(F32), axis=0, keepdims=True)
        xhat, _ = normalise(h_ref[rows, :])
        normed[rows, :] = (xhat * vec_ref[2:3, :] + vec_ref[3:4, :]).astype(BF)
        grad_m = dot(gpre[rows, :], weights[base:base + width, :], 1, 1)
        sums[0] += jnp.sum(grad_m * xhat, axis=0, keepdims=True)
        sums[1] += jnp.sum(grad_m, axis=0, keepdims=True)
        if gx_ref is not None:
            gx_ref[rows, :] = grad_m * vec_ref[2:3, :]
    for index, value in enumerate(sums):
        small_ref[small_row + index:small_row + index + 1, :] = value
    hook()
    for first in range(0, width, 256):
        for left, right, row in ((normed, gpre, 0), (active, g_ref, width)):
            value = dot(left[:, first:first + 256], right[...], 0, 0)
            prod_ref[row + first:row + first + 256, :] = value
            prod_b_ref[row + first:row + first + 256, :] = value.astype(BF)


def mlp_back_kernel(n_tp, g_ref, h_ref, pre_ref, opt0, opt1, opt2, opt3, vec_ref, gx_ref, prod_ref, prod_b_ref, small_ref,
                    weights, w_sem, normed, gpre, active):
    stage = lax.axis_index('pp')
    wait_weights = pick_weights(stage, (opt0, opt1, opt2, opt3), 4 * PART, weights.shape[0], weights, w_sem)
    wait_weights()
    mlp_body(g_ref, h_ref, pre_ref, vec_ref, weights, 0, gx_ref, prod_ref, prod_b_ref, small_ref, 0, normed, gpre, active, lambda: None)


def mlp_back(grad, hidden, pre_act, options, vec, n_tp):
    rows, width = hidden.shape
    block, anywhere = pl.BlockSpec(memory_space=pltpu.VMEM), pl.BlockSpec(memory_space=pl.ANY)
    return pl.pallas_call(
        functools.partial(mlp_back_kernel, n_tp),
        out_shape=(jax.ShapeDtypeStruct((rows, width), F32), jax.ShapeDtypeStruct((2 * width, width), F32), jax.ShapeDtypeStruct((2 * width, width), BF), jax.ShapeDtypeStruct((4, width), F32)),
        in_specs=[block] * 3 + [anywhere] * 4 + [block],
        out_specs=tuple([block] * 4),
        scratch_shapes=[pltpu.VMEM((2 * width, width), BF), pltpu.SemaphoreType.DMA] + [pltpu.VMEM((rows, width), BF)] * 3,
        compiler_params=pltpu.CompilerParams(vmem_limit_bytes=LIMIT),
        cost_estimate=pl.CostEstimate(flops=10_000_000_000, bytes_accessed=12_000_000, transcendentals=0),
    )(grad, hidden, pre_act, *options, vec)


def attention_body(g_ref, q_ref, kv_ref, lse_ref, weights, dqkv, dkv, core, between):
    for block in (1, 0):
        rows = block_rows(block)
        n_keys = (2, 4)[block] * BLOCK
        mask = causal_mask(core, block, n_keys)
        for head in range(HEADS):
            d_ctx = dot(g_ref[rows, :], weights[3 * PART + head * HEAD:3 * PART + (head + 1) * HEAD, :], 1, 1).astype(BF)
            q_part = q_ref[head, rows, :]
            k_part = kv_ref[head, :n_keys, :]
            scores = dot(q_part, k_part, 1, 1) * (HEAD ** -0.5)
            probs = jnp.where(mask, jnp.exp(scores - lse_ref[head, rows, :]), 0.0)
            dprobs = dot(d_ctx, kv_ref[HEADS + head, :n_keys, :], 1, 1).astype(BF).astype(F32)
            delta = jnp.sum(probs * dprobs, axis=-1, keepdims=True)
            dscores = (probs * (dprobs - delta) * (HEAD ** -0.5)).astype(BF)
            dqkv[head, rows, :] = dot(dscores, k_part, 1, 0).astype(BF)
            d_k = dot(dscores, q_part, 0, 0)
            d_v = dot(probs.astype(BF), d_ctx, 0, 0)
            if block == 1:
                dkv[head] = d_k
                dkv[HEADS + head] = d_v
            else:
                dkv[head, :n_keys, :] += d_k
                dkv[HEADS + head, :n_keys, :] += d_v
        if block == 1:
            between()


def project_back(h_ref, vec_ref, cos_ref, sin_ref, weights, dqkv, dkv, landed, normed, small_ref, bias_row, pass_on):
    sums = [0.0] * 2
    bias = [0.0] * (3 * HEADS)
    for block in range(2):
        rows = block_rows(block)
        own = slice(2 * block * BLOCK, (2 * block + 1) * BLOCK)
        cos_tab, sin_tab = cos_ref[rows, :], sin_ref[rows, :]
        grad_a = 0.0
        for head in range(HEADS):
            d_q = rotate_head(dqkv[head, rows, :], cos_tab, sin_tab, True)
            d_k = rotate_head((dkv[head, own, :] + landed[head, rows, :]).astype(BF), cos_tab, sin_tab, True)
            d_v = (dkv[HEADS + head, own, :] + landed[HEADS + head, rows, :]).astype(BF)
            for kind, value in enumerate((d_q, d_k, d_v)):
                index = kind * HEADS + head
                dqkv[index, rows, :] = value
                bias[index] += jnp.sum(value.astype(F32), axis=0, keepdims=True)
                grad_a += dot(value, weights[index * HEAD:(index + 1) * HEAD, :], 1, 0)
        xhat, scale = normalise(h_ref[rows, :])
        normed[rows, :] = (xhat * vec_ref[0:1, :] + vec_ref[1:2, :]).astype(BF)
        sums[0] += jnp.sum(grad_a * xhat, axis=0, keepdims=True)
        sums[1] += jnp.sum(grad_a, axis=0, keepdims=True)
        if pass_on is not None:
            pass_on(block, rows, grad_a, xhat, scale)
    for index, value in enumerate(sums):
        small_ref[index:index + 1, :] = value
    for index, value in enumerate(bias):
        small_ref[bias_row + index:bias_row + index + 1, :HEAD] = value


def att_back_kernel(n_tp, layer, with_sum, n_red, g_ref, h_ref, gx_ref, q_ref, kv_ref, ctx_ref, lse_ref, opt0, opt1, opt2, opt3, vec_ref, cos_ref, sin_ref, *refs):
    n_in = (2, 4)[n_red - 1] + (0 if layer == 3 else n_red if layer < 2 else 1)
    given, refs = refs[:n_in], refs[n_in:]
    if with_sum:
        out_ref, refs = refs[0], refs[1:]
    prod_ref, prod_b_ref, small_ref = refs[:3]
    results, refs = refs[3:3 + n_red], refs[3 + n_red:]
    small_ref[...] = jnp.zeros_like(small_ref)
    weights, w_sem, dkv, landed, dqkv, normed, kv_send, kv_recv = refs[:8]
    line_refs = refs[8:]
    reductions = []
    for index in range(n_red):
        own = line_refs[-5 * (n_red - index):][:5]
        reductions.append(StageSum(layer + index, given[2 * index], given[2 * index + 1], results[index], *own))
    line_refs = line_refs[:len(line_refs) - 5 * n_red]
    stage = lax.axis_index('pp')
    core = lax.rem(stage, 2)
    wait_weights = pick_weights(stage, (opt0, opt1, opt2, opt3), 0, weights.shape[0], weights, w_sem)
    meet(n_tp, with_sum, True, True)
    for item in reductions:
        item.begin()
    wait_weights()
    def between():
        for item in reversed(reductions):
            item.relay()

    attention_body(g_ref, q_ref, kv_ref, lse_ref, weights, dqkv, dkv, core, between)
    swaps = []
    for block in range(2):
        copy = pltpu.make_async_remote_copy(
            src_ref=dkv.at[:, pl.ds((2 * block + 1) * BLOCK, BLOCK), :], dst_ref=landed.at[:, pl.ds(block * BLOCK, BLOCK), :],
            send_sem=kv_send.at[block], recv_sem=kv_recv.at[block],
            device_id={'pp': stage + 1 - 2 * core}, device_id_type=MESH_ID)
        copy.start()
        swaps.append(copy)
    if with_sum:
        part_ref = line_refs[0]
        line = LineSum(n_tp, part_ref, lambda rows: g_ref[rows, :].astype(F32), out_ref, *line_refs[1:4], line_refs[4:])
    for copy in swaps:
        copy.wait_recv()

    def pass_on(block, rows, grad_a, xhat, scale):
        grad_x = grad_a * vec_ref[0:1, :] + gx_ref[rows, :]
        branch = scale * (grad_x - jnp.mean(grad_x, axis=-1, keepdims=True) - xhat * jnp.mean(grad_x * xhat, axis=-1, keepdims=True))
        part_ref[rows, :] = branch.astype(BF)
        line.offer(range(block * CHUNKS // 2, (block + 1) * CHUNKS // 2))

    project_back(h_ref, vec_ref, cos_ref, sin_ref, weights, dqkv, dkv, landed, normed, small_ref, 8, pass_on)

    def product(index):
        value = dot(dqkv[index], normed[...], 0, 0) if index < 3 * HEADS else dot(ctx_ref[index - 3 * HEADS], g_ref[...], 0, 0)
        prod_ref[index * HEAD:(index + 1) * HEAD, :] = value
        prod_b_ref[index * HEAD:(index + 1) * HEAD, :] = value.astype(BF)

    n_prod = 4 * HEADS
    for chunk in range(CHUNKS):
        if with_sum:
            line.step(chunk)
        for index in range(chunk * n_prod // CHUNKS, (chunk + 1) * n_prod // CHUNKS):
            product(index)
        if with_sum and chunk:
            line.close(chunk - 1)
    if with_sum:
        line.close(CHUNKS - 1)
        line.drain()
    for copy in swaps:
        copy.wait_send()
    for item in reversed(reductions):
        item.end()


def att_back(layer, grad, hidden, gx, query, kv_all, context, lse, options, vec, cos_tab, sin_tab, n_tp, with_sum, parts, buffers):
    rows, width = hidden.shape
    block, anywhere = pl.BlockSpec(memory_space=pltpu.VMEM), pl.BlockSpec(memory_space=pl.ANY)
    n_att = 4 * PART
    out_shape = [jax.ShapeDtypeStruct((n_att, width), F32), jax.ShapeDtypeStruct((n_att, width), BF), jax.ShapeDtypeStruct((SMALL, width), F32)]
    scratch = [pltpu.VMEM((n_att, width), BF), pltpu.SemaphoreType.DMA, pltpu.VMEM((2 * HEADS, 2 * rows, HEAD), F32), pltpu.VMEM((2 * HEADS, rows, HEAD), F32),
               pltpu.VMEM((3 * HEADS, rows, HEAD), BF), pltpu.VMEM((rows, width), BF), pltpu.SemaphoreType.DMA((2,)), pltpu.SemaphoreType.DMA((2,))]
    if with_sum:
        out_shape = [jax.ShapeDtypeStruct((rows, width), BF)] + out_shape
        scratch += [pltpu.VMEM((rows, width), BF)] + line_scratch(rows, width)
    specs = [block] * len(out_shape)
    extra, aliases = [], {}
    for prod, prod_b in parts:
        extra += [prod, prod_b]
        scratch += stage_scratch(*prod.shape)
    for index, (prod, _) in enumerate(parts):
        if buffers[index] is not None:
            aliases[14 + len(extra)] = len(out_shape) + index
            extra.append(buffers[index])
    out_shape += [jax.ShapeDtypeStruct(prod.shape, F32) for prod, _ in parts]
    specs += [anywhere] * len(parts)
    return pl.pallas_call(
        functools.partial(att_back_kernel, n_tp, layer, with_sum, len(parts)),
        out_shape=tuple(out_shape),
        in_specs=[block] * 7 + [anywhere] * 4 + [block] * 3 + [anywhere] * len(extra),
        out_specs=tuple(specs),
        scratch_shapes=scratch,
        input_output_aliases=aliases,
        compiler_params=pltpu.CompilerParams(collective_id=3 + layer, has_side_effects=True, vmem_limit_bytes=LIMIT),
        cost_estimate=pl.CostEstimate(flops=45_000_000_000, bytes_accessed=12_000_000, transcendentals=0),
    )(grad, hidden, gx, query, kv_all, context, lse, *options, vec, cos_tab, sin_tab, *extra)


def causal_mask(core, block, n_keys):
    row = lax.broadcasted_iota(jnp.int32, (BLOCK, n_keys), 0)
    col = lax.broadcasted_iota(jnp.int32, (BLOCK, n_keys), 1)
    part = col // BLOCK
    starts = (core, 1 - core, 3 - core, 2 + core)
    start = jnp.where(part == 0, starts[0], jnp.where(part == 1, starts[1], jnp.where(part == 2, starts[2], starts[3])))
    mine = core if block == 0 else 3 - core
    return mine * BLOCK + row >= start * BLOCK + (col - part * BLOCK)


def first_layer_kernel(n_pp, n_tp, n_norm, g_ref, h_ref, pre_ref, q_ref, kv_ref, ctx_ref, lse_ref, opt0, opt1, opt2, opt3, vec_ref, cos_ref, sin_ref, rows_ref,
                       prev_ref, prev_b_ref, att_in, mlp_in, out_ref, att_ref, att_prev_ref, mlp_ref,
                       weights, w_sem, dkv, landed, dqkv, normed, kv_send, kv_recv, gpre, active,
                       prod_m, prod_m_b, near_m, far_m, sems_m, prod_a, prod_a_b, near_a, far_a, sems_a, staged_p, near_p, far_p, half_p, sems_p,
                       all_rows, box, stage_sum, norm_box, send_a, recv_a, send_b, recv_b):
    stage, rank = lax.axis_index('pp'), lax.axis_index('tp')
    core = lax.rem(stage, 2)
    wait_weights = pick_weights(stage, (opt0, opt1, opt2, opt3), 0, weights.shape[0], weights, w_sem)
    barrier = pltpu.get_barrier_semaphore()
    for step in range(1, n_pp):
        pl.semaphore_signal(barrier, inc=1, device_id={'pp': lax.rem(stage + step, n_pp)}, device_id_type=MESH_ID)
    for step in range(1, n_tp):
        pl.semaphore_signal(barrier, inc=1, device_id={'tp': lax.rem(rank + step, n_tp)}, device_id_type=MESH_ID)
    pl.semaphore_wait(barrier, n_pp + n_tp - 2)
    before = StageSum(1, prev_ref, prev_b_ref, att_prev_ref, staged_p, near_p, far_p, half_p, sems_p)
    mlp = StageSum(0, None, prod_m_b, mlp_ref, prod_m, near_m, far_m, prod_m_b, sems_m)
    att = StageSum(0, None, prod_a_b, att_ref, prod_a, near_a, far_a, prod_a_b, sems_a)
    before.begin()
    wait_weights()
    small = all_rows.at[0]
    small[...] = jnp.zeros_like(small)
    all_rows[1:, :, :] = rows_ref[...]
    mlp_body(g_ref, h_ref, pre_ref, vec_ref, weights, 4 * PART, None, prod_m, prod_m_b, small, 2, normed, gpre, active, before.relay)
    mlp.begin()
    attention_body(g_ref, q_ref, kv_ref, lse_ref, weights, dqkv, dkv, core, mlp.relay)
    swaps = []
    for block in range(2):
        copy = pltpu.make_async_remote_copy(
            src_ref=dkv.at[:, pl.ds((2 * block + 1) * BLOCK, BLOCK), :], dst_ref=landed.at[:, pl.ds(block * BLOCK, BLOCK), :],
            send_sem=kv_send.at[block], recv_sem=kv_recv.at[block],
            device_id={'pp': stage + 1 - 2 * core}, device_id_type=MESH_ID)
        copy.start()
        swaps.append(copy)
    for head in range(HEADS):
        index = 3 * HEADS + head
        value = dot(ctx_ref[head], g_ref[...], 0, 0)
        prod_a[index * HEAD:(index + 1) * HEAD, :] = value
        prod_a_b[index * HEAD:(index + 1) * HEAD, :] = value.astype(BF)
    for copy in swaps:
        copy.wait_recv()
    project_back(h_ref, vec_ref, cos_ref, sin_ref, weights, dqkv, dkv, landed, normed, small, 8, None)
    for index in range(3 * HEADS):
        value = dot(dqkv[index], normed[...], 0, 0)
        prod_a[index * HEAD:(index + 1) * HEAD, :] = value
        prod_a_b[index * HEAD:(index + 1) * HEAD, :] = value.astype(BF)
    att.begin()
    sends = []
    for step in range(1, n_pp):
        peer = lax.rem(stage + step, n_pp)
        copy = pltpu.make_async_remote_copy(
            src_ref=all_rows.at[peer], dst_ref=box.at[step - 1], send_sem=send_a.at[step - 1],
            recv_sem=recv_a.at[step - 1], device_id={'pp': peer}, device_id_type=MESH_ID)
        copy.start()
        sends.append(copy)
    att.relay()
    total = all_rows[stage]
    for step, copy in enumerate(sends):
        copy.wait_recv()
        total += box[step]
    stage_sum[...] = total
    norm_box[rank] = total[:n_norm]
    shares = []
    for step in range(1, n_tp):
        copy = pltpu.make_async_remote_copy(
            src_ref=stage_sum.at[pl.ds(0, n_norm)], dst_ref=norm_box.at[rank], send_sem=send_b.at[step - 1],
            recv_sem=recv_b.at[step - 1], device_id={'tp': lax.rem(rank + step, n_tp)}, device_id_type=MESH_ID)
        copy.start()
        shares.append(copy)
    before.end()
    mlp.end()
    for copy in shares:
        copy.wait()
    norms = norm_box[0]
    for index in range(1, n_tp):
        norms += norm_box[index]
    out_ref[:n_norm, :] = norms
    out_ref[n_norm:, :] = total[n_norm:]
    for copy in sends + swaps:
        copy.wait_send()
    att.end()


def first_layer_back(grad, hidden, saved, options, vec, cos_tab, sin_tab, rows, previous, grad_att, grad_mlp, n_tp):
    query, kv_all, context, lse, pre_act = saved
    n_others, count, width = rows.shape
    n_pp, tokens, n_att = n_others + 1, hidden.shape[0], 4 * PART
    n_norm = 4
    block, anywhere = pl.BlockSpec(memory_space=pltpu.VMEM), pl.BlockSpec(memory_space=pl.ANY)

    def resident(n_rows):
        return [pltpu.VMEM((n_rows, width), F32)] + [pltpu.VMEM((n_rows, width), BF)] * 3 + [pltpu.SemaphoreType.DMA((6,))]

    return pl.pallas_call(
        functools.partial(first_layer_kernel, n_pp, n_tp, n_norm),
        out_shape=(jax.ShapeDtypeStruct((count, width), F32), jax.ShapeDtypeStruct((n_att, width), F32), jax.ShapeDtypeStruct((n_att, width), F32), jax.ShapeDtypeStruct((2 * width, width), F32)),
        in_specs=[block] * 7 + [anywhere] * 4 + [block] * 4 + [anywhere] * 4,
        out_specs=(block, anywhere, anywhere, anywhere),
        scratch_shapes=[pltpu.VMEM((n_att + 2 * width, width), BF), pltpu.SemaphoreType.DMA, pltpu.VMEM((2 * HEADS, 2 * tokens, HEAD), F32), pltpu.VMEM((2 * HEADS, tokens, HEAD), F32),
                        pltpu.VMEM((3 * HEADS, tokens, HEAD), BF), pltpu.VMEM((tokens, width), BF), pltpu.SemaphoreType.DMA((2,)), pltpu.SemaphoreType.DMA((2,)),
                        pltpu.VMEM((tokens, width), BF), pltpu.VMEM((tokens, width), BF)]
        + resident(2 * width) + resident(n_att) + stage_scratch(n_att, width)
        + [pltpu.VMEM((n_pp, count, width), F32), pltpu.VMEM((n_pp - 1, count, width), F32), pltpu.VMEM((count, width), F32), pltpu.VMEM((n_tp, n_norm, width), F32),
           pltpu.SemaphoreType.DMA((n_pp - 1,)), pltpu.SemaphoreType.DMA((n_pp - 1,)), pltpu.SemaphoreType.DMA((n_tp - 1,)), pltpu.SemaphoreType.DMA((n_tp - 1,))],
        input_output_aliases={17: 2, 18: 3},
        compiler_params=pltpu.CompilerParams(collective_id=2, has_side_effects=True, vmem_limit_bytes=LIMIT),
        cost_estimate=pl.CostEstimate(flops=60_000_000_000, bytes_accessed=16_000_000, transcendentals=0),
    )(grad, hidden, pre_act, query, kv_all, context, lse, *options, vec, cos_tab, sin_tab, rows, *previous, grad_att, grad_mlp)


def solution(mesh):
    n_stages = mesh.shape['pp']
    n_tp = mesh.shape['tp']
    swap_core = [(stage, stage ^ 1) for stage in range(n_stages)]

    def device_fn(x_in, g_out, ln1_gain, ln1_bias, w_qkv, b_qkv, w_out, b_out, ln2_gain, ln2_bias, w_up, b_up, w_down, b_down):
        stage = lax.axis_index('pp')
        core = stage % 2
        seq_len, width = x_in.shape[2:]
        ffn = w_up.shape[2]

        def own_tokens(array):
            blocks = lax.dynamic_index_in_dim(array, stage // 2, 0, keepdims=False).reshape(4, BLOCK, width)
            first = lax.dynamic_index_in_dim(blocks, core, 0, keepdims=False)
            second = lax.dynamic_index_in_dim(blocks, 3 - core, 0, keepdims=False)
            return jnp.concatenate([first, second], axis=0).astype(BF)

        hidden = own_tokens(x_in)
        grad = own_tokens(g_out)

        half_rot = HEAD // 8
        inv_freq = ROPE_BASE ** (-(jnp.arange(half_rot, dtype=F32) * 2.0) / (2 * half_rot))
        spot = jnp.concatenate([core * BLOCK + jnp.arange(BLOCK), (3 - core) * BLOCK + jnp.arange(BLOCK)])
        angles = spot.astype(F32)[:, None] * inv_freq[None, :]
        still = jnp.zeros((ROWS, HEAD - 2 * half_rot), F32)
        cos_tab = jnp.tile(jnp.concatenate([jnp.cos(angles), jnp.cos(angles), still + 1.0], axis=1), (1, 1))
        sin_tab = jnp.tile(jnp.concatenate([jnp.sin(angles), jnp.sin(angles), still], axis=1), (1, 1))

        wq_rows = jnp.transpose(w_qkv[0], (2, 1, 3, 0)).reshape(3 * PART, width)
        bundle = jnp.concatenate([wq_rows, w_out[0].reshape(PART, width), w_up[0], w_down[0]], axis=0)
        bias_qkv = jnp.transpose(b_qkv[0], (1, 0, 2)).reshape(3 * PART).astype(F32)
        pad = jnp.zeros((width - 3 * PART,), F32)
        vectors = jnp.stack([ln1_gain[0], ln1_bias[0], ln2_gain[0], ln2_bias[0], b_out[0].astype(F32) + b_down[0].astype(F32), b_up[0].astype(F32), jnp.concatenate([bias_qkv, pad]), jnp.zeros((width,), F32)])

        n_att = 4 * PART
        pair_a, pair_b = [(0, 2), (2, 0)], [(1, 3), (3, 1)]
        all_vectors = lax.all_gather(vectors, 'pp')
        bundle, all_vectors = tie(bundle, all_vectors)
        first_wave = lax.ppermute(bundle, 'pp', pair_a)
        later, first_wave = tie(bundle, first_wave)
        second_wave = lax.ppermute(later, 'pp', pair_b)
        partner = lax.ppermute(bundle, 'pp', swap_core)
        first_wave, hidden, grad, cos_tab, sin_tab, all_vectors = tie(first_wave, hidden, grad, cos_tab, sin_tab, all_vectors)
        first_pass = lax.ppermute(first_wave, 'pp', [(2, 3), (0, 1)])
        sources = {0: (bundle, partner, first_wave, first_pass), 2: (first_wave, first_pass, bundle, partner)}
        saved = []
        for layer in range(n_stages):
            vec = all_vectors[layer]
            bias_q = vec[6, :3 * PART].reshape(3 * HEADS, HEAD)
            last = layer == n_stages - 1
            result, query, kv_all, context, lse, pre_act = forward_layer(hidden, sources[layer], vec, bias_q, cos_tab, sin_tab, n_tp, not last)
            saved.append((hidden, query, kv_all, context, lse, pre_act))
            if last:
                summed = lax.psum(result, 'tp')
                break
            hidden = result
            if layer == 0:
                hidden, second_wave = tie(hidden, second_wave)
                second_pass = lax.ppermute(second_wave, 'pp', [(3, 2), (1, 0)])
                sources[1] = (partner, bundle, second_pass, second_wave)
                sources[3] = (second_pass, second_wave, partner, bundle)

        small, prod = {}, {}
        grad_att = grad_mlp = None
        for layer in reversed(range(n_stages)):
            hidden, query, kv_all, context, lse, pre_act = saved[layer]
            vec = all_vectors[layer]
            if layer == 0:
                small, grad_att, prev_att, grad_mlp = first_layer_back(
                    grad, hidden, (query, kv_all, context, lse, pre_act), sources[0], vec, cos_tab, sin_tab,
                    jnp.stack([small[index] for index in range(1, n_stages)]), prod[1], grad_att, grad_mlp, n_tp)
                grad_att = jnp.where(stage == 0, grad_att, prev_att)
                break
            gx, prod_m, prod_m_b, small_m = mlp_back(grad, hidden, pre_act, sources[layer], vec, n_tp)
            parts, buffers = [(prod_m, prod_m_b)], [grad_mlp]
            if layer < n_stages - 1:
                parts.append(prod[layer + 1])
                buffers.append(grad_att)
            out = att_back(layer, grad, hidden, gx, query, kv_all, context, lse, sources[layer], vec, cos_tab, sin_tab, n_tp, True, parts, buffers)
            grad, prod[layer], small_a, grad_mlp = out[0], (out[1], out[2]), out[3], out[4]
            if layer < n_stages - 1:
                grad_att = out[5]
            small[layer] = jnp.concatenate([small_a[:2], small_m, small_a[6:]], axis=0)
            if layer == n_stages - 1:
                grad, summed = tie(grad, summed)
        norms = small

        final = (saved[-1][0].astype(F32) + all_vectors[-1][4:5] + summed.astype(F32)).astype(BF)
        gathered = lax.all_gather(final, 'pp').reshape(2, 2, 2, BLOCK, width)
        y_out = jnp.stack([gathered[:, 0, 0], gathered[:, 1, 0], gathered[:, 1, 1], gathered[:, 0, 1]], axis=1).reshape(x_in.shape)

        grad_qkv = jnp.transpose(grad_att[:3 * PART].reshape(3, HEADS, HEAD, width), (3, 1, 0, 2))
        grads = (
            norms[0], norms[1], grad_qkv, jnp.transpose(small[8:8 + 3 * HEADS, :HEAD].reshape(3, HEADS, HEAD), (1, 0, 2)),
            grad_att[3 * PART:].reshape(HEADS, HEAD, width), small[4], norms[2], norms[3],
            grad_mlp[:width], small[5], grad_mlp[width:], small[4])
        return tuple([y_out] + [item[None] for item in grads])

    return jax.shard_map(device_fn, mesh=mesh, in_specs=(P('dp'), P('dp')) + STAGE_SPECS, out_specs=(P('dp'),) + GRAD_SPECS, check_vma=False)
```

```python
import functools

import jax
import jax.numpy as jnp
from jax import lax
from jax.experimental import pallas as pl
from jax.experimental.pallas import tpu as pltpu
from jax.sharding import PartitionSpec as P

BF = jnp.bfloat16
F32 = jnp.float32
ROPE_BASE = 10000.0
LN_EPS = 1e-5
HEADS = 3
HEAD = 64
PART = HEADS * HEAD
BLOCK = 256
ROWS = 2 * BLOCK
STAGE_SPECS = (P('pp', None), P('pp', None), P('pp', None, 'tp', None, None), P('pp', 'tp', None, None), P('pp', 'tp', None, None), P('pp', None), P('pp', None), P('pp', None), P('pp', None, 'tp'), P('pp', 'tp'), P('pp', 'tp', None), P('pp', None))
GRAD_SPECS = (P(('dp', 'pp'), None), P(('dp', 'pp'), None), P(('dp', 'pp'), None, 'tp', None, None), P(('dp', 'pp'), 'tp', None, None), P(('dp', 'pp'), 'tp', None, None), P(('dp', 'pp'), None), P(('dp', 'pp'), None), P(('dp', 'pp'), None), P(('dp', 'pp'), None, 'tp'), P(('dp', 'pp'), 'tp'), P(('dp', 'pp'), 'tp', None), P(('dp', 'pp'), None))
CHUNKS = 8
SMALL = 24
LIMIT = 60 * 2 ** 20
MESH_ID = pl.DeviceIdType.MESH


def tie(*values):
    return lax.optimization_barrier(values)


def dot(left, right, left_dim, right_dim):
    return lax.dot_general(left, right, (((left_dim,), (right_dim,)), ((), ())), preferred_element_type=F32)


def normalise(hidden):
    hidden_f = hidden.astype(F32)
    center = hidden_f - jnp.mean(hidden_f, axis=-1, keepdims=True)
    scale = lax.rsqrt(jnp.mean(center * center, axis=-1, keepdims=True) + LN_EPS)
    return center * scale, scale


def turn_matrix(width, transposed):
    row = lax.broadcasted_iota(jnp.int32, (width, width), 0)
    col = lax.broadcasted_iota(jnp.int32, (width, width), 1)
    if transposed:
        row, col = col, row
    dim = col % HEAD
    minus = (dim < 8) & (row == col + 8)
    plus = (dim >= 8) & (dim < 16) & (row == col - 8)
    return (plus.astype(F32) - minus.astype(F32)).astype(BF)


def rotate_head(values, cos_tab, sin_tab, transposed):
    turned = dot(values, turn_matrix(HEAD, transposed), 1, 0)
    return (values.astype(F32) * cos_tab + turned * sin_tab).astype(BF)


def block_rows(block):
    return slice(block * BLOCK, (block + 1) * BLOCK)


def pick_weights(stage, options, first, count, scratch, sem):
    for index, option in enumerate(options):
        @pl.when(stage == index)
        def fetch():
            pltpu.make_async_copy(option.at[pl.ds(first, count)], scratch, sem).start()

    return pltpu.make_async_copy(options[0].at[pl.ds(first, count)], scratch, sem).wait


def meet(n_tp, with_sum, with_core, with_stage=False):
    rank, stage = lax.axis_index('tp'), lax.axis_index('pp')
    barrier = pltpu.get_barrier_semaphore()
    count = 0
    if with_core:
        pl.semaphore_signal(barrier, inc=1, device_id={'pp': stage + 1 - 2 * lax.rem(stage, 2)}, device_id_type=MESH_ID)
        count = 1
    if with_stage:
        pl.semaphore_signal(barrier, inc=1, device_id={'pp': lax.rem(stage + 2, 4)}, device_id_type=MESH_ID)
        count += 1
    if with_sum:
        is_inner = lax.rem((rank + 1) // 2, 2)
        near = rank + 1 - 2 * lax.rem(rank, 2)
        pl.semaphore_signal(barrier, inc=1, device_id={'tp': near}, device_id_type=MESH_ID)

        @pl.when(is_inner == 1)
        def greet():
            pl.semaphore_signal(barrier, inc=1, device_id={'tp': n_tp - 1 - rank}, device_id_type=MESH_ID)

        count = count + 1 + is_inner
    pl.semaphore_wait(barrier, count)


class LineSum:
    def __init__(self, n_tp, part, base, out, inbox, half, across, sems):
        self.part, self.base, self.out, self.inbox, self.half, self.across, self.sems = part, base, out, inbox, half, across, sems
        rank = lax.axis_index('tp')
        self.is_inner = lax.rem((rank + 1) // 2, 2)
        self.near = rank + 1 - 2 * lax.rem(rank, 2)
        self.mirror = n_tp - 1 - rank
        self.n_chunks = CHUNKS
        self.size = out.shape[0] // CHUNKS

    def span(self, chunk):
        return pl.ds(chunk * self.size, self.size)

    def copy(self, kind, chunk):
        source, target, device = ((self.part, self.inbox, self.near), (self.half, self.across, self.mirror), (self.out, self.out, self.near))[kind]
        return pltpu.make_async_remote_copy(
            src_ref=source.at[self.span(chunk)], dst_ref=target.at[self.span(chunk)], send_sem=self.sems[2 * kind].at[chunk],
            recv_sem=self.sems[2 * kind + 1].at[chunk], device_id={'tp': device}, device_id_type=MESH_ID)

    def offer(self, chunks):
        @pl.when(self.is_inner == 0)
        def start():
            for chunk in chunks:
                self.copy(0, chunk).start()

    def finish(self, chunk):
        rows = self.span(chunk)
        self.copy(1, chunk).wait_recv()
        both = self.half[rows, :].astype(F32) + self.across[rows, :].astype(F32)
        self.out[rows, :] = (self.base(rows) + both).astype(BF)
        self.copy(2, chunk).start()

    def step(self, chunk):
        @pl.when(self.is_inner == 1)
        def merge():
            rows = self.span(chunk)
            self.copy(0, chunk).wait_recv()
            self.half[rows, :] = (self.part[rows, :].astype(F32) + self.inbox[rows, :].astype(F32)).astype(BF)
            self.copy(1, chunk).start()

    def close(self, chunk):
        @pl.when(self.is_inner == 1)
        def end():
            self.finish(chunk)

    def drain(self):
        @pl.when(self.is_inner == 1)
        def inner_end():
            for chunk in range(self.n_chunks):
                self.copy(1, chunk).wait_send()
                self.copy(2, chunk).wait_send()

        @pl.when(self.is_inner == 0)
        def outer_end():
            for chunk in range(self.n_chunks):
                self.copy(2, chunk).wait_recv()
                self.copy(0, chunk).wait_send()


def line_scratch(rows, width):
    return [pltpu.VMEM((rows, width), BF)] * 3 + [pltpu.SemaphoreType.DMA((CHUNKS,))] * 6


class StageSum:
    def __init__(self, layer, prod, prod_b, result, staged, near, far, half, sems):
        self.prod, self.prod_b, self.result, self.staged, self.near, self.far, self.half, self.sems = prod, prod_b, result, staged, near, far, half, sems
        self.stage = lax.axis_index('pp')
        self.is_owner = self.stage == layer
        self.is_relay = self.stage == (layer ^ 2)
        self.is_giver = lax.rem(self.stage, 2) != layer % 2
        self.is_keeper = lax.rem(self.stage, 2) == layer % 2

    def load(self):
        return pltpu.make_async_copy(self.prod, self.staged, self.sems.at[0])

    def store(self):
        return pltpu.make_async_copy(self.staged, self.result, self.sems.at[1])

    def hand(self):
        return pltpu.make_async_remote_copy(
            src_ref=self.prod_b, dst_ref=self.near, send_sem=self.sems.at[2], recv_sem=self.sems.at[3],
            device_id={'pp': self.stage + 1 - 2 * lax.rem(self.stage, 2)}, device_id_type=MESH_ID)

    def cross(self):
        return pltpu.make_async_remote_copy(
            src_ref=self.half, dst_ref=self.far, send_sem=self.sems.at[4], recv_sem=self.sems.at[5],
            device_id={'pp': lax.rem(self.stage + 2, 4)}, device_id_type=MESH_ID)

    def blocks(self):
        return [pl.ds(first, BLOCK) for first in range(0, self.staged.shape[0], BLOCK)]

    def begin(self):
        @pl.when(self.is_giver)
        def give():
            self.hand().start()

        if self.prod is not None:
            @pl.when(self.is_keeper)
            def keep():
                self.load().start()

    def ready(self):
        if self.prod is not None:
            self.load().wait()

    def relay(self):
        @pl.when(self.is_relay)
        def send_on():
            self.ready()
            self.hand().wait_recv()
            for rows in self.blocks():
                self.half[rows, :] = (self.staged[rows, :] + self.near[rows, :].astype(F32)).astype(BF)
            self.cross().start()

    def end(self):
        @pl.when(self.is_owner)
        def close():
            self.ready()
            self.hand().wait_recv()
            self.cross().wait_recv()
            for rows in self.blocks():
                self.staged[rows, :] += self.near[rows, :].astype(F32) + self.far[rows, :].astype(F32)
            self.store().start()
            self.store().wait()

        @pl.when(self.is_relay)
        def relayed():
            self.cross().wait_send()

        @pl.when(self.is_giver)
        def given():
            self.hand().wait_send()


def stage_scratch(rows, width):
    return [pltpu.VMEM((rows, width), F32)] + [pltpu.VMEM((rows, width), BF)] * 3 + [pltpu.SemaphoreType.DMA((6,))]


def forward_kernel(n_tp, with_sum, h_ref, opt0, opt1, opt2, opt3, vec_ref, bq_ref, cos_ref, sin_ref,
                   out_ref, q_ref, kv_ref, ctx_ref, lse_ref, pre_ref, weights, w_sem, active, kv_send, kv_recv, *line_refs):
    stage = lax.axis_index('pp')
    core = lax.rem(stage, 2)
    width = h_ref.shape[1]
    wait_weights = pick_weights(stage, (opt0, opt1, opt2, opt3), 0, weights.shape[0], weights, w_sem)
    meet(n_tp, with_sum, True)
    wait_weights()

    def project(normed, index):
        return (dot(normed, weights[index * HEAD:(index + 1) * HEAD, :], 1, 1) + bq_ref[index:index + 1, :]).astype(BF)

    swaps = []
    for block in range(2):
        rows = block_rows(block)
        xhat, _ = normalise(h_ref[rows, :])
        normed_a = (xhat * vec_ref[0:1, :] + vec_ref[1:2, :]).astype(BF)
        active[rows, :] = (xhat * vec_ref[2:3, :] + vec_ref[3:4, :]).astype(BF)
        cos_tab, sin_tab = cos_ref[rows, :], sin_ref[rows, :]
        place = slice(2 * block * BLOCK, (2 * block + 1) * BLOCK)
        for head in range(HEADS):
            q_ref[head, rows, :] = rotate_head(project(normed_a, head), cos_tab, sin_tab, False)
            kv_ref[head, place, :] = rotate_head(project(normed_a, HEADS + head), cos_tab, sin_tab, False)
            kv_ref[HEADS + head, place, :] = project(normed_a, 2 * HEADS + head)
        copy = pltpu.make_async_remote_copy(
            src_ref=kv_ref.at[:, pl.ds(2 * block * BLOCK, BLOCK), :], dst_ref=kv_ref.at[:, pl.ds((2 * block + 1) * BLOCK, BLOCK), :],
            send_sem=kv_send.at[block], recv_sem=kv_recv.at[block],
            device_id={'pp': stage + 1 - 2 * core}, device_id_type=MESH_ID)
        copy.start()
        swaps.append(copy)
    for block in range(2):
        rows = block_rows(block)
        pre_act = dot(active[rows, :], weights[4 * PART:4 * PART + width, :], 1, 0) + vec_ref[5:6, :]
        pre_ref[rows, :] = pre_act
        active[rows, :] = (0.5 * pre_act * (1.0 + lax.erf(pre_act * (2.0 ** -0.5)))).astype(BF)
    for copy in swaps:
        copy.wait_recv()
    if with_sum:
        part_ref = line_refs[0]
        line = LineSum(n_tp, part_ref, lambda rows: h_ref[rows, :].astype(F32) + vec_ref[4:5, :], out_ref, *line_refs[1:4], line_refs[4:])
    else:
        part_ref = out_ref
    for block in range(2):
        rows = block_rows(block)
        n_keys = (2, 4)[block] * BLOCK
        mask = causal_mask(core, block, n_keys)
        part = dot(active[rows, :], weights[4 * PART + width:, :], 1, 0)
        for head in range(HEADS):
            scores = dot(q_ref[head, rows, :], kv_ref[head, :n_keys, :], 1, 1) * (HEAD ** -0.5)
            scores = jnp.where(mask, scores, -1e30)
            top = jnp.max(scores, axis=-1, keepdims=True)
            expo = jnp.exp(scores - top)
            total = jnp.sum(expo, axis=-1, keepdims=True)
            probs = (expo / total).astype(BF)
            context = dot(probs, kv_ref[HEADS + head, :n_keys, :], 1, 0).astype(BF)
            ctx_ref[head, rows, :] = context
            lse_ref[head, rows, :] = top + jnp.log(total)
            part += dot(context, weights[3 * PART + head * HEAD:3 * PART + (head + 1) * HEAD, :], 1, 0)
        part_ref[rows, :] = part.astype(BF)
        if with_sum:
            line.offer(range(block * CHUNKS // 2, (block + 1) * CHUNKS // 2))
    if with_sum:
        for chunk in range(CHUNKS):
            line.step(chunk)
            if chunk:
                line.close(chunk - 1)
        line.close(CHUNKS - 1)
        line.drain()
    for copy in swaps:
        copy.wait_send()


def forward_layer(hidden, options, vec, bias_q, cos_tab, sin_tab, n_tp, with_sum):
    rows, width = hidden.shape
    block, anywhere = pl.BlockSpec(memory_space=pltpu.VMEM), pl.BlockSpec(memory_space=pl.ANY)
    scratch = [pltpu.VMEM(options[0].shape, BF), pltpu.SemaphoreType.DMA, pltpu.VMEM((rows, width), BF), pltpu.SemaphoreType.DMA((2,)), pltpu.SemaphoreType.DMA((2,))]
    if with_sum:
        scratch += [pltpu.VMEM((rows, width), BF)] + line_scratch(rows, width)
    return pl.pallas_call(
        functools.partial(forward_kernel, n_tp, with_sum),
        out_shape=(jax.ShapeDtypeStruct((rows, width), BF), jax.ShapeDtypeStruct((HEADS, rows, HEAD), BF), jax.ShapeDtypeStruct((2 * HEADS, 2 * rows, HEAD), BF),
                   jax.ShapeDtypeStruct((HEADS, rows, HEAD), BF), jax.ShapeDtypeStruct((HEADS, rows, 1), F32), jax.ShapeDtypeStruct((rows, width), F32)),
        in_specs=[block] + [anywhere] * 4 + [block] * 4,
        out_specs=tuple([block] * 6),
        scratch_shapes=scratch,
        compiler_params=pltpu.CompilerParams(collective_id=0 if with_sum else 1, has_side_effects=True, vmem_limit_bytes=LIMIT),
        cost_estimate=pl.CostEstimate(flops=40_000_000_000, bytes_accessed=8_000_000, transcendentals=0),
    )(hidden, *options, vec, bias_q, cos_tab, sin_tab)


def mlp_body(g_ref, h_ref, pre_ref, vec_ref, weights, base, gx_ref, prod_ref, prod_b_ref, small_ref, small_row, normed, gpre, active, hook):
    width = h_ref.shape[1]
    sums = [0.0] * 4
    for block in range(2):
        rows = block_rows(block)
        grad = g_ref[rows, :]
        pre_act = pre_ref[rows, :]
        gauss = 0.5 * (1.0 + lax.erf(pre_act * (2.0 ** -0.5)))
        active[rows, :] = (pre_act * gauss).astype(BF)
        slope = gauss + pre_act * jnp.exp(-0.5 * pre_act * pre_act) * 0.3989422804014327
        grad_pre = dot(grad, weights[base + width:base + 2 * width, :], 1, 1) * slope
        gpre[rows, :] = grad_pre.astype(BF)
        sums[3] += jnp.sum(grad_pre, axis=0, keepdims=True)
        sums[2] += jnp.sum(grad.astype(F32), axis=0, keepdims=True)
        xhat, _ = normalise(h_ref[rows, :])
        normed[rows, :] = (xhat * vec_ref[2:3, :] + vec_ref[3:4, :]).astype(BF)
        grad_m = dot(gpre[rows, :], weights[base:base + width, :], 1, 1)
        sums[0] += jnp.sum(grad_m * xhat, axis=0, keepdims=True)
        sums[1] += jnp.sum(grad_m, axis=0, keepdims=True)
        if gx_ref is not None:
            gx_ref[rows, :] = grad_m * vec_ref[2:3, :]
    for index, value in enumerate(sums):
        small_ref[small_row + index:small_row + index + 1, :] = value
    hook()
    for first in range(0, width, 256):
        for left, right, row in ((normed, gpre, 0), (active, g_ref, width)):
            value = dot(left[:, first:first + 256], right[...], 0, 0)
            prod_ref[row + first:row + first + 256, :] = value
            prod_b_ref[row + first:row + first + 256, :] = value.astype(BF)


def mlp_back_kernel(n_tp, g_ref, h_ref, pre_ref, opt0, opt1, opt2, opt3, vec_ref, gx_ref, prod_ref, prod_b_ref, small_ref,
                    weights, w_sem, normed, gpre, active):
    stage = lax.axis_index('pp')
    wait_weights = pick_weights(stage, (opt0, opt1, opt2, opt3), 4 * PART, weights.shape[0], weights, w_sem)
    wait_weights()
    mlp_body(g_ref, h_ref, pre_ref, vec_ref, weights, 0, gx_ref, prod_ref, prod_b_ref, small_ref, 0, normed, gpre, active, lambda: None)


def mlp_back(grad, hidden, pre_act, options, vec, n_tp):
    rows, width = hidden.shape
    block, anywhere = pl.BlockSpec(memory_space=pltpu.VMEM), pl.BlockSpec(memory_space=pl.ANY)
    return pl.pallas_call(
        functools.partial(mlp_back_kernel, n_tp),
        out_shape=(jax.ShapeDtypeStruct((rows, width), F32), jax.ShapeDtypeStruct((2 * width, width), F32), jax.ShapeDtypeStruct((2 * width, width), BF), jax.ShapeDtypeStruct((4, width), F32)),
        in_specs=[block] * 3 + [anywhere] * 4 + [block],
        out_specs=tuple([block] * 4),
        scratch_shapes=[pltpu.VMEM((2 * width, width), BF), pltpu.SemaphoreType.DMA] + [pltpu.VMEM((rows, width), BF)] * 3,
        compiler_params=pltpu.CompilerParams(vmem_limit_bytes=LIMIT),
        cost_estimate=pl.CostEstimate(flops=10_000_000_000, bytes_accessed=12_000_000, transcendentals=0),
    )(grad, hidden, pre_act, *options, vec)


def attention_body(g_ref, q_ref, kv_ref, lse_ref, weights, dqkv, dkv, core, between):
    for block in (1, 0):
        rows = block_rows(block)
        n_keys = (2, 4)[block] * BLOCK
        mask = causal_mask(core, block, n_keys)
        for head in range(HEADS):
            d_ctx = dot(g_ref[rows, :], weights[3 * PART + head * HEAD:3 * PART + (head + 1) * HEAD, :], 1, 1).astype(BF)
            q_part = q_ref[head, rows, :]
            k_part = kv_ref[head, :n_keys, :]
            scores = dot(q_part, k_part, 1, 1) * (HEAD ** -0.5)
            probs = jnp.where(mask, jnp.exp(scores - lse_ref[head, rows, :]), 0.0)
            dprobs = dot(d_ctx, kv_ref[HEADS + head, :n_keys, :], 1, 1).astype(BF).astype(F32)
            delta = jnp.sum(probs * dprobs, axis=-1, keepdims=True)
            dscores = (probs * (dprobs - delta) * (HEAD ** -0.5)).astype(BF)
            dqkv[head, rows, :] = dot(dscores, k_part, 1, 0).astype(BF)
            d_k = dot(dscores, q_part, 0, 0)
            d_v = dot(probs.astype(BF), d_ctx, 0, 0)
            if block == 1:
                dkv[head] = d_k
                dkv[HEADS + head] = d_v
            else:
                dkv[head, :n_keys, :] += d_k
                dkv[HEADS + head, :n_keys, :] += d_v
        if block == 1:
            between()


def project_back(h_ref, vec_ref, cos_ref, sin_ref, weights, dqkv, dkv, landed, normed, small_ref, bias_row, pass_on):
    sums = [0.0] * 2
    bias = [0.0] * (3 * HEADS)
    for block in range(2):
        rows = block_rows(block)
        own = slice(2 * block * BLOCK, (2 * block + 1) * BLOCK)
        cos_tab, sin_tab = cos_ref[rows, :], sin_ref[rows, :]
        grad_a = 0.0
        for head in range(HEADS):
            d_q = rotate_head(dqkv[head, rows, :], cos_tab, sin_tab, True)
            d_k = rotate_head((dkv[head, own, :] + landed[head, rows, :]).astype(BF), cos_tab, sin_tab, True)
            d_v = (dkv[HEADS + head, own, :] + landed[HEADS + head, rows, :]).astype(BF)
            for kind, value in enumerate((d_q, d_k, d_v)):
                index = kind * HEADS + head
                dqkv[index, rows, :] = value
                bias[index] += jnp.sum(value.astype(F32), axis=0, keepdims=True)
                grad_a += dot(value, weights[index * HEAD:(index + 1) * HEAD, :], 1, 0)
        xhat, scale = normalise(h_ref[rows, :])
        normed[rows, :] = (xhat * vec_ref[0:1, :] + vec_ref[1:2, :]).astype(BF)
        sums[0] += jnp.sum(grad_a * xhat, axis=0, keepdims=True)
        sums[1] += jnp.sum(grad_a, axis=0, keepdims=True)
        if pass_on is not None:
            pass_on(block, rows, grad_a, xhat, scale)
    for index, value in enumerate(sums):
        small_ref[index:index + 1, :] = value
    for index, value in enumerate(bias):
        small_ref[bias_row + index:bias_row + index + 1, :HEAD] = value


def att_back_kernel(n_tp, layer, with_sum, n_red, g_ref, h_ref, gx_ref, q_ref, kv_ref, ctx_ref, lse_ref, opt0, opt1, opt2, opt3, vec_ref, cos_ref, sin_ref, *refs):
    n_in = (2, 4)[n_red - 1] + (0 if layer == 3 else n_red if layer < 2 else 1)
    given, refs = refs[:n_in], refs[n_in:]
    if with_sum:
        out_ref, refs = refs[0], refs[1:]
    prod_ref, prod_b_ref, small_ref = refs[:3]
    results, refs = refs[3:3 + n_red], refs[3 + n_red:]
    small_ref[...] = jnp.zeros_like(small_ref)
    weights, w_sem, dkv, landed, dqkv, normed, kv_send, kv_recv = refs[:8]
    line_refs = refs[8:]
    reductions = []
    for index in range(n_red):
        own = line_refs[-5 * (n_red - index):][:5]
        reductions.append(StageSum(layer + index, given[2 * index], given[2 * index + 1], results[index], *own))
    line_refs = line_refs[:len(line_refs) - 5 * n_red]
    stage = lax.axis_index('pp')
    core = lax.rem(stage, 2)
    wait_weights = pick_weights(stage, (opt0, opt1, opt2, opt3), 0, weights.shape[0], weights, w_sem)
    meet(n_tp, with_sum, True, True)
    for item in reductions:
        item.begin()
    wait_weights()
    def between():
        for item in reversed(reductions):
            item.relay()

    attention_body(g_ref, q_ref, kv_ref, lse_ref, weights, dqkv, dkv, core, between)
    swaps = []
    for block in range(2):
        copy = pltpu.make_async_remote_copy(
            src_ref=dkv.at[:, pl.ds((2 * block + 1) * BLOCK, BLOCK), :], dst_ref=landed.at[:, pl.ds(block * BLOCK, BLOCK), :],
            send_sem=kv_send.at[block], recv_sem=kv_recv.at[block],
            device_id={'pp': stage + 1 - 2 * core}, device_id_type=MESH_ID)
        copy.start()
        swaps.append(copy)
    if with_sum:
        part_ref = line_refs[0]
        line = LineSum(n_tp, part_ref, lambda rows: g_ref[rows, :].astype(F32), out_ref, *line_refs[1:4], line_refs[4:])
    for copy in swaps:
        copy.wait_recv()

    def pass_on(block, rows, grad_a, xhat, scale):
        grad_x = grad_a * vec_ref[0:1, :] + gx_ref[rows, :]
        branch = scale * (grad_x - jnp.mean(grad_x, axis=-1, keepdims=True) - xhat * jnp.mean(grad_x * xhat, axis=-1, keepdims=True))
        part_ref[rows, :] = branch.astype(BF)
        line.offer(range(block * CHUNKS // 2, (block + 1) * CHUNKS // 2))

    project_back(h_ref, vec_ref, cos_ref, sin_ref, weights, dqkv, dkv, landed, normed, small_ref, 8, pass_on)

    def product(index):
        value = dot(dqkv[index], normed[...], 0, 0) if index < 3 * HEADS else dot(ctx_ref[index - 3 * HEADS], g_ref[...], 0, 0)
        prod_ref[index * HEAD:(index + 1) * HEAD, :] = value
        prod_b_ref[index * HEAD:(index + 1) * HEAD, :] = value.astype(BF)

    n_prod = 4 * HEADS
    for chunk in range(CHUNKS):
        if with_sum:
            line.step(chunk)
        for index in range(chunk * n_prod // CHUNKS, (chunk + 1) * n_prod // CHUNKS):
            product(index)
        if with_sum and chunk:
            line.close(chunk - 1)
    if with_sum:
        line.close(CHUNKS - 1)
        line.drain()
    for copy in swaps:
        copy.wait_send()
    for item in reversed(reductions):
        item.end()


def att_back(layer, grad, hidden, gx, query, kv_all, context, lse, options, vec, cos_tab, sin_tab, n_tp, with_sum, parts, buffers):
    rows, width = hidden.shape
    block, anywhere = pl.BlockSpec(memory_space=pltpu.VMEM), pl.BlockSpec(memory_space=pl.ANY)
    n_att = 4 * PART
    out_shape = [jax.ShapeDtypeStruct((n_att, width), F32), jax.ShapeDtypeStruct((n_att, width), BF), jax.ShapeDtypeStruct((SMALL, width), F32)]
    scratch = [pltpu.VMEM((n_att, width), BF), pltpu.SemaphoreType.DMA, pltpu.VMEM((2 * HEADS, 2 * rows, HEAD), F32), pltpu.VMEM((2 * HEADS, rows, HEAD), F32),
               pltpu.VMEM((3 * HEADS, rows, HEAD), BF), pltpu.VMEM((rows, width), BF), pltpu.SemaphoreType.DMA((2,)), pltpu.SemaphoreType.DMA((2,))]
    if with_sum:
        out_shape = [jax.ShapeDtypeStruct((rows, width), BF)] + out_shape
        scratch += [pltpu.VMEM((rows, width), BF)] + line_scratch(rows, width)
    specs = [block] * len(out_shape)
    extra, aliases = [], {}
    for prod, prod_b in parts:
        extra += [prod, prod_b]
        scratch += stage_scratch(*prod.shape)
    for index, (prod, _) in enumerate(parts):
        if buffers[index] is not None:
            aliases[14 + len(extra)] = len(out_shape) + index
            extra.append(buffers[index])
    out_shape += [jax.ShapeDtypeStruct(prod.shape, F32) for prod, _ in parts]
    specs += [anywhere] * len(parts)
    return pl.pallas_call(
        functools.partial(att_back_kernel, n_tp, layer, with_sum, len(parts)),
        out_shape=tuple(out_shape),
        in_specs=[block] * 7 + [anywhere] * 4 + [block] * 3 + [anywhere] * len(extra),
        out_specs=tuple(specs),
        scratch_shapes=scratch,
        input_output_aliases=aliases,
        compiler_params=pltpu.CompilerParams(collective_id=3 + layer, has_side_effects=True, vmem_limit_bytes=LIMIT),
        cost_estimate=pl.CostEstimate(flops=45_000_000_000, bytes_accessed=12_000_000, transcendentals=0),
    )(grad, hidden, gx, query, kv_all, context, lse, *options, vec, cos_tab, sin_tab, *extra)


def causal_mask(core, block, n_keys):
    row = lax.broadcasted_iota(jnp.int32, (BLOCK, n_keys), 0)
    col = lax.broadcasted_iota(jnp.int32, (BLOCK, n_keys), 1)
    part = col // BLOCK
    starts = (core, 1 - core, 3 - core, 2 + core)
    start = jnp.where(part == 0, starts[0], jnp.where(part == 1, starts[1], jnp.where(part == 2, starts[2], starts[3])))
    mine = core if block == 0 else 3 - core
    return mine * BLOCK + row >= start * BLOCK + (col - part * BLOCK)


def first_layer_kernel(n_pp, n_tp, n_norm, g_ref, h_ref, pre_ref, q_ref, kv_ref, ctx_ref, lse_ref, opt0, opt1, opt2, opt3, vec_ref, cos_ref, sin_ref, rows_ref,
                       prev_ref, prev_b_ref, att_in, mlp_in, out_ref, att_ref, att_prev_ref, mlp_ref,
                       weights, w_sem, dkv, landed, dqkv, normed, kv_send, kv_recv, gpre, active,
                       prod_m, prod_m_b, near_m, far_m, sems_m, prod_a, prod_a_b, near_a, far_a, sems_a, staged_p, near_p, far_p, half_p, sems_p,
                       all_rows, box, stage_sum, norm_box, send_a, recv_a, send_b, recv_b):
    stage, rank = lax.axis_index('pp'), lax.axis_index('tp')
    core = lax.rem(stage, 2)
    wait_weights = pick_weights(stage, (opt0, opt1, opt2, opt3), 0, weights.shape[0], weights, w_sem)
    barrier = pltpu.get_barrier_semaphore()
    for step in range(1, n_pp):
        pl.semaphore_signal(barrier, inc=1, device_id={'pp': lax.rem(stage + step, n_pp)}, device_id_type=MESH_ID)
    for step in range(1, n_tp):
        pl.semaphore_signal(barrier, inc=1, device_id={'tp': lax.rem(rank + step, n_tp)}, device_id_type=MESH_ID)
    pl.semaphore_wait(barrier, n_pp + n_tp - 2)
    before = StageSum(1, prev_ref, prev_b_ref, att_prev_ref, staged_p, near_p, far_p, half_p, sems_p)
    mlp = StageSum(0, None, prod_m_b, mlp_ref, prod_m, near_m, far_m, prod_m_b, sems_m)
    att = StageSum(0, None, prod_a_b, att_ref, prod_a, near_a, far_a, prod_a_b, sems_a)
    before.begin()
    wait_weights()
    small = all_rows.at[0]
    small[...] = jnp.zeros_like(small)
    all_rows[1:, :, :] = rows_ref[...]
    mlp_body(g_ref, h_ref, pre_ref, vec_ref, weights, 4 * PART, None, prod_m, prod_m_b, small, 2, normed, gpre, active, before.relay)
    mlp.begin()
    attention_body(g_ref, q_ref, kv_ref, lse_ref, weights, dqkv, dkv, core, mlp.relay)
    swaps = []
    for block in range(2):
        copy = pltpu.make_async_remote_copy(
            src_ref=dkv.at[:, pl.ds((2 * block + 1) * BLOCK, BLOCK), :], dst_ref=landed.at[:, pl.ds(block * BLOCK, BLOCK), :],
            send_sem=kv_send.at[block], recv_sem=kv_recv.at[block],
            device_id={'pp': stage + 1 - 2 * core}, device_id_type=MESH_ID)
        copy.start()
        swaps.append(copy)
    for head in range(HEADS):
        index = 3 * HEADS + head
        value = dot(ctx_ref[head], g_ref[...], 0, 0)
        prod_a[index * HEAD:(index + 1) * HEAD, :] = value
        prod_a_b[index * HEAD:(index + 1) * HEAD, :] = value.astype(BF)
    for copy in swaps:
        copy.wait_recv()
    project_back(h_ref, vec_ref, cos_ref, sin_ref, weights, dqkv, dkv, landed, normed, small, 8, None)
    for index in range(3 * HEADS):
        value = dot(dqkv[index], normed[...], 0, 0)
        prod_a[index * HEAD:(index + 1) * HEAD, :] = value
        prod_a_b[index * HEAD:(index + 1) * HEAD, :] = value.astype(BF)
    att.begin()
    sends = []
    for step in range(1, n_pp):
        peer = lax.rem(stage + step, n_pp)
        copy = pltpu.make_async_remote_copy(
            src_ref=all_rows.at[peer], dst_ref=box.at[step - 1], send_sem=send_a.at[step - 1],
            recv_sem=recv_a.at[step - 1], device_id={'pp': peer}, device_id_type=MESH_ID)
        copy.start()
        sends.append(copy)
    att.relay()
    total = all_rows[stage]
    for step, copy in enumerate(sends):
        copy.wait_recv()
        total += box[step]
    stage_sum[...] = total
    norm_box[rank] = total[:n_norm]
    shares = []
    for step in range(1, n_tp):
        copy = pltpu.make_async_remote_copy(
            src_ref=stage_sum.at[pl.ds(0, n_norm)], dst_ref=norm_box.at[rank], send_sem=send_b.at[step - 1],
            recv_sem=recv_b.at[step - 1], device_id={'tp': lax.rem(rank + step, n_tp)}, device_id_type=MESH_ID)
        copy.start()
        shares.append(copy)
    before.end()
    mlp.end()
    for copy in shares:
        copy.wait()
    norms = norm_box[0]
    for index in range(1, n_tp):
        norms += norm_box[index]
    out_ref[:n_norm, :] = norms
    out_ref[n_norm:, :] = total[n_norm:]
    for copy in sends + swaps:
        copy.wait_send()
    att.end()


def first_layer_back(grad, hidden, saved, options, vec, cos_tab, sin_tab, rows, previous, grad_att, grad_mlp, n_tp):
    query, kv_all, context, lse, pre_act = saved
    n_others, count, width = rows.shape
    n_pp, tokens, n_att = n_others + 1, hidden.shape[0], 4 * PART
    n_norm = 4
    block, anywhere = pl.BlockSpec(memory_space=pltpu.VMEM), pl.BlockSpec(memory_space=pl.ANY)

    def resident(n_rows):
        return [pltpu.VMEM((n_rows, width), F32)] + [pltpu.VMEM((n_rows, width), BF)] * 3 + [pltpu.SemaphoreType.DMA((6,))]

    return pl.pallas_call(
        functools.partial(first_layer_kernel, n_pp, n_tp, n_norm),
        out_shape=(jax.ShapeDtypeStruct((count, width), F32), jax.ShapeDtypeStruct((n_att, width), F32), jax.ShapeDtypeStruct((n_att, width), F32), jax.ShapeDtypeStruct((2 * width, width), F32)),
        in_specs=[block] * 7 + [anywhere] * 4 + [block] * 4 + [anywhere] * 4,
        out_specs=(block, anywhere, anywhere, anywhere),
        scratch_shapes=[pltpu.VMEM((n_att + 2 * width, width), BF), pltpu.SemaphoreType.DMA, pltpu.VMEM((2 * HEADS, 2 * tokens, HEAD), F32), pltpu.VMEM((2 * HEADS, tokens, HEAD), F32),
                        pltpu.VMEM((3 * HEADS, tokens, HEAD), BF), pltpu.VMEM((tokens, width), BF), pltpu.SemaphoreType.DMA((2,)), pltpu.SemaphoreType.DMA((2,)),
                        pltpu.VMEM((tokens, width), BF), pltpu.VMEM((tokens, width), BF)]
        + resident(2 * width) + resident(n_att) + stage_scratch(n_att, width)
        + [pltpu.VMEM((n_pp, count, width), F32), pltpu.VMEM((n_pp - 1, count, width), F32), pltpu.VMEM((count, width), F32), pltpu.VMEM((n_tp, n_norm, width), F32),
           pltpu.SemaphoreType.DMA((n_pp - 1,)), pltpu.SemaphoreType.DMA((n_pp - 1,)), pltpu.SemaphoreType.DMA((n_tp - 1,)), pltpu.SemaphoreType.DMA((n_tp - 1,))],
        input_output_aliases={17: 2, 18: 3},
        compiler_params=pltpu.CompilerParams(collective_id=2, has_side_effects=True, vmem_limit_bytes=LIMIT),
        cost_estimate=pl.CostEstimate(flops=60_000_000_000, bytes_accessed=16_000_000, transcendentals=0),
    )(grad, hidden, pre_act, query, kv_all, context, lse, *options, vec, cos_tab, sin_tab, rows, *previous, grad_att, grad_mlp)


def solution(mesh):
    n_stages = mesh.shape['pp']
    n_tp = mesh.shape['tp']
    swap_core = [(stage, stage ^ 1) for stage in range(n_stages)]

    def device_fn(x_in, g_out, ln1_gain, ln1_bias, w_qkv, b_qkv, w_out, b_out, ln2_gain, ln2_bias, w_up, b_up, w_down, b_down):
        stage = lax.axis_index('pp')
        core = stage % 2
        seq_len, width = x_in.shape[2:]
        ffn = w_up.shape[2]

        def own_tokens(array):
            blocks = lax.dynamic_index_in_dim(array, stage // 2, 0, keepdims=False).reshape(4, BLOCK, width)
            first = lax.dynamic_index_in_dim(blocks, core, 0, keepdims=False)
            second = lax.dynamic_index_in_dim(blocks, 3 - core, 0, keepdims=False)
            return jnp.concatenate([first, second], axis=0).astype(BF)

        hidden = own_tokens(x_in)
        grad = own_tokens(g_out)

        half_rot = HEAD // 8
        inv_freq = ROPE_BASE ** (-(jnp.arange(half_rot, dtype=F32) * 2.0) / (2 * half_rot))
        spot = jnp.concatenate([core * BLOCK + jnp.arange(BLOCK), (3 - core) * BLOCK + jnp.arange(BLOCK)])
        angles = spot.astype(F32)[:, None] * inv_freq[None, :]
        still = jnp.zeros((ROWS, HEAD - 2 * half_rot), F32)
        cos_tab = jnp.tile(jnp.concatenate([jnp.cos(angles), jnp.cos(angles), still + 1.0], axis=1), (1, 1))
        sin_tab = jnp.tile(jnp.concatenate([jnp.sin(angles), jnp.sin(angles), still], axis=1), (1, 1))

        wq_rows = jnp.transpose(w_qkv[0], (2, 1, 3, 0)).reshape(3 * PART, width)
        bundle = jnp.concatenate([wq_rows, w_out[0].reshape(PART, width), w_up[0], w_down[0]], axis=0)
        bias_qkv = jnp.transpose(b_qkv[0], (1, 0, 2)).reshape(3 * PART).astype(F32)
        pad = jnp.zeros((width - 3 * PART,), F32)
        vectors = jnp.stack([ln1_gain[0], ln1_bias[0], ln2_gain[0], ln2_bias[0], b_out[0].astype(F32) + b_down[0].astype(F32), b_up[0].astype(F32), jnp.concatenate([bias_qkv, pad]), jnp.zeros((width,), F32)])

        n_att = 4 * PART
        pair_a, pair_b = [(0, 2), (2, 0)], [(1, 3), (3, 1)]
        first_wave = lax.ppermute(bundle, 'pp', pair_a)
        later, first_wave = tie(bundle, first_wave)
        second_wave = lax.ppermute(later, 'pp', pair_b)
        partner = lax.ppermute(bundle, 'pp', swap_core)
        all_vectors = lax.all_gather(vectors, 'pp')
        first_wave, hidden, grad, cos_tab, sin_tab, all_vectors = tie(first_wave, hidden, grad, cos_tab, sin_tab, all_vectors)
        first_pass = lax.ppermute(first_wave, 'pp', [(2, 3), (0, 1)])
        sources = {0: (bundle, partner, first_wave, first_pass), 2: (first_wave, first_pass, bundle, partner)}
        saved = []
        for layer in range(n_stages):
            vec = all_vectors[layer]
            bias_q = vec[6, :3 * PART].reshape(3 * HEADS, HEAD)
            last = layer == n_stages - 1
            result, query, kv_all, context, lse, pre_act = forward_layer(hidden, sources[layer], vec, bias_q, cos_tab, sin_tab, n_tp, not last)
            saved.append((hidden, query, kv_all, context, lse, pre_act))
            if last:
                summed = lax.psum(result, 'tp')
                break
            hidden = result
            if layer == 0:
                hidden, second_wave = tie(hidden, second_wave)
                second_pass = lax.ppermute(second_wave, 'pp', [(3, 2), (1, 0)])
                sources[1] = (partner, bundle, second_pass, second_wave)
                sources[3] = (second_pass, second_wave, partner, bundle)

        small, prod = {}, {}
        grad_att = grad_mlp = None
        for layer in reversed(range(n_stages)):
            hidden, query, kv_all, context, lse, pre_act = saved[layer]
            vec = all_vectors[layer]
            if layer == 0:
                small, grad_att, prev_att, grad_mlp = first_layer_back(
                    grad, hidden, (query, kv_all, context, lse, pre_act), sources[0], vec, cos_tab, sin_tab,
                    jnp.stack([small[index] for index in range(1, n_stages)]), prod[1], grad_att, grad_mlp, n_tp)
                grad_att = jnp.where(stage == 0, grad_att, prev_att)
                break
            gx, prod_m, prod_m_b, small_m = mlp_back(grad, hidden, pre_act, sources[layer], vec, n_tp)
            parts, buffers = [(prod_m, prod_m_b)], [grad_mlp]
            if layer < n_stages - 1:
                parts.append(prod[layer + 1])
                buffers.append(grad_att)
            out = att_back(layer, grad, hidden, gx, query, kv_all, context, lse, sources[layer], vec, cos_tab, sin_tab, n_tp, True, parts, buffers)
            grad, prod[layer], small_a, grad_mlp = out[0], (out[1], out[2]), out[3], out[4]
            if layer < n_stages - 1:
                grad_att = out[5]
            small[layer] = jnp.concatenate([small_a[:2], small_m, small_a[6:]], axis=0)
            if layer == n_stages - 1:
                grad, summed = tie(grad, summed)
        norms = small

        final = (saved[-1][0].astype(F32) + all_vectors[-1][4:5] + summed.astype(F32)).astype(BF)
        gathered = lax.all_gather(final, 'pp').reshape(2, 2, 2, BLOCK, width)
        y_out = jnp.stack([gathered[:, 0, 0], gathered[:, 1, 0], gathered[:, 1, 1], gathered[:, 0, 1]], axis=1).reshape(x_in.shape)

        grad_qkv = jnp.transpose(grad_att[:3 * PART].reshape(3, HEADS, HEAD, width), (3, 1, 0, 2))
        grads = (
            norms[0], norms[1], grad_qkv, jnp.transpose(small[8:8 + 3 * HEADS, :HEAD].reshape(3, HEADS, HEAD), (1, 0, 2)),
            grad_att[3 * PART:].reshape(HEADS, HEAD, width), small[4], norms[2], norms[3],
            grad_mlp[:width], small[5], grad_mlp[width:], small[4])
        return tuple([y_out] + [item[None] for item in grads])

    return jax.shard_map(device_fn, mesh=mesh, in_specs=(P('dp'), P('dp')) + STAGE_SPECS, out_specs=(P('dp'),) + GRAD_SPECS, check_vma=False)
```
